16 devices in a mesh: tp: 2 (over z), side: 2 (over y), rep: 4 (over x, core).
Axes of the slice: x: 2, y: 2, z: 2, core: 2. Of those that a mesh axis runs over, the one named last changes fastest.
Arguments:
- w_up: float32 [2, 6, 896, 4864], P('side', None, ('rep', 'tp'))
- w_down: float32 [2, 6, 4864, 896], P('side', None, None, ('rep', 'tp'))
- g_up: float32 [2, 6, 896, 4864], P('side', None, ('rep', 'tp'))
- g_down: float32 [2, 6, 4864, 896], P('side', None, None, ('rep', 'tp'))
- learn_rate: float32 [2], P('side')
- prompts: bfloat16 [2, 4, 8192, 896], P('side', 'rep')
Outputs:
- output 1: float32 [2, 6, 896, 4864], P('side', None, ('rep', 'tp'))
- output 2: float32 [2, 6, 4864, 896], P('side', None, None, ('rep', 'tp'))
- output 3: bfloat16 [2, 4, 8192, 896], P('side', 'rep')
All inputs are finite; a program needn't handle non-finite values.
Results may differ from the reference program's by a relative error of at most 0.0155867.
Values are sent between devices in bfloat16 or wider.
A program may use at most 1 GiB of HBM per device.

```python
import jax
import jax.numpy as jnp
from jax import lax

NUM_LAYERS = 6
MODEL_DIM = 896
HIDDEN_DIM = 4864
NUM_REPS = 4
NUM_TOKENS = 8192


def setup_inputs(seed: int = 0) -> dict:
    keys = jax.random.split(jax.random.key(seed), 6)
    up_shape = (NUM_LAYERS, MODEL_DIM, HIDDEN_DIM)
    down_shape = (NUM_LAYERS, HIDDEN_DIM, MODEL_DIM)
    up_scale = MODEL_DIM ** -0.5
    down_scale = (2.0 / (HIDDEN_DIM * NUM_LAYERS)) ** 0.5
    w_up = jax.random.normal(keys[0], up_shape, jnp.float32) * up_scale
    w_down = jax.random.normal(keys[1], down_shape, jnp.float32) * down_scale
    g_up = jax.random.normal(keys[2], up_shape, jnp.float32) * up_scale
    g_down = jax.random.normal(keys[3], down_shape, jnp.float32) * down_scale
    rate = jax.random.uniform(keys[4], (1,), jnp.float32, 0.04, 0.2)
    prompts = jax.random.normal(keys[5], (NUM_REPS, NUM_TOKENS, MODEL_DIM), jnp.float32)
    zero_up = jnp.zeros(up_shape, jnp.float32)
    zero_down = jnp.zeros(down_shape, jnp.float32)
    return {
        "w_up": jnp.stack([w_up, zero_up]),
        "w_down": jnp.stack([w_down, zero_down]),
        "g_up": jnp.stack([g_up, zero_up]),
        "g_down": jnp.stack([g_down, zero_down]),
        "learn_rate": jnp.concatenate([rate, jnp.zeros((1,), jnp.float32)]),
        "prompts": jnp.stack([jnp.zeros_like(prompts), prompts]).astype(jnp.bfloat16),
    }


def reference(w_up, w_down, g_up, g_down, learn_rate, prompts):
    rate = learn_rate[0]
    new_up = w_up[0] - rate * g_up[0]
    new_down = w_down[0] - rate * g_down[0]
    cast_up = new_up.astype(jnp.bfloat16)
    cast_down = new_down.astype(jnp.bfloat16)

    def layer_step(hidden, weights):
        up_mat, down_mat = weights
        pre_act = jnp.dot(hidden, up_mat, preferred_element_type=jnp.float32)
        act_up = jax.nn.gelu(pre_act, approximate=True).astype(jnp.bfloat16)
        part_sum = jnp.dot(act_up, down_mat, preferred_element_type=jnp.float32)
        return (hidden.astype(jnp.float32) + part_sum).astype(jnp.bfloat16), None

    def replica_forward(rows):
        return lax.scan(layer_step, rows, (cast_up, cast_down))[0]

    gen_out = lax.map(replica_forward, prompts[1])
    up_out = jnp.stack([new_up, jnp.zeros_like(new_up)])
    down_out = jnp.stack([new_down, jnp.zeros_like(new_down)])
    tok_out = jnp.stack([jnp.zeros_like(gen_out), gen_out])
    return (up_out, down_out, tok_out)
```

```python
import jax
import jax.numpy as jnp
from jax import lax
from jax.sharding import PartitionSpec as P


def solution(mesh):
    up_spec = P("side", None, ("rep", "tp"), None)
    down_spec = P("side", None, None, ("rep", "tp"))
    tok_spec = P("side", "rep", None, None)

    def device_step(w_up, w_down, g_up, g_down, learn_rate, prompts):
        is_trainer = lax.axis_index("side") == 0
        rate = learn_rate[0]
        new_up = jnp.where(is_trainer, w_up - rate * g_up, 0.0)
        new_down = jnp.where(is_trainer, w_down - rate * g_down, 0.0)
        layers = w_up.shape[1]
        full_up, full_down = [], []
        for layer in range(layers):
            up_band = (w_up[0, layer] - rate * g_up[0, layer]).astype(jnp.bfloat16)
            down_band = (w_down[0, layer] - rate * g_down[0, layer]).astype(jnp.bfloat16).T
            recv_up = lax.ppermute(up_band, "side", perm=[(0, 1)])
            recv_down = lax.ppermute(down_band, "side", perm=[(0, 1)])
            full_up.append(lax.all_gather(recv_up, ("rep", "tp"), axis=0, tiled=True))
            full_down.append(lax.all_gather(recv_down, ("rep", "tp"), axis=0, tiled=True))
        rows = prompts.shape[2] // mesh.shape["tp"]
        hidden = lax.dynamic_slice_in_dim(prompts[0, 0], lax.axis_index("tp") * rows, rows, 0)
        for layer in range(layers):
            pre_act = jnp.dot(hidden, full_up[layer], preferred_element_type=jnp.float32)
            act_up = jax.nn.gelu(pre_act, approximate=True).astype(jnp.bfloat16)
            part_sum = lax.dot_general(
                act_up, full_down[layer], (((1,), (1,)), ((), ())), preferred_element_type=jnp.float32
            )
            hidden = (hidden.astype(jnp.float32) + part_sum).astype(jnp.bfloat16)
        hidden = lax.all_gather(hidden, "tp", axis=0, tiled=True)
        gen_out = jnp.where(is_trainer, jnp.zeros_like(hidden), hidden)
        return new_up, new_down, gen_out[None, None]

    return jax.shard_map(
        device_step,
        mesh=mesh,
        in_specs=(up_spec, down_spec, up_spec, down_spec, P("side"), tok_spec),
        out_specs=(up_spec, down_spec, tok_spec),
        check_vma=False,
    )
```

```python
import functools

import jax
import jax.numpy as jnp
from jax import lax
from jax.experimental import pallas as pl
from jax.experimental.pallas import tpu as pltpu
from jax.sharding import PartitionSpec as P

MESH = pl.DeviceIdType.MESH
UNIT = 256
HALF = 2048
OUT_ROWS = 512
LOAD_SLOTS = 4
STAGE_SLOTS = 8
GELU_A = 0.7978845608028654
GELU_B = 0.7978845608028654 * 0.044715


def gelu(a):
    return a * (0.5 * jnp.tanh(a * (GELU_A + GELU_B * (a * a))) + 0.5)


def kernel(
    rate_ref, w_up, w_dn, g_up, g_dn, prompts, out, wbuf,
    h, p, wv, fin, stage, rows_buf, zrow,
    rs, ss, lsem, fsem, tss, iosem, osem,
):
    layers, band, hidden = w_up.shape
    chunks = hidden // UNIT
    total = layers * chunks
    pairs = (chunks - 1) // 2
    n_rows, d = out.shape
    my_rows = n_rows // 2
    halves = my_rows // HALF
    blocks = my_rows // OUT_ROWS

    tp = lax.axis_index("tp")
    side = lax.axis_index("side")
    rep = lax.axis_index("rep")
    x, k = rep // 2, rep % 2
    flip_tp = 1 - tp
    flip_rep = (1 - x) * 2 + k
    sib_rep = x * 2 + (1 - k)

    def band_of(r, t):
        return pl.multiple_of((r * 2 + t) * band, 16)

    own = band_of(rep, tp)
    znb = band_of(rep, flip_tp)
    xnb = band_of(flip_rep, tp)
    dia = band_of(flip_rep, flip_tp)

    def both(c, b):
        return wbuf.at[c, :, pl.ds(b, band), :]

    def one(c, m, b):
        return wbuf.at[c, m, pl.ds(b, band), :]

    Y, YD, Z, X, DG, SB = range(6)

    def send(src, dst, ssem, rsem, t, s, r):
        pltpu.make_async_remote_copy(
            src_ref=src, dst_ref=dst, send_sem=ssem, recv_sem=rsem,
            device_id={"tp": t, "side": s, "rep": r}, device_id_type=MESH,
        ).start()

    def wait(ref, sem):
        pltpu.make_async_copy(ref, ref, sem).wait()

    @pl.when(side == 0)
    def _():
        rate = rate_ref[0]

        def loads(c):
            l, j = c // chunks, c % chunks
            cols = pl.ds(pl.multiple_of(j * UNIT, UNIT), UNIT)
            slot = c % LOAD_SLOTS
            return [
                pltpu.make_async_copy(r.at[l, :, cols], fin.at[slot, i], lsem.at[slot, i])
                for i, r in enumerate((w_up, g_up, w_dn, g_dn))
            ]

        for c in range(LOAD_SLOTS - 1):
            for cp in loads(c):
                cp.start()

        def send_chunk(c):
            slot = c % STAGE_SLOTS
            send(stage.at[slot], both(c, own), tss.at[slot, 0], rs.at[Y, c], tp, 1, rep)
            send(stage.at[slot, 1], one(c, 1, own), tss.at[slot, 1], rs.at[DG, c], flip_tp, 0, flip_rep)

        def wait_sent(c):
            slot = c % STAGE_SLOTS
            wait(stage.at[slot], tss.at[slot, 0])
            wait(stage.at[slot, 1], tss.at[slot, 1])

        def relay(c):
            wait(one(c, 1, dia), rs.at[DG, c])
            send(one(c, 1, dia), one(c, 1, dia), ss.at[0, c // chunks], rs.at[YD, c], tp, 1, rep)

        lag = 3

        def body(c, _):
            @pl.when(c < total)
            def _():
                @pl.when(c + LOAD_SLOTS - 1 < total)
                def _():
                    for cp in loads(c + LOAD_SLOTS - 1):
                        cp.start()

                for cp in loads(c):
                    cp.wait()
                slot, lslot = c % STAGE_SLOTS, c % LOAD_SLOTS

                @pl.when(c >= STAGE_SLOTS)
                def _():
                    wait_sent(c - STAGE_SLOTS)

                stage[slot, 0] = (fin[lslot, 0] - rate * fin[lslot, 1]).astype(jnp.bfloat16)
                stage[slot, 1] = (fin[lslot, 2] - rate * fin[lslot, 3]).astype(jnp.bfloat16)

            @pl.when((c >= 1) & (c < total + 1))
            def _():
                send_chunk(c - 1)

            @pl.when(c >= lag)
            def _():
                relay(c - lag)

            return 0

        lax.fori_loop(0, total + lag, body, 0)

        zrow[...] = jnp.zeros_like(zrow)
        copies = [
            pltpu.make_async_copy(zrow, out.at[pl.ds(b * OUT_ROWS, OUT_ROWS)], iosem.at[b])
            for b in range(2 * blocks)
        ]
        for cp in copies:
            cp.start()

        def drain(c, _):
            wait_sent(total - STAGE_SLOTS + c)
            return 0

        lax.fori_loop(0, STAGE_SLOTS, drain, 0)
        for l in range(layers):
            wait(wbuf.at[pl.ds(l * chunks, chunks), 0, pl.ds(0, band), :], ss.at[0, l])
        for cp in copies:
            cp.wait()

    @pl.when(side == 1)
    def _():
        def y_stage(c):
            l = c // chunks
            wait(both(c, own), rs.at[Y, c])
            send(both(c, own), both(c, own), ss.at[0, l], rs.at[Z, c], flip_tp, 1, rep)
            send(both(c, own), both(c, own), ss.at[1, l], rs.at[X, c], tp, 1, flip_rep)
            send(one(c, 0, own), one(c, 0, own), ss.at[2, l], rs.at[DG, c], flip_tp, 1, flip_rep)
            send(both(c, own), both(c, own), ss.at[3, l], rs.at[SB, c], tp, 1, sib_rep)

        def n_stage(c):
            l = c // chunks
            wait(both(c, znb), rs.at[Z, c])
            send(both(c, znb), both(c, znb), ss.at[4, l], rs.at[SB, c], tp, 1, sib_rep)
            wait(both(c, xnb), rs.at[X, c])
            send(both(c, xnb), both(c, xnb), ss.at[5, l], rs.at[SB, c], tp, 1, sib_rep)
            wait(one(c, 0, dia), rs.at[DG, c])
            send(one(c, 0, dia), one(c, 0, dia), ss.at[6, l], rs.at[SB, c], tp, 1, sib_rep)
            wait(one(c, 1, dia), rs.at[YD, c])
            send(one(c, 1, dia), one(c, 1, dia), ss.at[7, l], rs.at[SB, c], tp, 1, sib_rep)

        def wload(c, slot, half):
            cols = pl.ds(half * UNIT, UNIT)
            return [
                pltpu.make_async_copy(wbuf.at[c, m], wv.at[slot, m, :, cols], fsem.at[slot, half, m])
                for m in range(2)
            ]

        def s_stage(c, slot, half):
            wait(wbuf.at[c, :, pl.ds(0, 4 * band), :], rs.at[SB, c])
            for cp in wload(c, slot, half):
                cp.start()

        def guarded(fn, c, *a):
            @pl.when(c < total)
            def _():
                fn(c, *a)

        base = tp * my_rows

        def pload(b, slot):
            return pltpu.make_async_copy(
                prompts.at[pl.ds(base + b * OUT_ROWS, OUT_ROWS)], rows_buf.at[slot], iosem.at[slot]
            )

        pload(0, 0).start()
        for b in range(blocks):
            if b + 1 < blocks:
                pload(b + 1, (b + 1) % 2).start()
            pload(b, b % 2).wait()
            per = HALF // OUT_ROWS
            h[b // per, :, pl.ds((b % per) * OUT_ROWS, OUT_ROWS)] = rows_buf[b % 2].T

        y_stage(0)
        y_stage(1)
        n_stage(0)
        n_stage(1)
        y_stage(2)
        y_stage(3)
        s_stage(0, 0, 0)
        s_stage(1, 0, 1)
        n_stage(2)
        n_stage(3)
        y_stage(4)
        y_stage(5)

        def compute(slot, width, first):
            def half_body(i, _):
                a = lax.dot_general(
                    wv[slot, 0, :, :width], h[i], (((0,), (0,)), ((), ())), preferred_element_type=jnp.float32
                )
                u = gelu(a).astype(jnp.bfloat16)
                prev = jnp.where(first, 0.0, p[i])
                p[i] = prev + jnp.dot(wv[slot, 1, :, :width], u, preferred_element_type=jnp.float32)
                return 0

            lax.fori_loop(0, halves, half_body, 0)

        def layer_body(l, _):
            c_layer = l * chunks

            def pair_body(i, _):
                step = l * (pairs + 1) + i
                slot = step % 2
                c0 = c_layer + 2 * i
                for half in range(2):
                    for cp in wload(c0 + half, slot, half):
                        cp.wait()
                guarded(y_stage, c0 + 6)
                guarded(y_stage, c0 + 7)
                guarded(n_stage, c0 + 4)
                guarded(n_stage, c0 + 5)
                s_stage(c0 + 2, 1 - slot, 0)

                @pl.when(i < pairs - 1)
                def _():
                    s_stage(c0 + 3, 1 - slot, 1)

                compute(slot, 2 * UNIT, i == 0)
                return 0

            lax.fori_loop(0, pairs, pair_body, 0)
            step = l * (pairs + 1) + pairs
            slot = step % 2
            c0 = c_layer + 2 * pairs
            for cp in wload(c0, slot, 0):
                cp.wait()
            guarded(y_stage, c0 + 6)
            guarded(n_stage, c0 + 4)
            guarded(s_stage, c0 + 1, 1 - slot, 0)
            guarded(s_stage, c0 + 2, 1 - slot, 1)
            compute(slot, UNIT, False)

            @pl.when(l < layers - 1)
            def _():
                def fin_body(b, _):
                    cols = pl.ds(pl.multiple_of((b % 4) * (HALF // 4), HALF // 4), HALF // 4)
                    i = b // 4
                    h[i, :, cols] = (h[i, :, cols].astype(jnp.float32) + p[i, :, cols]).astype(jnp.bfloat16)
                    return 0

                lax.fori_loop(0, halves * 4, fin_body, 0)

            return 0

        lax.fori_loop(0, layers, layer_body, 0)

        per = HALF // OUT_ROWS

        def put(b):
            rows = pl.ds(base + b * OUT_ROWS, OUT_ROWS)
            pltpu.make_async_copy(rows_buf.at[b % 2], out.at[rows], iosem.at[b % 2]).start()
            send(rows_buf.at[b % 2], out.at[rows], tss.at[b % 2, 0], osem.at[b], flip_tp, 1, rep)

        def put_wait(b):
            wait(rows_buf.at[b % 2], iosem.at[b % 2])
            wait(rows_buf.at[b % 2], tss.at[b % 2, 0])

        for b in range(blocks):
            if b >= 2:
                put_wait(b - 2)
            cols = pl.ds((b % per) * OUT_ROWS, OUT_ROWS)
            i = b // per
            rows_buf[b % 2] = (h[i, :, cols].astype(jnp.float32) + p[i, :, cols]).astype(jnp.bfloat16).T
            if b >= 1:
                put(b - 1)
        put(blocks - 1)
        put_wait(blocks - 2)
        put_wait(blocks - 1)
        other = flip_tp * my_rows
        for b in range(blocks):
            wait(out.at[pl.ds(other + b * OUT_ROWS, OUT_ROWS)], osem.at[b])
        kinds = [2, 2, 1, 2, 2, 2, 1, 1]
        for l in range(layers):
            for i, n in enumerate(kinds):
                wait(wbuf.at[pl.ds(l * chunks, chunks), pl.ds(0, n), pl.ds(0, band), :], ss.at[i, l])


def solution(mesh):
    up_spec = P("side", None, ("rep", "tp"), None)
    down_spec = P("side", None, None, ("rep", "tp"))
    tok_spec = P("side", "rep", None, None)

    def device_step(w_up, w_down, g_up, g_down, learn_rate, prompts):
        is_trainer = lax.axis_index("side") == 0
        rate = learn_rate[0]
        layers, band, hidden = w_up.shape[1:]
        n_rows, d = prompts.shape[2:]
        total = layers * hidden // UNIT
        w_dn = jnp.swapaxes(w_down[0], 1, 2)
        g_dn = jnp.swapaxes(g_down[0], 1, 2)
        my_rows = n_rows // 2
        blocks = my_rows // OUT_ROWS
        any_spec = pl.BlockSpec(memory_space=pl.ANY)
        gen_out, _ = pl.pallas_call(
            kernel,
            name="sync_and_forward",
            out_shape=(
                jax.ShapeDtypeStruct((n_rows, d), jnp.bfloat16),
                jax.ShapeDtypeStruct((total, 2, d, UNIT), jnp.bfloat16),
            ),
            in_specs=[pl.BlockSpec(memory_space=pltpu.SMEM)] + [any_spec] * 5,
            out_specs=(any_spec, any_spec),
            scratch_shapes=[
                pltpu.VMEM((my_rows // HALF, d, HALF), jnp.bfloat16),
                pltpu.VMEM((my_rows // HALF, d, HALF), jnp.float32),
                pltpu.VMEM((2, 2, d, 2 * UNIT), jnp.bfloat16),
                pltpu.VMEM((LOAD_SLOTS, 4, band, UNIT), jnp.float32),
                pltpu.VMEM((STAGE_SLOTS, 2, band, UNIT), jnp.bfloat16),
                pltpu.VMEM((2, OUT_ROWS, d), jnp.bfloat16),
                pltpu.VMEM((OUT_ROWS, d), jnp.bfloat16),
                pltpu.SemaphoreType.DMA((6, total)),
                pltpu.SemaphoreType.DMA((8, layers)),
                pltpu.SemaphoreType.DMA((LOAD_SLOTS, 4)),
                pltpu.SemaphoreType.DMA((2, 2, 2)),
                pltpu.SemaphoreType.DMA((STAGE_SLOTS, 2)),
                pltpu.SemaphoreType.DMA((2 * blocks,)),
                pltpu.SemaphoreType.DMA((blocks,)),
            ],
            compiler_params=pltpu.CompilerParams(
                has_side_effects=True, vmem_limit_bytes=60 * 1024 * 1024
            ),
        )(learn_rate, w_up[0], w_dn, g_up[0], g_dn, prompts[0, 0])
        new_up = jnp.where(is_trainer, w_up - rate * g_up, 0.0)
        new_down = jnp.where(is_trainer, w_down - rate * g_down, 0.0)
        return new_up, new_down, gen_out[None, None]

    return jax.shard_map(
        device_step,
        mesh=mesh,
        in_specs=(up_spec, down_spec, up_spec, down_spec, P("side"), tok_spec),
        out_specs=(up_spec, down_spec, tok_spec),
        check_vma=False,
    )
```

```python
import jax
import jax.numpy as jnp
from jax import lax
from jax.experimental import pallas as pl
from jax.experimental.pallas import tpu as pltpu
from jax.sharding import PartitionSpec as P

MESH = pl.DeviceIdType.MESH
UNIT = 256
GROUP = 4
BLOCK = 1024
PIECE = 128
LOAD_SLOTS = 4
STAGE_SLOTS = 8
GELU_A = 0.7978845608028654
GELU_B = 0.7978845608028654 * 0.044715


def gelu(a):
    return a * (0.5 * jnp.tanh(a * (GELU_A + GELU_B * (a * a))) + 0.5)


def relays_of(rb, blocks, pieces):
    return pieces // 2 - (rb == blocks - 1).astype(jnp.int32)


def sync_kernel(
    rate_ref, w_up, w_dn, g_up, g_dn, prompts, out, wbuf, rin, rx,
    h, p, wv, fin, stage, rows_buf,
    rs, ss, lsem, fsem, tss, iosem, psem, osem, rsem,
):
    layers, band, hidden = w_up.shape
    chunks = hidden // UNIT
    total = layers * chunks
    groups = -(-chunks // GROUP)
    lead = chunks - (groups - 1) * GROUP
    n_rows, d = out.shape
    my_rows = n_rows // 2
    blocks = my_rows // BLOCK
    pieces = BLOCK // PIECE
    n_relay = blocks * (pieces // 2) - 1

    tp = lax.axis_index("tp")
    side = lax.axis_index("side")
    rep = lax.axis_index("rep")
    x, k = rep // 2, rep % 2
    flip_tp = 1 - tp
    flip_rep = (1 - x) * 2 + k
    sib_rep = x * 2 + (1 - k)

    def band_of(r, t):
        return pl.multiple_of((r * 2 + t) * band, 16)

    own = band_of(rep, tp)
    znb = band_of(rep, flip_tp)
    xnb = band_of(flip_rep, tp)
    dia = band_of(flip_rep, flip_tp)

    def both(c, b):
        return wbuf.at[c, :, pl.ds(b, band), :]

    Y, Z, X, DG, SB = range(5)

    def send(src, dst, ssem, rsem_, t, s, r):
        pltpu.make_async_remote_copy(
            src_ref=src, dst_ref=dst, send_sem=ssem, recv_sem=rsem_,
            device_id={"tp": t, "side": s, "rep": r}, device_id_type=MESH,
        ).start()

    def wait(ref, sem):
        pltpu.make_async_copy(ref, ref, sem).wait()

    def n_mod(l, m):
        return sum(1 for c in range(l * chunks, (l + 1) * chunks) if c % 3 == m)

    def piece_rows(t, rb, j):
        return pl.ds(pl.multiple_of(t * my_rows + rb * BLOCK + j * PIECE, PIECE), PIECE)

    @pl.when(side == 0)
    def _():
        rate = rate_ref[0]

        def loads(c):
            l, j = c // chunks, c % chunks
            cols = pl.ds(pl.multiple_of(j * UNIT, UNIT), UNIT)
            slot = c % LOAD_SLOTS
            return [
                pltpu.make_async_copy(r.at[l, :, cols], fin.at[slot, i], lsem.at[slot, i])
                for i, r in enumerate((w_up, g_up, w_dn, g_dn))
            ]

        for c in range(LOAD_SLOTS - 1):
            for cp in loads(c):
                cp.start()

        def send_chunk(c):
            slot = c % STAGE_SLOTS
            send(stage.at[slot], both(c, own), tss.at[slot, 0], rs.at[Y, c], tp, 1, rep)

            @pl.when(c % 3 == 0)
            def _():
                send(stage.at[slot], both(c, own), tss.at[slot, 1], rs.at[DG, c], flip_tp, 0, flip_rep)

        def wait_sent(c):
            slot = c % STAGE_SLOTS
            wait(stage.at[slot], tss.at[slot, 0])

            @pl.when(c % 3 == 0)
            def _():
                wait(stage.at[slot], tss.at[slot, 1])

        lag = 2

        def body(c, _):
            @pl.when(c < total)
            def _():
                @pl.when(c + LOAD_SLOTS - 1 < total)
                def _():
                    for cp in loads(c + LOAD_SLOTS - 1):
                        cp.start()

                for cp in loads(c):
                    cp.wait()
                slot, lslot = c % STAGE_SLOTS, c % LOAD_SLOTS

                @pl.when(c >= STAGE_SLOTS)
                def _():
                    wait_sent(c - STAGE_SLOTS)

                stage[slot, 0] = (fin[lslot, 0] - rate * fin[lslot, 1]).astype(jnp.bfloat16)
                stage[slot, 1] = (fin[lslot, 2] - rate * fin[lslot, 3]).astype(jnp.bfloat16)

            @pl.when((c >= 1) & (c < total + 1))
            def _():
                send_chunk(c - 1)

            @pl.when((c >= lag) & ((c - lag) % 3 == 0))
            def _():
                r = c - lag
                wait(both(r, dia), rs.at[DG, r])
                send(both(r, dia), both(r, dia), ss.at[0, r // chunks], rs.at[DG, r], tp, 1, rep)

            return 0

        lax.fori_loop(0, total + lag, body, 0)

        def drain(c, _):
            wait_sent(total - STAGE_SLOTS + c)
            return 0

        lax.fori_loop(0, STAGE_SLOTS, drain, 0)
        for l in range(layers):
            wait(wbuf.at[pl.ds(l * chunks, n_mod(l, 0)), :, pl.ds(0, band), :], ss.at[0, l])

        per = pieces // 2

        def relay(i, _):
            @pl.when(i < n_relay)
            def _():
                wait(rin.at[i], rsem.at[0, i])
                send(rin.at[i], rx.at[i], tss.at[0, 0], rsem.at[1, i], flip_tp, 0, rep)

            @pl.when(i >= 1)
            def _():
                q = i - 1
                wait(rx.at[q], rsem.at[1, q])
                rb, j = q // per, q % per
                send(rx.at[q], out.at[piece_rows(flip_tp, rb, j)], tss.at[1, 0],
                     osem.at[rb * pieces + j], tp, 1, rep)

            return 0

        lax.fori_loop(0, n_relay + 1, relay, 0)
        wait(rin.at[pl.ds(0, n_relay)], tss.at[0, 0])
        wait(rx.at[pl.ds(0, n_relay)], tss.at[1, 0])

    @pl.when(side == 1)
    def _():
        def y_stage(c):
            l = c // chunks
            wait(both(c, own), rs.at[Y, c])
            send(both(c, own), both(c, own), ss.at[0, l], rs.at[Z, c], flip_tp, 1, rep)
            send(both(c, own), both(c, own), ss.at[1, l], rs.at[X, c], tp, 1, flip_rep)
            send(both(c, own), both(c, own), ss.at[2, l], rs.at[SB, c], tp, 1, sib_rep)

        def n_stage(c):
            l = c // chunks
            wait(both(c, znb), rs.at[Z, c])

            @pl.when(c % 3 == 1)
            def _():
                send(both(c, znb), both(c, znb), ss.at[6, l], rs.at[DG, c], tp, 1, flip_rep)

            send(both(c, znb), both(c, znb), ss.at[3, l], rs.at[SB, c], tp, 1, sib_rep)
            wait(both(c, xnb), rs.at[X, c])

            @pl.when(c % 3 == 2)
            def _():
                send(both(c, xnb), both(c, xnb), ss.at[7, l], rs.at[DG, c], flip_tp, 1, rep)

            send(both(c, xnb), both(c, xnb), ss.at[4, l], rs.at[SB, c], tp, 1, sib_rep)

        def d_stage(c):
            wait(both(c, dia), rs.at[DG, c])
            send(both(c, dia), both(c, dia), ss.at[5, c // chunks], rs.at[SB, c], tp, 1, sib_rep)

        def s_wait(c):
            wait(wbuf.at[c, :, pl.ds(0, 4 * band), :], rs.at[SB, c])

        def wload(c, slot, j):
            return [
                pltpu.make_async_copy(
                    wbuf.at[c, m], wv.at[slot, m, :, pl.ds(j * UNIT, UNIT)], fsem.at[slot, j, m]
                )
                for m in range(2)
            ]

        def start(cps):
            for cp in cps:
                cp.start()

        def finish(cps):
            for cp in cps:
                cp.wait()

        def y_front(q):
            return jnp.minimum(total, 7 + q + q // 8)

        def n_front(q):
            return jnp.minimum(total, 5 + q + q // 9)

        def d_front(q):
            return jnp.minimum(total, 4 + q + q // 10)

        def run(fn, lo, hi):
            def body(c, _):
                fn(c)
                return 0

            lax.fori_loop(lo, hi, body, 0)

        def advance(q):
            run(y_stage, y_front(q), y_front(q + 1))
            run(n_stage, n_front(q), n_front(q + 1))
            run(d_stage, d_front(q), d_front(q + 1))

        def pload(b):
            rows = pl.ds(pl.multiple_of(tp * my_rows + b * BLOCK, BLOCK), BLOCK)
            return pltpu.make_async_copy(prompts.at[rows], rows_buf.at[b % 2], iosem.at[b % 2])

        pload(0).start()
        for b in range(blocks):
            if b + 1 < blocks:
                pload(b + 1).start()
            pload(b).wait()
            for j in range(pieces):
                h[b, :, pl.ds(j * PIECE, PIECE)] = rows_buf[b % 2, pl.ds(j * PIECE, PIECE), :].T

        for c in range(7):
            y_stage(c)
            if c >= 2:
                n_stage(c - 2)
            if c >= 3:
                d_stage(c - 3)
            if c >= 7 - lead:
                s_wait(c - (7 - lead))
                start(wload(c - (7 - lead), 0, c - (7 - lead)))

        def matmuls(slot, rb, width):
            a = lax.dot_general(
                wv[slot, 0, :, :width], h[rb], (((0,), (0,)), ((), ())), preferred_element_type=jnp.float32
            )
            u = gelu(a).astype(jnp.bfloat16)
            return jnp.dot(wv[slot, 1, :, :width], u, preferred_element_type=jnp.float32)

        def first_part(slot, rb):
            p[rb] = matmuls(slot, rb, lead * UNIT)

        def mid_part(slot, rb):
            p[rb] = p[rb] + matmuls(slot, rb, GROUP * UNIT)

        def last_part(slot, rb):
            s = p[rb] + matmuls(slot, rb, GROUP * UNIT)
            h[rb] = (h[rb].astype(jnp.float32) + s).astype(jnp.bfloat16)

        def group_step(l, g, width, n_next, part):
            step = l * groups + g
            slot = step % 2
            c0 = l * chunks + (0 if width == lead else lead + (g - 1) * GROUP)
            for j in range(width):
                finish(wload(c0 + j, slot, j))

            def block(rb, _):
                advance(step * blocks + rb)

                @pl.when(rb < n_next)
                def _():
                    c = c0 + width + rb
                    s_wait(c)
                    cols = pl.ds(pl.multiple_of(rb * UNIT, UNIT), UNIT)
                    for m in range(2):
                        pltpu.make_async_copy(
                            wbuf.at[c, m], wv.at[1 - slot, m, :, cols], fsem.at[1 - slot, rb, m]
                        ).start()

                part(slot, rb)
                return 0

            lax.fori_loop(0, blocks, block, 0)

        def layer_body(l, _):
            group_step(l, 0, lead, GROUP, first_part)

            def mid(g, _):
                group_step(l, g, GROUP, GROUP, mid_part)
                return 0

            lax.fori_loop(1, groups - 1, mid, 0)
            group_step(l, groups - 1, GROUP, lead, last_part)
            return 0

        lax.fori_loop(0, layers - 1, layer_body, 0)
        fine = (layers - 1) * groups * blocks
        run(y_stage, y_front(fine), total)
        run(n_stage, n_front(fine), total)
        run(d_stage, d_front(fine), total)
        run(s_wait, total - chunks + lead, total)

        c_last = total - chunks

        def group_chunk(g):
            return c_last + lead + (g - 1) * GROUP

        def load_group(c0, width, slot):
            for j in range(width):
                start(wload(c0 + j, slot, j))

        def wait_group(c0, width, slot):
            for j in range(width):
                finish(wload(c0 + j, slot, j))

        def put(rb, j):
            src = rows_buf.at[rb % 2, pl.ds(j * PIECE, PIECE), :]
            rows = piece_rows(tp, rb, j)
            pltpu.make_async_copy(src, out.at[rows], psem.at[rb % 2, j, 0]).start()
            by_relay = j < relays_of(rb, blocks, pieces)

            @pl.when(by_relay)
            def _():
                i = rb * (pieces // 2) + min(j, pieces // 2 - 1)
                send(src, rin.at[i], psem.at[rb % 2, j, 1], rsem.at[0, i], tp, 0, rep)

            @pl.when(jnp.logical_not(by_relay))
            def _():
                send(src, out.at[rows], psem.at[rb % 2, j, 1], osem.at[rb * pieces + j], flip_tp, 1, rep)

        def put_wait(rb):
            for j in range(pieces):
                src = rows_buf.at[rb % 2, pl.ds(j * PIECE, PIECE), :]
                wait(src, psem.at[rb % 2, j, 0])
                wait(src, psem.at[rb % 2, j, 1])

        def row_block(rb, _):
            step = (layers - 1) * groups + rb * groups
            slot = step % 2
            wait_group(c_last, lead, slot)
            load_group(c_last + lead, GROUP, 1 - slot)
            first_part(slot, rb)

            def mid(g, _):
                s = (step + g) % 2
                wait_group(group_chunk(g), GROUP, s)
                load_group(group_chunk(g + 1), GROUP, 1 - s)
                mid_part(s, rb)
                return 0

            lax.fori_loop(1, groups - 1, mid, 0)
            s = (step + groups - 1) % 2
            wait_group(group_chunk(groups - 1), GROUP, s)

            @pl.when(rb < blocks - 1)
            def _():
                load_group(c_last, lead, 1 - s)

            last_part(s, rb)

            @pl.when(rb >= 2)
            def _():
                put_wait(rb - 2)

            for j in range(pieces):
                cols = pl.ds(j * PIECE, PIECE)
                rows_buf[rb % 2, cols, :] = h[rb, :, cols].T
                if j >= 1:
                    put(rb, j - 1)
            put(rb, pieces - 1)
            return 0

        lax.fori_loop(0, blocks, row_block, 0)
        for rb in range(max(blocks - 2, 0), blocks):
            put_wait(rb)
        for i in range(blocks * pieces):
            wait(out.at[piece_rows(flip_tp, i // pieces, i % pieces)], osem.at[i])
        for l in range(layers):
            for i in range(8):
                n = n_mod(l, i - 5) if i >= 6 else chunks
                wait(wbuf.at[pl.ds(l * chunks, n), :, pl.ds(0, band), :], ss.at[i, l])


def finish_kernel(rate_ref, w_up, w_dn, g_up, g_dn, mid, new_up, new_dn, out, wb, gb, nb, ob, lsem, ssem, csem, zsem):
    layers, band, hidden = w_up.shape
    n_rows, d = out.shape
    slots, piece = ob.shape[:2]
    n_pieces = n_rows // piece
    side = lax.axis_index("side")
    arrays = ((w_up, g_up, new_up), (w_dn, g_dn, new_dn))
    work = [(a, l) for l in range(layers) for a in range(2)]

    @pl.when(side == 0)
    def _():
        rate = rate_ref[0]

        def load(i):
            a, l = work[i]
            return [
                pltpu.make_async_copy(arrays[a][0].at[l], wb.at[i % 2], lsem.at[i % 2, 0]),
                pltpu.make_async_copy(arrays[a][1].at[l], gb.at[i % 2], lsem.at[i % 2, 1]),
            ]

        def store(i):
            a, l = work[i]
            return pltpu.make_async_copy(nb.at[i % 2], arrays[a][2].at[l], ssem.at[i % 2])

        ob[0] = jnp.zeros(ob.shape[1:], ob.dtype)
        for cp in load(0):
            cp.start()
        for i in range(len(work)):
            if i + 1 < len(work):
                for cp in load(i + 1):
                    cp.start()
            for cp in load(i):
                cp.wait()
            if i >= 2:
                store(i - 2).wait()
            nb[i % 2] = wb[i % 2] - rate * gb[i % 2]
            store(i).start()
        zeros = [
            pltpu.make_async_copy(ob.at[0], out.at[pl.ds(i * piece, piece)], zsem.at[i]) for i in range(n_pieces)
        ]
        for cp in zeros:
            cp.start()
        for i in (len(work) - 2, len(work) - 1):
            store(i).wait()
        for cp in zeros:
            cp.wait()

    @pl.when(side == 1)
    def _():
        def load(i):
            return pltpu.make_async_copy(mid.at[pl.ds(i * piece, piece)], ob.at[i % slots], csem.at[i % slots, 0])

        def store(i):
            return pltpu.make_async_copy(ob.at[i % slots], out.at[pl.ds(i * piece, piece)], csem.at[i % slots, 1])

        for i in range(min(slots, n_pieces)):
            load(i).start()
        nb[0] = jnp.zeros(nb.shape[1:], nb.dtype)
        half = slots // 2
        for i in range(n_pieces):
            load(i).wait()
            store(i).start()
            n = i + half
            if i >= half and n < n_pieces:
                store(n - slots).wait()
                load(n).start()
        zeros = [
            pltpu.make_async_copy(nb.at[0], arrays[a][2].at[l], zsem.at[i]) for i, (a, l) in enumerate(work)
        ]
        for cp in zeros:
            cp.start()
        for i in range(max(n_pieces - slots, 0), n_pieces):
            store(i).wait()
        for cp in zeros:
            cp.wait()


def solution(mesh):
    up_spec = P("side", None, ("rep", "tp"), None)
    down_spec = P("side", None, None, ("rep", "tp"))
    tok_spec = P("side", "rep", None, None)

    def device_step(w_up, w_down, g_up, g_down, learn_rate, prompts):
        layers, band, hidden = w_up.shape[1:]
        n_rows, d = prompts.shape[2:]
        chunks = hidden // UNIT
        total = layers * chunks
        my_rows = n_rows // 2
        blocks, pieces = my_rows // BLOCK, BLOCK // PIECE
        weights = (w_up[0], jnp.swapaxes(w_down[0], 1, 2), g_up[0], jnp.swapaxes(g_down[0], 1, 2))
        smem = pl.BlockSpec(memory_space=pltpu.SMEM)
        hbm = pl.BlockSpec(memory_space=pl.ANY)
        bf16 = jnp.bfloat16
        relay = jax.ShapeDtypeStruct((blocks * pieces // 2, PIECE, d), bf16)
        rows_out, _, _, _ = pl.pallas_call(
            sync_kernel,
            name="sync_and_forward",
            out_shape=(
                jax.ShapeDtypeStruct((n_rows, d), bf16),
                jax.ShapeDtypeStruct((total, 2, d, UNIT), bf16),
                relay,
                relay,
            ),
            in_specs=[smem] + [hbm] * 5,
            out_specs=(hbm,) * 4,
            scratch_shapes=[
                pltpu.VMEM((blocks, d, BLOCK), bf16),
                pltpu.VMEM((blocks, d, BLOCK), jnp.float32),
                pltpu.VMEM((2, 2, d, GROUP * UNIT), bf16),
                pltpu.VMEM((LOAD_SLOTS, 4, band, UNIT), jnp.float32),
                pltpu.VMEM((STAGE_SLOTS, 2, band, UNIT), bf16),
                pltpu.VMEM((2, BLOCK, d), bf16),
                pltpu.SemaphoreType.DMA((5, total)),
                pltpu.SemaphoreType.DMA((8, layers)),
                pltpu.SemaphoreType.DMA((LOAD_SLOTS, 4)),
                pltpu.SemaphoreType.DMA((2, GROUP, 2)),
                pltpu.SemaphoreType.DMA((STAGE_SLOTS, 2)),
                pltpu.SemaphoreType.DMA((2,)),
                pltpu.SemaphoreType.DMA((2, pieces, 2)),
                pltpu.SemaphoreType.DMA((blocks * pieces,)),
                pltpu.SemaphoreType.DMA((2, blocks * pieces // 2)),
            ],
            compiler_params=pltpu.CompilerParams(has_side_effects=True, vmem_limit_bytes=60 * 1024 * 1024),
        )(learn_rate, *weights, prompts[0, 0])
        piece = n_rows // 16
        new_up, new_dn, gen_out = pl.pallas_call(
            finish_kernel,
            name="write_outputs",
            out_shape=(
                jax.ShapeDtypeStruct((layers, band, hidden), jnp.float32),
                jax.ShapeDtypeStruct((layers, band, hidden), jnp.float32),
                jax.ShapeDtypeStruct((n_rows, d), bf16),
            ),
            in_specs=[smem] + [hbm] * 5,
            out_specs=(hbm,) * 3,
            scratch_shapes=[
                pltpu.VMEM((2, band, hidden), jnp.float32),
                pltpu.VMEM((2, band, hidden), jnp.float32),
                pltpu.VMEM((2, band, hidden), jnp.float32),
                pltpu.VMEM((8, piece, d), bf16),
                pltpu.SemaphoreType.DMA((2, 2)),
                pltpu.SemaphoreType.DMA((2,)),
                pltpu.SemaphoreType.DMA((8, 2)),
                pltpu.SemaphoreType.DMA((max(16, 2 * layers),)),
            ],
            compiler_params=pltpu.CompilerParams(vmem_limit_bytes=62 * 1024 * 1024),
        )(learn_rate, *weights, rows_out)
        return new_up[None], jnp.swapaxes(new_dn, 1, 2)[None], gen_out[None, None]

    return jax.shard_map(
        device_step,
        mesh=mesh,
        in_specs=(up_spec, down_spec, up_spec, down_spec, P("side"), tok_spec),
        out_specs=(up_spec, down_spec, tok_spec),
        check_vma=False,
    )
```

```python
import jax
import jax.numpy as jnp
from jax import lax
from jax.experimental import pallas as pl
from jax.experimental.pallas import tpu as pltpu
from jax.sharding import PartitionSpec as P

MESH = pl.DeviceIdType.MESH
UNIT = 256
GROUP = 4
BLOCK = 1024
PIECE = 128
LOAD_SLOTS = 4
STAGE_SLOTS = 12
AHEAD = 3
GELU_A = 0.7978845608028654
GELU_B = 0.7978845608028654 * 0.044715


def gelu(a):
    return a * (0.5 * jnp.tanh(a * (GELU_A + GELU_B * (a * a))) + 0.5)


def relays_of(rb, blocks, pieces):
    return pieces // 2 - (rb == blocks - 1).astype(jnp.int32)


def sync_kernel(
    rate_ref, w_up, w_dn, g_up, g_dn, prompts, out, nu, nd, wbuf, rin, rx,
    h, p, wv, fin, fnew, stage, rows_buf,
    rs, ss, lsem, fsem, tss, iosem, psem, osem, rsem,
):
    layers, band, hidden = w_up.shape
    chunks = hidden // UNIT
    total = layers * chunks
    groups = -(-chunks // GROUP)
    lead = chunks - (groups - 1) * GROUP
    n_rows, d = out.shape
    my_rows = n_rows // 2
    blocks = my_rows // BLOCK
    pieces = BLOCK // PIECE
    n_relay = blocks * (pieces // 2) - 1

    tp = lax.axis_index("tp")
    side = lax.axis_index("side")
    rep = lax.axis_index("rep")
    x, k = rep // 2, rep % 2
    flip_tp = 1 - tp
    flip_rep = (1 - x) * 2 + k
    sib_rep = x * 2 + (1 - k)

    own, znb, xnb, dia = (x, tp), (x, flip_tp), (1 - x, tp), (1 - x, flip_tp)

    def both(c, b):
        return wbuf.at[c, :, b[0], k, b[1]]

    Y, Z, X, DG, SB = range(5)

    def send(src, dst, ssem, rsem_, t, s, r):
        pltpu.make_async_remote_copy(
            src_ref=src, dst_ref=dst, send_sem=ssem, recv_sem=rsem_,
            device_id={"tp": t, "side": s, "rep": r}, device_id_type=MESH,
        ).start()

    def wait(ref, sem):
        pltpu.make_async_copy(ref, ref, sem).wait()

    def start(cps):
        for cp in cps:
            cp.start()

    def finish(cps):
        for cp in cps:
            cp.wait()

    def n_mod(l, m):
        return sum(1 for c in range(l * chunks, (l + 1) * chunks) if c % 3 == m)

    def piece_rows(t, rb, j):
        return pl.ds(pl.multiple_of(t * my_rows + rb * BLOCK + j * PIECE, PIECE), PIECE)

    @pl.when(side == 0)
    def _():
        rate = rate_ref[0]
        parts = ((w_up, g_up, nu), (w_dn, g_dn, nd))

        def cols_of(c):
            return c // chunks, pl.ds(pl.multiple_of((c % chunks) * UNIT, UNIT), UNIT)

        def loads(c):
            l, cols = cols_of(c)
            slot = c % LOAD_SLOTS
            return [
                pltpu.make_async_copy(r.at[l, :, cols], fin.at[slot, 2 * m + i], lsem.at[slot, 2 * m + i])
                for m in range(2)
                for i, r in enumerate(parts[m][:2])
            ]

        def stores(c):
            l, cols = cols_of(c)
            slot = c % LOAD_SLOTS
            return [
                pltpu.make_async_copy(fnew.at[slot, m], parts[m][2].at[l, :, cols], fsem.at[slot // 2, slot % 2, m])
                for m in range(2)
            ]

        for c in range(LOAD_SLOTS - 1):
            start(loads(c))

        def send_own(c):
            send(stage.at[c % STAGE_SLOTS], both(c, own), tss.at[c % STAGE_SLOTS, 0], rs.at[Y, c], tp, 1, rep)

        def send_dia(c):
            send(stage.at[c % STAGE_SLOTS], both(c, own), tss.at[c % STAGE_SLOTS, 1], rs.at[DG, c], flip_tp, 0, flip_rep)

        def wait_sent(c):
            slot = c % STAGE_SLOTS
            wait(stage.at[slot], tss.at[slot, 0])

            @pl.when(c % 3 == 0)
            def _():
                wait(stage.at[slot], tss.at[slot, 1])

        def body(c, _):
            @pl.when(c < total)
            def _():
                @pl.when(c + LOAD_SLOTS - 1 < total)
                def _():
                    start(loads(c + LOAD_SLOTS - 1))

                finish(loads(c))
                slot, lslot = c % STAGE_SLOTS, c % LOAD_SLOTS

                @pl.when(c >= STAGE_SLOTS)
                def _():
                    wait_sent(c - STAGE_SLOTS)

                @pl.when(c >= LOAD_SLOTS)
                def _():
                    finish(stores(c - LOAD_SLOTS))

                for m in range(2):
                    new = fin[lslot, 2 * m] - rate * fin[lslot, 2 * m + 1]
                    fnew[lslot, m] = new
                    stage[slot, m] = new.astype(jnp.bfloat16)

            @pl.when((c >= 1) & (c < total + 1))
            def _():
                start(stores(c - 1))

                @pl.when((c - 1) % 3 == 0)
                def _():
                    send_dia(c - 1)

            r = c - 1 - AHEAD

            @pl.when(r >= 0)
            def _():
                send_own(r)

                @pl.when(r % 3 == 0)
                def _():
                    wait(both(r, dia), rs.at[DG, r])
                    send(both(r, dia), both(r, dia), ss.at[0, r // chunks], rs.at[DG, r], tp, 1, rep)

            return 0

        lax.fori_loop(0, total + 1 + AHEAD, body, 0)

        def drain(c, _):
            wait_sent(total - STAGE_SLOTS + c)
            return 0

        lax.fori_loop(0, STAGE_SLOTS, drain, 0)
        for c in range(total - LOAD_SLOTS, total):
            finish(stores(c))
        for l in range(layers):
            wait(wbuf.at[pl.ds(l * chunks, n_mod(l, 0)), :, 0, 0, 0], ss.at[0, l])

        per = pieces // 2

        def relay(i, _):
            @pl.when(i < n_relay)
            def _():
                wait(rin.at[i], rsem.at[0, i])
                send(rin.at[i], rx.at[i], tss.at[0, 0], rsem.at[1, i], flip_tp, 0, rep)

            @pl.when(i >= 1)
            def _():
                q = i - 1
                wait(rx.at[q], rsem.at[1, q])
                rb, j = q // per, q % per
                send(rx.at[q], out.at[piece_rows(flip_tp, rb, j)], tss.at[1, 0],
                     osem.at[rb * pieces + j], tp, 1, rep)

            return 0

        lax.fori_loop(0, n_relay + 1, relay, 0)
        wait(rin.at[pl.ds(0, n_relay)], tss.at[0, 0])
        wait(rx.at[pl.ds(0, n_relay)], tss.at[1, 0])

    @pl.when(side == 1)
    def _():
        def y_stage(c):
            l = c // chunks
            wait(both(c, own), rs.at[Y, c])
            send(both(c, own), both(c, own), ss.at[0, l], rs.at[Z, c], flip_tp, 1, rep)
            send(both(c, own), both(c, own), ss.at[1, l], rs.at[X, c], tp, 1, flip_rep)

        def n_stage(c):
            l = c // chunks
            wait(both(c, znb), rs.at[Z, c])

            @pl.when(c % 3 == 1)
            def _():
                send(both(c, znb), both(c, znb), ss.at[2, l], rs.at[DG, c], tp, 1, flip_rep)

            wait(both(c, xnb), rs.at[X, c])

            @pl.when(c % 3 == 2)
            def _():
                send(both(c, xnb), both(c, xnb), ss.at[3, l], rs.at[DG, c], flip_tp, 1, rep)

        def core_half(c, core):
            return wbuf.at[c, :, :, core]

        def d_stage(c):
            wait(both(c, dia), rs.at[DG, c])
            send(core_half(c, k), core_half(c, k), ss.at[4, c // chunks], rs.at[SB, c], tp, 1, sib_rep)

        def s_wait(c):
            wait(core_half(c, 1 - k), rs.at[SB, c])

        def wload(c, slot, j):
            cols = pl.ds(j * UNIT if isinstance(j, int) else pl.multiple_of(j * UNIT, UNIT), UNIT)
            return [
                pltpu.make_async_copy(wbuf.at[c, m], wv.at[slot, m, :, :, :, :, cols], fsem.at[slot, j, m])
                for m in range(2)
            ]

        def y_front(q):
            return jnp.minimum(total, 8 + q + q // 5)

        def n_front(q):
            return jnp.minimum(total, 6 + q + q // 6)

        def d_front(q):
            return jnp.minimum(total, 4 + q + q // 10)

        def run(fn, lo, hi):
            def body(c, _):
                fn(c)
                return 0

            lax.fori_loop(lo, hi, body, 0)

        def pload(b):
            rows = pl.ds(pl.multiple_of(tp * my_rows + b * BLOCK, BLOCK), BLOCK)
            return pltpu.make_async_copy(prompts.at[rows], rows_buf.at[b % 2], iosem.at[b % 2])

        pload(0).start()
        for b in range(blocks):
            if b + 1 < blocks:
                pload(b + 1).start()
            pload(b).wait()
            for j in range(pieces):
                h[b, :, pl.ds(j * PIECE, PIECE)] = rows_buf[b % 2, pl.ds(j * PIECE, PIECE), :].T

        for c in range(8):
            y_stage(c)
            if c >= 2:
                n_stage(c - 2)
            if c >= 4:
                d_stage(c - 4)
            if c >= 8 - lead:
                s_wait(c - (8 - lead))
                start(wload(c - (8 - lead), 0, c - (8 - lead)))

        def matmuls(slot, rb, width):
            def weight(m):
                return wv[slot, m, :, :, :, :, : width * UNIT].reshape(d, width * UNIT)

            a = lax.dot_general(weight(0), h[rb], (((0,), (0,)), ((), ())), preferred_element_type=jnp.float32)
            u = gelu(a).astype(jnp.bfloat16)
            return jnp.dot(weight(1), u, preferred_element_type=jnp.float32)

        def put(rb, j):
            src = rows_buf.at[rb % 2, pl.ds(j * PIECE, PIECE), :]
            rows = piece_rows(tp, rb, j)
            pltpu.make_async_copy(src, out.at[rows], psem.at[rb % 2, j, 0]).start()
            by_relay = j < relays_of(rb, blocks, pieces)

            @pl.when(by_relay)
            def _():
                i = rb * (pieces // 2) + min(j, pieces // 2 - 1)
                send(src, rin.at[i], psem.at[rb % 2, j, 1], rsem.at[0, i], tp, 0, rep)

            @pl.when(jnp.logical_not(by_relay))
            def _():
                send(src, out.at[rows], psem.at[rb % 2, j, 1], osem.at[rb * pieces + j], flip_tp, 1, rep)

        def put_wait(rb):
            for j in range(pieces):
                src = rows_buf.at[rb % 2, pl.ds(j * PIECE, PIECE), :]
                wait(src, psem.at[rb % 2, j, 0])
                wait(src, psem.at[rb % 2, j, 1])

        per_layer = groups * blocks
        turn = (layers - 1) * per_layer

        def visit(t, _):
            early = t < turn
            late = t - turn
            l = jnp.where(early, t // per_layer, layers - 1)
            g = jnp.where(early, (t % per_layer) // blocks, late % groups)
            rb = jnp.where(early, t % blocks, late // groups)
            use = jnp.where(early, t // blocks, (layers - 1) * groups + late)
            slot = use % 2
            width = jnp.where(g == 0, lead, GROUP)
            c0 = l * chunks + jnp.where(g == 0, 0, lead + (g - 1) * GROUP)

            @pl.when(jnp.logical_not(early) | (rb == 0))
            def _():
                for j in range(GROUP):

                    @pl.when(j < width)
                    def _():
                        finish(wload(c0 + j, slot, j))

            @pl.when(early)
            def _():
                run(y_stage, y_front(t), y_front(t + 1))
                run(n_stage, n_front(t), n_front(t + 1))
                run(d_stage, d_front(t), d_front(t + 1))

                @pl.when(rb < jnp.where(g == groups - 1, lead, GROUP))
                def _():
                    s_wait(c0 + width + rb)
                    start(wload(c0 + width + rb, 1 - slot, rb))

            @pl.when(t == turn)
            def _():
                run(y_stage, y_front(turn), total)
                run(n_stage, n_front(turn), total)
                run(d_stage, d_front(turn), total)
                run(s_wait, total - chunks + lead, total)

            @pl.when(jnp.logical_not(early) & (late < per_layer - 1))
            def _():
                wrap = g == groups - 1
                n0 = jnp.where(wrap, total - chunks, c0 + width)
                for j in range(GROUP):

                    @pl.when(j < jnp.where(wrap, lead, GROUP))
                    def _():
                        start(wload(n0 + j, 1 - slot, j))

            @pl.when(g == 0)
            def _():
                p[rb] = matmuls(slot, rb, lead)

            @pl.when((g > 0) & (g < groups - 1))
            def _():
                p[rb] = p[rb] + matmuls(slot, rb, GROUP)

            @pl.when(g == groups - 1)
            def _():
                s = p[rb] + matmuls(slot, rb, GROUP)
                h[rb] = (h[rb].astype(jnp.float32) + s).astype(jnp.bfloat16)

            @pl.when(jnp.logical_not(early) & (g == groups - 1))
            def _():
                @pl.when(rb >= 2)
                def _():
                    put_wait(rb - 2)

                for j in range(pieces):
                    cols = pl.ds(j * PIECE, PIECE)
                    rows_buf[rb % 2, cols, :] = h[rb, :, cols].T
                    if j >= 1:
                        put(rb, j - 1)
                put(rb, pieces - 1)

            return 0

        lax.fori_loop(0, layers * per_layer, visit, 0)
        for rb in range(max(blocks - 2, 0), blocks):
            put_wait(rb)
        for i in range(blocks * pieces):
            wait(out.at[piece_rows(flip_tp, i // pieces, i % pieces)], osem.at[i])
        for l in range(layers):
            for i in range(5):
                if i == 4:
                    wait(wbuf.at[pl.ds(l * chunks, chunks), :, :, 0], ss.at[i, l])
                else:
                    n = n_mod(l, i - 1) if i >= 2 else chunks
                    wait(wbuf.at[pl.ds(l * chunks, n), :, 0, 0, 0], ss.at[i, l])


def finish_kernel(up, dn, rows, new_up, new_dn, out, buf, zbuf, lsem, ssem, zsem):
    layers = up.shape[0]
    n_rows = rows.shape[0]
    slots, band, hidden = buf.shape
    side = lax.axis_index("side")
    items = [(i, o, l) for l in range(layers) for i, o in ((up, new_up), (dn, new_dn))]
    piece = zbuf.shape[1]
    n_pieces = n_rows // piece
    n_slots = zbuf.shape[0]

    def pipeline(n, n_slots, load, store):
        for i in range(min(n_slots, n)):
            load(i).start()
        half = n_slots // 2
        for i in range(n):
            load(i).wait()
            store(i).start()
            nxt = i + half
            if i >= half and nxt < n:
                store(nxt - n_slots).wait()
                load(nxt).start()

    @pl.when(side == 0)
    def _():
        zbuf[0] = jnp.zeros(zbuf.shape[1:], zbuf.dtype)
        zeros = [
            pltpu.make_async_copy(zbuf.at[0], out.at[pl.ds(i * piece, piece)], zsem.at[i]) for i in range(n_pieces)
        ]
        for cp in zeros:
            cp.start()

        def load(i):
            src, _, l = items[i]
            return pltpu.make_async_copy(src.at[l], buf.at[i % slots], lsem.at[i % slots])

        def store(i):
            _, dst, l = items[i]
            return pltpu.make_async_copy(buf.at[i % slots], dst.at[l], ssem.at[i % slots])

        n = len(items)
        pipeline(n, slots, load, store)
        for i in range(max(n - slots, 0), n):
            store(i).wait()
        for cp in zeros:
            cp.wait()

    @pl.when(side == 1)
    def _():
        buf[0] = jnp.zeros(buf.shape[1:], buf.dtype)
        zeros = [pltpu.make_async_copy(buf.at[0], dst.at[l], zsem.at[i]) for i, (_, dst, l) in enumerate(items)]
        for cp in zeros:
            cp.start()

        def load(i):
            return pltpu.make_async_copy(rows.at[pl.ds(i * piece, piece)], zbuf.at[i % n_slots], lsem.at[i % n_slots])

        def store(i):
            return pltpu.make_async_copy(zbuf.at[i % n_slots], out.at[pl.ds(i * piece, piece)], ssem.at[i % n_slots])

        pipeline(n_pieces, n_slots, load, store)
        for i in range(max(n_pieces - n_slots, 0), n_pieces):
            store(i).wait()
        for cp in zeros:
            cp.wait()


def solution(mesh):
    up_spec = P("side", None, ("rep", "tp"), None)
    down_spec = P("side", None, None, ("rep", "tp"))
    tok_spec = P("side", "rep", None, None)

    def device_step(w_up, w_down, g_up, g_down, learn_rate, prompts):
        layers, band, hidden = w_up.shape[1:]
        n_rows, d = prompts.shape[2:]
        chunks = hidden // UNIT
        total = layers * chunks
        my_rows = n_rows // 2
        blocks, pieces = my_rows // BLOCK, BLOCK // PIECE
        weights = (w_up[0], jnp.swapaxes(w_down[0], 1, 2), g_up[0], jnp.swapaxes(g_down[0], 1, 2))
        smem = pl.BlockSpec(memory_space=pltpu.SMEM)
        hbm = pl.BlockSpec(memory_space=pl.ANY)
        bf16 = jnp.bfloat16
        relay = jax.ShapeDtypeStruct((blocks * pieces // 2, PIECE, d), bf16)
        new_w = jax.ShapeDtypeStruct((layers, band, hidden), jnp.float32)
        rows = jax.ShapeDtypeStruct((n_rows, d), bf16)
        rows_mid, up_mid, dn_mid, _, _, _ = pl.pallas_call(
            sync_kernel,
            name="sync_and_forward",
            out_shape=(
                rows,
                new_w,
                new_w,
                jax.ShapeDtypeStruct((total, 2, 2, 2, 2, band, UNIT), bf16),
                relay,
                relay,
            ),
            in_specs=[smem] + [hbm] * 5,
            out_specs=(hbm,) * 6,
            scratch_shapes=[
                pltpu.VMEM((blocks, d, BLOCK), bf16),
                pltpu.VMEM((blocks, d, BLOCK), jnp.float32),
                pltpu.VMEM((2, 2, 2, 2, 2, band, GROUP * UNIT), bf16),
                pltpu.VMEM((LOAD_SLOTS, 4, band, UNIT), jnp.float32),
                pltpu.VMEM((LOAD_SLOTS, 2, band, UNIT), jnp.float32),
                pltpu.VMEM((STAGE_SLOTS, 2, band, UNIT), bf16),
                pltpu.VMEM((2, BLOCK, d), bf16),
                pltpu.SemaphoreType.DMA((5, total)),
                pltpu.SemaphoreType.DMA((5, layers)),
                pltpu.SemaphoreType.DMA((LOAD_SLOTS, 4)),
                pltpu.SemaphoreType.DMA((2, GROUP, 2)),
                pltpu.SemaphoreType.DMA((STAGE_SLOTS, 2)),
                pltpu.SemaphoreType.DMA((2,)),
                pltpu.SemaphoreType.DMA((2, pieces, 2)),
                pltpu.SemaphoreType.DMA((blocks * pieces,)),
                pltpu.SemaphoreType.DMA((2, blocks * pieces // 2)),
            ],
            compiler_params=pltpu.CompilerParams(has_side_effects=True, vmem_limit_bytes=60 * 1024 * 1024),
        )(learn_rate, *weights, prompts[0, 0])
        new_up, new_dn, gen_out = pl.pallas_call(
            finish_kernel,
            name="write_outputs",
            out_shape=(new_w, new_w, rows),
            in_specs=[hbm] * 3,
            out_specs=(hbm,) * 3,
            scratch_shapes=[
                pltpu.VMEM((8, band, hidden), jnp.float32),
                pltpu.VMEM((8, n_rows // 16, d), bf16),
                pltpu.SemaphoreType.DMA((8,)),
                pltpu.SemaphoreType.DMA((8,)),
                pltpu.SemaphoreType.DMA((max(16, 2 * layers),)),
            ],
            compiler_params=pltpu.CompilerParams(vmem_limit_bytes=62 * 1024 * 1024),
        )(up_mid, dn_mid, rows_mid)
        return new_up[None], jnp.swapaxes(new_dn, 1, 2)[None], gen_out[None, None]

    return jax.shard_map(
        device_step,
        mesh=mesh,
        in_specs=(up_spec, down_spec, up_spec, down_spec, P("side"), tok_spec),
        out_specs=(up_spec, down_spec, tok_spec),
        check_vma=False,
    )
```

```python
import jax
import jax.numpy as jnp
from jax import lax
from jax.experimental import pallas as pl
from jax.experimental.pallas import tpu as pltpu
from jax.sharding import PartitionSpec as P

MESH = pl.DeviceIdType.MESH
UNIT = 256
GROUP = 5
BLOCK = 512
PIECE = 128
EARLY = 2
LOAD_SLOTS = 4
STAGE_SLOTS = 12
RELAY_LAG = 4
FIRST_LATE = 2
RELAY_BLOCK = 6
FRONTS = ((10, 15, 7, 44), (8, 14, 2, 48), (6, 13, 3, 56))
GELU_A = 0.7978845608028654
GELU_B = 0.7978845608028654 * 0.044715


def gelu(a):
    return a * (0.5 * jnp.tanh(a * (GELU_A + GELU_B * (a * a))) + 0.5)


def sync_kernel(
    rate_ref, w_up, w_dn, g_up, g_dn, prompts, out, nu, nd, wbuf, rin, rx,
    h, p, wv, fin, fnew, stage, rows_buf,
    rs, ss, lsem, fsem, tss, csem, iosem, psem, osem, rsem, hs, hr,
):
    layers, band, hidden = w_up.shape
    chunks = hidden // UNIT
    groups = -(-chunks // GROUP)
    lead = chunks - (groups - 1) * GROUP
    mid = EARLY * chunks
    gen = 2 * mid
    n_rows, d = out.shape
    my_rows = n_rows // 2
    blocks = my_rows // BLOCK
    pieces = BLOCK // PIECE

    tp = lax.axis_index("tp")
    side = lax.axis_index("side")
    rep = lax.axis_index("rep")
    x, k = rep // 2, rep % 2
    flip_tp = 1 - tp
    flip_rep = (1 - x) * 2 + k
    sib_rep = x * 2 + (1 - k)

    own, znb, xnb, dia = (x, tp), (x, flip_tp), (1 - x, tp), (1 - x, flip_tp)

    def both(c, b):
        return wbuf.at[c, :, b[0], k, b[1]]

    def core_half(c, core):
        return wbuf.at[c, :, :, core]

    def chunk_of(e):
        return e + jnp.where(e >= mid, mid, 0)

    def relayed(e):
        return e % 5 == 4

    Y, Z, X, DG, SB = range(5)

    def send(src, dst, ssem, rsem_, t, s, r):
        pltpu.make_async_remote_copy(
            src_ref=src, dst_ref=dst, send_sem=ssem, recv_sem=rsem_,
            device_id={"tp": t, "side": s, "rep": r}, device_id_type=MESH,
        ).start()

    def wait(ref, sem):
        pltpu.make_async_copy(ref, ref, sem).wait()

    def start(cps):
        for cp in cps:
            cp.start()

    def finish(cps):
        for cp in cps:
            cp.wait()

    def run(fn, lo, hi):
        def body(c, _):
            fn(c)
            return 0

        lax.fori_loop(lo, hi, body, 0)

    def piece_rows(t, b, j):
        return pl.ds(pl.multiple_of(t * my_rows + b * BLOCK + j * PIECE, PIECE), PIECE)

    def s_wait(c):
        wait(core_half(c, 1 - k), rs.at[SB, c])

    def wload(c, slot, j):
        cols = pl.ds(j * UNIT if isinstance(j, int) else pl.multiple_of(j * UNIT, UNIT), UNIT)
        return [
            pltpu.make_async_copy(wbuf.at[c, m], wv.at[slot, m, :, :, :, :, cols], fsem.at[slot, j, m])
            for m in range(2)
        ]

    def each_chunk(c0, width, fn):
        for j in range(GROUP):

            @pl.when(j < width)
            def _():
                fn(c0 + j, j)

    def width_of(g):
        return jnp.where(g == 0, lead, GROUP)

    def first_of(l, g):
        return l * chunks + jnp.where(g == 0, 0, lead + (g - 1) * GROUP)

    def matmuls(slot, hb, width):
        def weight(m):
            return wv[slot, m, :, :, :, :, : width * UNIT].reshape(d, width * UNIT)

        a = lax.dot_general(weight(0), h[hb], (((0,), (0,)), ((), ())), preferred_element_type=jnp.float32)
        u = gelu(a).astype(jnp.bfloat16)
        return jnp.dot(weight(1), u, preferred_element_type=jnp.float32)

    def group_part(slot, g, hb, pb):
        @pl.when(g == 0)
        def _():
            p[pb] = matmuls(slot, hb, lead)

        @pl.when((g > 0) & (g < groups - 1))
        def _():
            p[pb] = p[pb] + matmuls(slot, hb, GROUP)

        @pl.when(g == groups - 1)
        def _():
            s = p[pb] + matmuls(slot, hb, GROUP)
            h[hb] = (h[hb].astype(jnp.float32) + s).astype(jnp.bfloat16)

    @pl.when(side == 0)
    def _():
        rate = rate_ref[0]
        parts = ((w_up, g_up, nu), (w_dn, g_dn, nd))
        steps = gen + mid

        def chunk_at(s):
            return jnp.where(s % 3 == 2, mid + s // 3, chunk_of(2 * (s // 3) + s % 3))

        def cols_of(c):
            return c // chunks, pl.ds(pl.multiple_of((c % chunks) * UNIT, UNIT), UNIT)

        def loads(s):
            l, cols = cols_of(chunk_at(s))
            slot = s % LOAD_SLOTS
            return [
                pltpu.make_async_copy(r.at[l, :, cols], fin.at[slot, 2 * m + i], lsem.at[slot, 2 * m + i])
                for m in range(2)
                for i, r in enumerate(parts[m][:2])
            ]

        def stores(s):
            l, cols = cols_of(chunk_at(s))
            slot = s % LOAD_SLOTS
            return [
                pltpu.make_async_copy(fnew.at[slot, m], parts[m][2].at[l, :, cols], fsem.at[slot // 2, slot % 2, m])
                for m in range(2)
            ]

        def own_copy(s):
            slot = s % STAGE_SLOTS
            return pltpu.make_async_copy(stage.at[slot], both(mid + s // 3, own), csem.at[slot])

        def post(s):
            slot = s % STAGE_SLOTS
            src = stage.at[slot]
            start(stores(s))

            @pl.when(s % 3 != 2)
            def _():
                e = 2 * (s // 3) + s % 3
                c = chunk_of(e)
                send(src, both(c, own), tss.at[slot, 0], rs.at[Y, c], tp, 1, rep)

                @pl.when(relayed(e))
                def _():
                    send(src, both(c, own), tss.at[slot, 1], rs.at[DG, c], flip_tp, 0, flip_rep)

                @pl.when(e >= RELAY_LAG)
                def _():
                    relay(e - RELAY_LAG)

            @pl.when(s % 3 == 2)
            def _():
                c = mid + s // 3
                own_copy(s).start()
                send(src, both(c, own), tss.at[slot, 0], rs.at[Z, c], flip_tp, 0, rep)
                send(src, both(c, own), tss.at[slot, 1], rs.at[X, c], tp, 0, flip_rep)

        def relay(e):
            @pl.when(relayed(e))
            def _():
                c = chunk_of(e)
                wait(both(c, dia), rs.at[DG, c])
                send(both(c, dia), both(c, dia), ss.at[0, e // chunks], rs.at[DG, c], tp, 1, rep)

        def wait_sent(s):
            slot = s % STAGE_SLOTS
            is_mid = s % 3 == 2
            wait(stage.at[slot], tss.at[slot, 0])

            @pl.when(is_mid | relayed(2 * (s // 3) + s % 3))
            def _():
                wait(stage.at[slot], tss.at[slot, 1])

            @pl.when(is_mid)
            def _():
                own_copy(s).wait()

        def n_stage(f):
            c = mid + f
            wait(both(c, znb), rs.at[Z, c])
            wait(both(c, xnb), rs.at[X, c])

            @pl.when(f % 2 == 0)
            def _():
                send(both(c, znb), both(c, znb), ss.at[2, f // chunks], rs.at[DG, c], tp, 0, flip_rep)

            @pl.when(f % 2 == 1)
            def _():
                send(both(c, xnb), both(c, xnb), ss.at[3, f // chunks], rs.at[DG, c], flip_tp, 0, rep)

        def d_stage(f):
            c = mid + f
            wait(both(c, dia), rs.at[DG, c])
            send(core_half(c, k), core_half(c, k), ss.at[4, f // chunks], rs.at[SB, c], tp, 0, sib_rep)

        for s in range(LOAD_SLOTS - 1):
            start(loads(s))

        def body(s, _):
            @pl.when(s + LOAD_SLOTS - 1 < steps)
            def _():
                start(loads(s + LOAD_SLOTS - 1))

            finish(loads(s))
            slot, lslot = s % STAGE_SLOTS, s % LOAD_SLOTS

            @pl.when(s >= STAGE_SLOTS)
            def _():
                wait_sent(s - STAGE_SLOTS)

            @pl.when(s >= LOAD_SLOTS)
            def _():
                finish(stores(s - LOAD_SLOTS))

            for m in range(2):
                new = fin[lslot, 2 * m] - rate * fin[lslot, 2 * m + 1]
                fnew[lslot, m] = new
                stage[slot, m] = new.astype(jnp.bfloat16)

            @pl.when(s >= 1)
            def _():
                post(s - 1)

            @pl.when(s % 3 == 2)
            def _():
                f = s // 3

                @pl.when(f >= 1)
                def _():
                    n_stage(f - 1)

                @pl.when(f >= 4)
                def _():
                    d_stage(f - 4)

            return 0

        lax.fori_loop(0, steps, body, 0)
        post(steps - 1)
        run(relay, gen - RELAY_LAG, gen)
        n_stage(mid - 1)
        run(wait_sent, steps - STAGE_SLOTS, steps)
        run(d_stage, mid - 4, mid)
        for s in range(steps - LOAD_SLOTS, steps):
            finish(stores(s))
        run(s_wait, mid, 2 * mid)

        def load_group(c, j, slot):
            start(wload(c, slot, j))

        each_chunk(mid, lead, lambda c, j: load_group(c, j, 0))
        per_block = EARLY * groups

        def give_back(b):
            send(h.at[b], h.at[blocks + b], hs.at[b], hr.at[b], tp, 1, rep)

        def visit(t, _):
            b, q = t // per_block, t % per_block
            g, slot = q % groups, q % 2
            each_chunk(0, width_of(g), lambda c, j: finish(wload(c, slot, j)))

            @pl.when(t + 1 < blocks * per_block)
            def _():
                nq = (t + 1) % per_block
                ng = nq % groups
                each_chunk(
                    first_of(EARLY + nq // groups, ng), width_of(ng), lambda c, j: load_group(c, j, 1 - slot)
                )

            @pl.when(q == 0)
            def _():
                @pl.when(b > 0)
                def _():
                    give_back(b - 1)

                wait(h.at[b], hr.at[b])

            group_part(slot, g, b, 0)
            return 0

        lax.fori_loop(0, blocks * per_block, visit, 0)
        run(lambda b: wait(h.at[b], hs.at[b]), 0, blocks - 2)
        give_back(blocks - 1)

        def relay_out(i, _):
            @pl.when(i < pieces)
            def _():
                wait(rin.at[i], rsem.at[0, i])
                send(rin.at[i], rx.at[i], tss.at[0, 0], rsem.at[1, i], flip_tp, 0, rep)

            @pl.when(i >= 1)
            def _():
                q = i - 1
                wait(rx.at[q], rsem.at[1, q])
                send(rx.at[q], out.at[piece_rows(flip_tp, RELAY_BLOCK, q)], tss.at[1, 0],
                     osem.at[RELAY_BLOCK * pieces + q], tp, 1, rep)

            return 0

        lax.fori_loop(0, pieces + 1, relay_out, 0)
        wait(rin, tss.at[0, 0])
        wait(rx, tss.at[1, 0])
        run(lambda b: wait(h.at[b], hs.at[b]), blocks - 2, blocks)
        for l in range(2 * EARLY):
            n = sum(1 for e in range(l * chunks, (l + 1) * chunks) if e % 5 == 4)
            if n:
                wait(wbuf.at[pl.ds(0, n), :, 0, 0, 0], ss.at[0, l])
        for l in range(EARLY):
            for m in range(2):
                n = sum(1 for f in range(l * chunks, (l + 1) * chunks) if f % 2 == m)
                wait(wbuf.at[pl.ds(0, n), :, 0, 0, 0], ss.at[2 + m, l])
            wait(wbuf.at[pl.ds(0, chunks), :, :, 0], ss.at[4, l])

    @pl.when(side == 1)
    def _():
        def y_stage(e):
            c, l = chunk_of(e), e // chunks
            wait(both(c, own), rs.at[Y, c])
            send(both(c, own), both(c, own), ss.at[0, l], rs.at[Z, c], flip_tp, 1, rep)
            send(both(c, own), both(c, own), ss.at[1, l], rs.at[X, c], tp, 1, flip_rep)

        def n_stage(e):
            c, l = chunk_of(e), e // chunks
            wait(both(c, znb), rs.at[Z, c])
            wait(both(c, xnb), rs.at[X, c])
            r = e % 5

            @pl.when((r == 0) | (r == 2))
            def _():
                send(both(c, znb), both(c, znb), ss.at[2, l], rs.at[DG, c], tp, 1, flip_rep)

            @pl.when((r == 1) | (r == 3))
            def _():
                send(both(c, xnb), both(c, xnb), ss.at[3, l], rs.at[DG, c], flip_tp, 1, rep)

        def d_stage(e):
            c = chunk_of(e)
            wait(both(c, dia), rs.at[DG, c])
            send(core_half(c, k), core_half(c, k), ss.at[4, e // chunks], rs.at[SB, c], tp, 1, sib_rep)

        turn = EARLY * groups * blocks

        def front(i, t):
            a, s1, jump, s2 = FRONTS[i]
            late = jump + (s1 * turn) // 16 + (s2 * (t - turn)) // 16
            return jnp.minimum(gen, a + jnp.where(t <= turn, (s1 * t) // 16, late))

        def pload(b):
            rows = pl.ds(pl.multiple_of(tp * my_rows + b * BLOCK, BLOCK), BLOCK)
            return pltpu.make_async_copy(prompts.at[rows], rows_buf.at[b % 2], iosem.at[b % 2])

        pload(0).start()
        for b in range(blocks):
            if b + 1 < blocks:
                pload(b + 1).start()
            pload(b).wait()
            for j in range(pieces):
                h[b, :, pl.ds(j * PIECE, PIECE)] = rows_buf[b % 2, pl.ds(j * PIECE, PIECE), :].T

        n_pro = FRONTS[0][0]
        for e in range(n_pro):
            y_stage(e)
            for i, fn in ((1, n_stage), (2, d_stage)):
                if e >= n_pro - FRONTS[i][0]:
                    fn(e - (n_pro - FRONTS[i][0]))
            j = e - (n_pro - lead)
            if j >= 0:
                s_wait(j)
                start(wload(j, 0, j))

        def put(b, j):
            src = rows_buf.at[b % 2, pl.ds(j * PIECE, PIECE), :]
            rows = piece_rows(tp, b, j)
            pltpu.make_async_copy(src, out.at[rows], psem.at[b % 2, j, 0]).start()

            @pl.when(b == RELAY_BLOCK)
            def _():
                send(src, rin.at[j], psem.at[b % 2, j, 1], rsem.at[0, j], tp, 0, rep)

            @pl.when(b != RELAY_BLOCK)
            def _():
                send(src, out.at[rows], psem.at[b % 2, j, 1], osem.at[b * pieces + j], flip_tp, 1, rep)

        def put_wait(b):
            for j in range(pieces):
                src = rows_buf.at[b % 2, pl.ds(j * PIECE, PIECE), :]
                wait(src, psem.at[b % 2, j, 0])
                wait(src, psem.at[b % 2, j, 1])

        wide = turn - (groups // 2) * blocks
        n_late = EARLY * groups * blocks
        paired = FIRST_LATE + 2 * (blocks - FIRST_LATE)
        first_late, last_late = 2 * EARLY, 2 * EARLY + 1

        def late_task(q):
            j = (q - FIRST_LATE) // 2
            in_pairs = (q >= FIRST_LATE) & (q < paired)
            last = jnp.where(in_pairs, (q - FIRST_LATE) % 2 == 0, q >= paired)
            b = jnp.where(in_pairs, jnp.where(last, j, j + FIRST_LATE), jnp.where(q < FIRST_LATE, q, q - blocks))
            return jnp.where(last, last_late, first_late), b

        def give(b):
            send(h.at[b], h.at[b], hs.at[b], hr.at[b], tp, 0, rep)

        def visit(t, _):
            late = t >= turn
            split = (t >= wide) & (t < turn)
            tl, tb = late_task((t - turn) // groups)
            per_layer = groups * blocks
            l = jnp.where(late, tl, jnp.where(split, EARLY - 1, t // per_layer))
            half = groups // 2
            g = jnp.where(late, t % groups, jnp.where(split, half + (t - wide) % half, (t // blocks) % groups))
            b = jnp.where(late, tb, jnp.where(split, (t - wide) // half, t % blocks))
            slot = g % 2
            hb = jnp.where(late, blocks + b, b)
            width = width_of(g)

            @pl.when(late | (b == 0))
            def _():
                each_chunk(0, width, lambda c, j: finish(wload(c, slot, j)))

            @pl.when(t < turn + FIRST_LATE * groups)
            def _():
                for i, fn in enumerate((y_stage, n_stage, d_stage)):
                    run(fn, front(i, t), front(i, t + 1))

            @pl.when((t > wide) & (t <= turn) & (g % half == 0))
            def _():
                give((t - wide) // half - 1)

            @pl.when(t < wide)
            def _():
                @pl.when(b < jnp.where(g == groups - 1, lead, GROUP))
                def _():
                    c = first_of(l, g) + width + b
                    s_wait(c)
                    start(wload(c, 1 - slot, b))

            @pl.when(t == turn - 1)
            def _():
                run(lambda e: s_wait(chunk_of(e)), mid, mid + chunks)

            @pl.when(t == turn + FIRST_LATE * groups - 1)
            def _():
                for i, fn in enumerate((y_stage, n_stage, d_stage)):
                    run(fn, front(i, t + 1), gen)
                run(lambda e: s_wait(chunk_of(e)), mid + chunks, gen)

            @pl.when((t == wide) | ((t >= turn - 1) & (t + 1 < turn + n_late)))
            def _():
                ntl, _ = late_task((t + 1 - turn) // groups)
                nl = jnp.where(t == wide, EARLY - 1, ntl)
                ng = jnp.where(t == wide, groups - 1, (t + 1) % groups)

                def fetch(c, j):
                    @pl.when(t == wide)
                    def _():
                        s_wait(c)

                    start(wload(c, 1 - slot, j))

                each_chunk(first_of(nl, ng), width_of(ng), fetch)

            @pl.when(late & (l == first_late) & (g == 0))
            def _():
                wait(h.at[hb], hr.at[b])

            group_part(slot, g, hb, b)

            @pl.when((l == last_late) & (g == groups - 1))
            def _():
                @pl.when(b >= 2)
                def _():
                    put_wait(b - 2)

                for j in range(pieces):
                    cols = pl.ds(j * PIECE, PIECE)
                    rows_buf[b % 2, cols, :] = h[hb, :, cols].T
                    if j >= 1:
                        put(b, j - 1)
                put(b, pieces - 1)

            return 0

        lax.fori_loop(0, turn + n_late, visit, 0)
        for b in range(blocks - 2, blocks):
            put_wait(b)
        run(lambda b: wait(h.at[b], hs.at[b]), 0, blocks)
        for i in range(blocks * pieces):
            wait(out.at[piece_rows(flip_tp, i // pieces, i % pieces)], osem.at[i])
        for l in range(2 * EARLY):
            for i in range(5):
                if i == 4:
                    wait(wbuf.at[pl.ds(0, chunks), :, :, 0], ss.at[i, l])
                else:
                    es = range(l * chunks, (l + 1) * chunks)
                    n = sum(1 for e in es if i < 2 or e % 5 in ((0, 2), (1, 3))[i - 2])
                    wait(wbuf.at[pl.ds(0, n), :, 0, 0, 0], ss.at[i, l])


def finish_kernel(up, dn, rows, new_up, new_dn, out, buf, zbuf, lsem, ssem, zsem):
    layers = up.shape[0]
    n_rows = rows.shape[0]
    slots, band, hidden = buf.shape
    side = lax.axis_index("side")
    items = [(i, o, l) for l in range(layers) for i, o in ((up, new_up), (dn, new_dn))]
    piece = zbuf.shape[1]
    n_pieces = n_rows // piece
    n_slots = zbuf.shape[0]

    def pipeline(n, n_slots, load, store):
        for i in range(min(n_slots, n)):
            load(i).start()
        half = n_slots // 2
        for i in range(n):
            load(i).wait()
            store(i).start()
            nxt = i + half
            if i >= half and nxt < n:
                store(nxt - n_slots).wait()
                load(nxt).start()

    @pl.when(side == 0)
    def _():
        zbuf[0] = jnp.zeros(zbuf.shape[1:], zbuf.dtype)
        zeros = [
            pltpu.make_async_copy(zbuf.at[0], out.at[pl.ds(i * piece, piece)], zsem.at[i]) for i in range(n_pieces)
        ]
        for cp in zeros:
            cp.start()

        def load(i):
            src, _, l = items[i]
            return pltpu.make_async_copy(src.at[l], buf.at[i % slots], lsem.at[i % slots])

        def store(i):
            _, dst, l = items[i]
            return pltpu.make_async_copy(buf.at[i % slots], dst.at[l], ssem.at[i % slots])

        n = len(items)
        pipeline(n, slots, load, store)
        for i in range(max(n - slots, 0), n):
            store(i).wait()
        for cp in zeros:
            cp.wait()

    @pl.when(side == 1)
    def _():
        buf[0] = jnp.zeros(buf.shape[1:], buf.dtype)
        zeros = [pltpu.make_async_copy(buf.at[0], dst.at[l], zsem.at[i]) for i, (_, dst, l) in enumerate(items)]
        for cp in zeros:
            cp.start()

        def load(i):
            return pltpu.make_async_copy(rows.at[pl.ds(i * piece, piece)], zbuf.at[i % n_slots], lsem.at[i % n_slots])

        def store(i):
            return pltpu.make_async_copy(zbuf.at[i % n_slots], out.at[pl.ds(i * piece, piece)], ssem.at[i % n_slots])

        pipeline(n_pieces, n_slots, load, store)
        for i in range(max(n_pieces - n_slots, 0), n_pieces):
            store(i).wait()
        for cp in zeros:
            cp.wait()


def solution(mesh):
    up_spec = P("side", None, ("rep", "tp"), None)
    down_spec = P("side", None, None, ("rep", "tp"))
    tok_spec = P("side", "rep", None, None)

    def device_step(w_up, w_down, g_up, g_down, learn_rate, prompts):
        layers, band, hidden = w_up.shape[1:]
        n_rows, d = prompts.shape[2:]
        chunks = hidden // UNIT
        total = layers * chunks
        my_rows = n_rows // 2
        blocks, pieces = my_rows // BLOCK, BLOCK // PIECE
        weights = (w_up[0], jnp.swapaxes(w_down[0], 1, 2), g_up[0], jnp.swapaxes(g_down[0], 1, 2))
        smem = pl.BlockSpec(memory_space=pltpu.SMEM)
        hbm = pl.BlockSpec(memory_space=pl.ANY)
        bf16 = jnp.bfloat16
        relay = jax.ShapeDtypeStruct((pieces, PIECE, d), bf16)
        new_w = jax.ShapeDtypeStruct((layers, band, hidden), jnp.float32)
        rows = jax.ShapeDtypeStruct((n_rows, d), bf16)
        rows_mid, up_mid, dn_mid, _, _, _ = pl.pallas_call(
            sync_kernel,
            name="sync_and_forward",
            out_shape=(
                rows,
                new_w,
                new_w,
                jax.ShapeDtypeStruct((total, 2, 2, 2, 2, band, UNIT), bf16),
                relay,
                relay,
            ),
            in_specs=[smem] + [hbm] * 5,
            out_specs=(hbm,) * 6,
            scratch_shapes=[
                pltpu.VMEM((2 * blocks, d, BLOCK), bf16),
                pltpu.VMEM((blocks, d, BLOCK), jnp.float32),
                pltpu.VMEM((2, 2, 2, 2, 2, band, GROUP * UNIT), bf16),
                pltpu.VMEM((LOAD_SLOTS, 4, band, UNIT), jnp.float32),
                pltpu.VMEM((LOAD_SLOTS, 2, band, UNIT), jnp.float32),
                pltpu.VMEM((STAGE_SLOTS, 2, band, UNIT), bf16),
                pltpu.VMEM((2, BLOCK, d), bf16),
                pltpu.SemaphoreType.DMA((5, total)),
                pltpu.SemaphoreType.DMA((5, 2 * EARLY)),
                pltpu.SemaphoreType.DMA((LOAD_SLOTS, 4)),
                pltpu.SemaphoreType.DMA((2, GROUP, 2)),
                pltpu.SemaphoreType.DMA((STAGE_SLOTS, 2)),
                pltpu.SemaphoreType.DMA((STAGE_SLOTS,)),
                pltpu.SemaphoreType.DMA((2,)),
                pltpu.SemaphoreType.DMA((2, pieces, 2)),
                pltpu.SemaphoreType.DMA((blocks * pieces,)),
                pltpu.SemaphoreType.DMA((2, pieces)),
                pltpu.SemaphoreType.DMA((blocks,)),
                pltpu.SemaphoreType.DMA((blocks,)),
            ],
            compiler_params=pltpu.CompilerParams(has_side_effects=True, vmem_limit_bytes=60 * 1024 * 1024),
        )(learn_rate, *weights, prompts[0, 0])
        new_up, new_dn, gen_out = pl.pallas_call(
            finish_kernel,
            name="write_outputs",
            out_shape=(new_w, new_w, rows),
            in_specs=[hbm] * 3,
            out_specs=(hbm,) * 3,
            scratch_shapes=[
                pltpu.VMEM((8, band, hidden), jnp.float32),
                pltpu.VMEM((8, n_rows // 16, d), bf16),
                pltpu.SemaphoreType.DMA((8,)),
                pltpu.SemaphoreType.DMA((8,)),
                pltpu.SemaphoreType.DMA((max(16, 2 * layers),)),
            ],
            compiler_params=pltpu.CompilerParams(vmem_limit_bytes=62 * 1024 * 1024),
        )(up_mid, dn_mid, rows_mid)
        return new_up[None], jnp.swapaxes(new_dn, 1, 2)[None], gen_out[None, None]

    return jax.shard_map(
        device_step,
        mesh=mesh,
        in_specs=(up_spec, down_spec, up_spec, down_spec, P("side"), tok_spec),
        out_specs=(up_spec, down_spec, tok_spec),
        check_vma=False,
    )
```

```python
import jax
import jax.numpy as jnp
from jax import lax
from jax.experimental import pallas as pl
from jax.experimental.pallas import tpu as pltpu
from jax.sharding import PartitionSpec as P

MESH = pl.DeviceIdType.MESH
SC = jax.named_scope
UNIT = 256
GROUP = 5
BLOCK = 512
PIECE = 128
EARLY = 2
LOAD_SLOTS = 4
STAGE_SLOTS = 36
N_LAG, D_LAG = 3, 6
RELAY_LAG = 4
FIRST_LATE = 2
RELAY_BLOCK, RELAY_PIECES = 6, 3
FRONTS = ((10, 15, 7, 44), (8, 14, 2, 48), (6, 13, 3, 56))
GELU_A = 0.7978845608028654
GELU_B = 0.7978845608028654 * 0.044715


def gelu(a):
    return a * (0.5 * jnp.tanh(a * (GELU_A + GELU_B * (a * a))) + 0.5)


def sync_kernel(
    rate_ref, w_up, w_dn, g_up, g_dn, prompts, out, nu, nd, wbuf, rin, rx,
    h, p, wv, fin, fnew, stage, rows_buf,
    rs, ss, lsem, fsem, tss, csem, iosem, psem, osem, rsem, hs, hr,
):
    layers, band, hidden = w_up.shape
    chunks = hidden // UNIT
    groups = -(-chunks // GROUP)
    lead = chunks - (groups - 1) * GROUP
    mid = EARLY * chunks
    gen = 2 * mid
    n_rows, d = out.shape
    my_rows = n_rows // 2
    blocks = my_rows // BLOCK
    pieces = BLOCK // PIECE

    tp = lax.axis_index("tp")
    side = lax.axis_index("side")
    rep = lax.axis_index("rep")
    x, k = rep // 2, rep % 2
    flip_tp = 1 - tp
    flip_rep = (1 - x) * 2 + k
    sib_rep = x * 2 + (1 - k)

    own, znb, xnb, dia = (x, tp), (x, flip_tp), (1 - x, tp), (1 - x, flip_tp)

    def both(c, b):
        return wbuf.at[c, :, b[0], k, b[1]]

    def core_half(c, core):
        return wbuf.at[c, :, :, core]

    def chunk_of(e):
        return e + jnp.where(e >= mid, mid, 0)

    def relayed(e):
        return e % 5 == 4

    Y, Z, X, DG, SB = range(5)

    def send(src, dst, ssem, rsem_, t, s, r):
        pltpu.make_async_remote_copy(
            src_ref=src, dst_ref=dst, send_sem=ssem, recv_sem=rsem_,
            device_id={"tp": t, "side": s, "rep": r}, device_id_type=MESH,
        ).start()

    def wait(ref, sem):
        pltpu.make_async_copy(ref, ref, sem).wait()

    def start(cps):
        for cp in cps:
            cp.start()

    def finish(cps):
        for cp in cps:
            cp.wait()

    def run(fn, lo, hi):
        def body(c, _):
            fn(c)
            return 0

        lax.fori_loop(lo, hi, body, 0)

    def piece_rows(t, b, j):
        return pl.ds(pl.multiple_of(t * my_rows + b * BLOCK + j * PIECE, PIECE), PIECE)

    def s_wait(c):
        wait(core_half(c, 1 - k), rs.at[SB, c])

    def wload(c, slot, j):
        cols = pl.ds(j * UNIT if isinstance(j, int) else pl.multiple_of(j * UNIT, UNIT), UNIT)
        return [
            pltpu.make_async_copy(wbuf.at[c, m], wv.at[slot, m, :, :, :, :, cols], fsem.at[slot, j, m])
            for m in range(2)
        ]

    def each_chunk(c0, width, fn):
        for j in range(GROUP):

            @pl.when(j < width)
            def _():
                fn(c0 + j, j)

    def width_of(g):
        return jnp.where(g == 0, lead, GROUP)

    def first_of(l, g):
        return l * chunks + jnp.where(g == 0, 0, lead + (g - 1) * GROUP)

    def matmuls(slot, hb, width):
        def weight(m):
            return wv[slot, m, :, :, :, :, : width * UNIT].reshape(d, width * UNIT)

        a = lax.dot_general(weight(0), h[hb], (((0,), (0,)), ((), ())), preferred_element_type=jnp.float32)
        u = gelu(a).astype(jnp.bfloat16)
        return jnp.dot(weight(1), u, preferred_element_type=jnp.float32)

    def group_part(slot, g, hb, pb):
        @pl.when(g == 0)
        def _():
            p[pb] = matmuls(slot, hb, lead)

        @pl.when((g > 0) & (g < groups - 1))
        def _():
            p[pb] = p[pb] + matmuls(slot, hb, GROUP)

        @pl.when(g == groups - 1)
        def _():
            s = p[pb] + matmuls(slot, hb, GROUP)
            h[hb] = (h[hb].astype(jnp.float32) + s).astype(jnp.bfloat16)

    @pl.when(side == 0)
    def _():
        rate = rate_ref[0]
        parts = ((w_up, g_up, nu), (w_dn, g_dn, nd))
        steps = gen + mid

        def chunk_at(s):
            return jnp.where(s % 3 == 2, mid + s // 3, chunk_of(2 * (s // 3) + s % 3))

        def cols_of(c):
            return c // chunks, pl.ds(pl.multiple_of((c % chunks) * UNIT, UNIT), UNIT)

        def loads(s):
            l, cols = cols_of(chunk_at(s))
            slot = s % LOAD_SLOTS
            return [
                pltpu.make_async_copy(r.at[l, :, cols], fin.at[slot, 2 * m + i], lsem.at[slot, 2 * m + i])
                for m in range(2)
                for i, r in enumerate(parts[m][:2])
            ]

        def stores(s):
            l, cols = cols_of(chunk_at(s))
            slot = s % LOAD_SLOTS
            return [
                pltpu.make_async_copy(fnew.at[slot, m], parts[m][2].at[l, :, cols], fsem.at[slot // 2, slot % 2, m])
                for m in range(2)
            ]

        def own_copy(s):
            slot = s % STAGE_SLOTS
            return pltpu.make_async_copy(stage.at[slot], both(mid + s // 3, own), csem.at[slot])

        def post(s):
            slot = s % STAGE_SLOTS
            src = stage.at[slot]
            start(stores(s))

            @pl.when(s % 3 != 2)
            def _():
                e = 2 * (s // 3) + s % 3
                c = chunk_of(e)
                send(src, both(c, own), tss.at[slot, 0], rs.at[Y, c], tp, 1, rep)

                @pl.when(relayed(e))
                def _():
                    send(src, both(c, own), tss.at[slot, 1], rs.at[DG, c], flip_tp, 0, flip_rep)

                @pl.when(e >= RELAY_LAG)
                def _():
                    relay(e - RELAY_LAG)

            @pl.when(s % 3 == 2)
            def _():
                c = mid + s // 3
                own_copy(s).start()
                send(src, both(c, own), tss.at[slot, 0], rs.at[Z, c], flip_tp, 0, rep)
                send(src, both(c, own), tss.at[slot, 1], rs.at[X, c], tp, 0, flip_rep)

        def relay(e):
            @pl.when(relayed(e))
            def _():
                c = chunk_of(e)
                wait(both(c, dia), rs.at[DG, c])
                send(both(c, dia), both(c, dia), ss.at[0, e // chunks], rs.at[DG, c], tp, 1, rep)

        def wait_sent(s):
            slot = s % STAGE_SLOTS
            is_mid = s % 3 == 2
            wait(stage.at[slot], tss.at[slot, 0])

            @pl.when(is_mid | relayed(2 * (s // 3) + s % 3))
            def _():
                wait(stage.at[slot], tss.at[slot, 1])

        def n_stage(f):
            c = mid + f
            wait(both(c, znb), rs.at[Z, c])
            wait(both(c, xnb), rs.at[X, c])

            @pl.when(f % 2 == 0)
            def _():
                send(both(c, znb), both(c, znb), ss.at[2, f // chunks], rs.at[DG, c], tp, 0, flip_rep)

            @pl.when(f % 2 == 1)
            def _():
                send(both(c, xnb), both(c, xnb), ss.at[3, f // chunks], rs.at[DG, c], flip_tp, 0, rep)

        def d_stage(f):
            c = mid + f
            wait(both(c, dia), rs.at[DG, c])
            own_copy(3 * f + 2).wait()
            send(core_half(c, k), core_half(c, k), ss.at[4, f // chunks], rs.at[SB, c], tp, 0, sib_rep)

        for s in range(LOAD_SLOTS - 1):
            start(loads(s))

        def body(s, _):
            @pl.when(s + LOAD_SLOTS - 1 < steps)
            def _():
                start(loads(s + LOAD_SLOTS - 1))

            finish(loads(s))
            slot, lslot = s % STAGE_SLOTS, s % LOAD_SLOTS

            @pl.when(s >= STAGE_SLOTS)
            def _():
                wait_sent(s - STAGE_SLOTS)

            @pl.when(s >= LOAD_SLOTS)
            def _():
                finish(stores(s - LOAD_SLOTS))

            for m in range(2):
                new = fin[lslot, 2 * m] - rate * fin[lslot, 2 * m + 1]
                fnew[lslot, m] = new
                stage[slot, m] = new.astype(jnp.bfloat16)

            @pl.when(s >= 1)
            def _():
                post(s - 1)

            @pl.when(s % 3 == 2)
            def _():
                f = s // 3

                @pl.when(f >= N_LAG)
                def _():
                    n_stage(f - N_LAG)

                @pl.when(f >= D_LAG)
                def _():
                    d_stage(f - D_LAG)

            return 0

        with SC("t_cast"):
            lax.fori_loop(0, steps, body, 0)
        post(steps - 1)
        run(relay, gen - RELAY_LAG, gen)
        run(n_stage, mid - N_LAG, mid)
        run(d_stage, mid - D_LAG, mid)
        for s in range(steps - LOAD_SLOTS, steps):
            finish(stores(s))
        with SC("t_sw"):
            run(s_wait, mid, 2 * mid)

        def load_group(c, j, slot):
            start(wload(c, slot, j))

        each_chunk(mid, lead, lambda c, j: load_group(c, j, 0))
        per_block = EARLY * groups

        def give_back(b):
            send(h.at[b], h.at[blocks + b], hs.at[b], hr.at[b], tp, 1, rep)

        def visit(t, _):
            b, q = t // per_block, t % per_block
            g, slot = q % groups, q % 2
            with SC("t_ld"):
                each_chunk(0, width_of(g), lambda c, j: finish(wload(c, slot, j)))

            @pl.when(t + 1 < blocks * per_block)
            def _():
                nq = (t + 1) % per_block
                ng = nq % groups
                each_chunk(
                    first_of(EARLY + nq // groups, ng), width_of(ng), lambda c, j: load_group(c, j, 1 - slot)
                )

            @pl.when(q == 0)
            def _():
                @pl.when(b > 0)
                def _():
                    give_back(b - 1)

                with SC("t_hw"):
                    wait(h.at[b], hr.at[b])

            with SC("t_mm"):
                group_part(slot, g, b, 0)
            return 0

        lax.fori_loop(0, blocks * per_block, visit, 0)
        run(lambda b: wait(h.at[b], hs.at[b]), 0, blocks - 2)
        give_back(blocks - 1)

        def relay_out(i, _):
            @pl.when(i < RELAY_PIECES)
            def _():
                wait(rin.at[i], rsem.at[0, i])
                send(rin.at[i], rx.at[i], psem.at[0, 0, 0], rsem.at[1, i], flip_tp, 0, rep)

            @pl.when(i >= 1)
            def _():
                q = i - 1
                wait(rx.at[q], rsem.at[1, q])
                send(rx.at[q], out.at[piece_rows(flip_tp, RELAY_BLOCK, q)], psem.at[0, 0, 1],
                     osem.at[RELAY_BLOCK * pieces + q], tp, 1, rep)

            return 0

        lax.fori_loop(0, RELAY_PIECES + 1, relay_out, 0)
        wait(rin.at[pl.ds(0, RELAY_PIECES)], psem.at[0, 0, 0])
        wait(rx.at[pl.ds(0, RELAY_PIECES)], psem.at[0, 0, 1])
        run(wait_sent, steps - STAGE_SLOTS, steps)
        run(lambda b: wait(h.at[b], hs.at[b]), blocks - 2, blocks)
        for l in range(2 * EARLY):
            n = sum(1 for e in range(l * chunks, (l + 1) * chunks) if e % 5 == 4)
            if n:
                wait(wbuf.at[pl.ds(0, n), :, 0, 0, 0], ss.at[0, l])
        for l in range(EARLY):
            for m in range(2):
                n = sum(1 for f in range(l * chunks, (l + 1) * chunks) if f % 2 == m)
                wait(wbuf.at[pl.ds(0, n), :, 0, 0, 0], ss.at[2 + m, l])
            wait(wbuf.at[pl.ds(0, chunks), :, :, 0], ss.at[4, l])

    @pl.when(side == 1)
    def _():
        def y_stage(e):
            c, l = chunk_of(e), e // chunks
            wait(both(c, own), rs.at[Y, c])
            send(both(c, own), both(c, own), ss.at[0, l], rs.at[Z, c], flip_tp, 1, rep)
            send(both(c, own), both(c, own), ss.at[1, l], rs.at[X, c], tp, 1, flip_rep)

        def n_stage(e):
            c, l = chunk_of(e), e // chunks
            wait(both(c, znb), rs.at[Z, c])
            wait(both(c, xnb), rs.at[X, c])
            r = e % 5

            @pl.when((r == 0) | (r == 2))
            def _():
                send(both(c, znb), both(c, znb), ss.at[2, l], rs.at[DG, c], tp, 1, flip_rep)

            @pl.when((r == 1) | (r == 3))
            def _():
                send(both(c, xnb), both(c, xnb), ss.at[3, l], rs.at[DG, c], flip_tp, 1, rep)

        def d_stage(e):
            c = chunk_of(e)
            wait(both(c, dia), rs.at[DG, c])
            send(core_half(c, k), core_half(c, k), ss.at[4, e // chunks], rs.at[SB, c], tp, 1, sib_rep)

        turn = EARLY * groups * blocks

        def front(i, t):
            a, s1, jump, s2 = FRONTS[i]
            late = jump + (s1 * turn) // 16 + (s2 * (t - turn)) // 16
            return jnp.minimum(gen, a + jnp.where(t <= turn, (s1 * t) // 16, late))

        def pload(b):
            rows = pl.ds(pl.multiple_of(tp * my_rows + b * BLOCK, BLOCK), BLOCK)
            return pltpu.make_async_copy(prompts.at[rows], rows_buf.at[b % 2], iosem.at[b % 2])

        pload(0).start()
        for b in range(blocks):
            if b + 1 < blocks:
                pload(b + 1).start()
            pload(b).wait()
            for j in range(pieces):
                h[b, :, pl.ds(j * PIECE, PIECE)] = rows_buf[b % 2, pl.ds(j * PIECE, PIECE), :].T

        n_pro = FRONTS[0][0]
        for e in range(n_pro):
            with SC(f"pro{e}"):
                y_stage(e)
            for i, fn in ((1, n_stage), (2, d_stage)):
                if e >= n_pro - FRONTS[i][0]:
                    fn(e - (n_pro - FRONTS[i][0]))
            j = e - (n_pro - lead)
            if j >= 0:
                s_wait(j)
                start(wload(j, 0, j))

        def put(b, j):
            src = rows_buf.at[b % 2, pl.ds(j * PIECE, PIECE), :]
            rows = piece_rows(tp, b, j)
            pltpu.make_async_copy(src, out.at[rows], psem.at[b % 2, j, 0]).start()

            by_relay = (b == RELAY_BLOCK) & (j < RELAY_PIECES)

            @pl.when(by_relay)
            def _():
                send(src, rin.at[j], psem.at[b % 2, j, 1], rsem.at[0, j], tp, 0, rep)

            @pl.when(jnp.logical_not(by_relay))
            def _():
                send(src, out.at[rows], psem.at[b % 2, j, 1], osem.at[b * pieces + j], flip_tp, 1, rep)

        def put_wait(b):
            for j in range(pieces):
                src = rows_buf.at[b % 2, pl.ds(j * PIECE, PIECE), :]
                wait(src, psem.at[b % 2, j, 0])
                wait(src, psem.at[b % 2, j, 1])

        wide = turn - (groups // 2) * blocks
        n_late = EARLY * groups * blocks
        paired = FIRST_LATE + 2 * (blocks - FIRST_LATE)
        first_late, last_late = 2 * EARLY, 2 * EARLY + 1

        def late_task(q):
            j = (q - FIRST_LATE) // 2
            in_pairs = (q >= FIRST_LATE) & (q < paired)
            last = jnp.where(in_pairs, (q - FIRST_LATE) % 2 == 0, q >= paired)
            b = jnp.where(in_pairs, jnp.where(last, j, j + FIRST_LATE), jnp.where(q < FIRST_LATE, q, q - blocks))
            return jnp.where(last, last_late, first_late), b

        def give(b):
            send(h.at[b], h.at[b], hs.at[b], hr.at[b], tp, 0, rep)

        def visit(t, _):
            late = t >= turn
            split = (t >= wide) & (t < turn)
            tl, tb = late_task((t - turn) // groups)
            per_layer = groups * blocks
            l = jnp.where(late, tl, jnp.where(split, EARLY - 1, t // per_layer))
            half = groups // 2
            g = jnp.where(late, t % groups, jnp.where(split, half + (t - wide) % half, (t // blocks) % groups))
            b = jnp.where(late, tb, jnp.where(split, (t - wide) // half, t % blocks))
            slot = g % 2
            hb = jnp.where(late, blocks + b, b)
            width = width_of(g)

            @pl.when(late | (b == 0))
            def _():
                with SC("ld"):
                    each_chunk(0, width, lambda c, j: finish(wload(c, slot, j)))

            @pl.when(t < turn + FIRST_LATE * groups)
            def _():
                for i, fn in enumerate((y_stage, n_stage, d_stage)):
                    with SC("fw" + "ynd"[i]):
                        run(fn, front(i, t), front(i, t + 1))

            @pl.when((t > wide) & (t <= turn) & (g % half == 0))
            def _():
                give((t - wide) // half - 1)

            @pl.when(t < wide)
            def _():
                @pl.when(b < jnp.where(g == groups - 1, lead, GROUP))
                def _():
                    c = first_of(l, g) + width + b
                    with SC("sw"):
                        s_wait(c)
                    start(wload(c, 1 - slot, b))

            @pl.when(t == turn - 1)
            def _():
              with SC("sw4"):
                run(lambda e: s_wait(chunk_of(e)), mid, mid + chunks)

            @pl.when(t == turn + FIRST_LATE * groups - 1)
            def _():
              with SC("sw5"):
                for i, fn in enumerate((y_stage, n_stage, d_stage)):
                    run(fn, front(i, t + 1), gen)
                run(lambda e: s_wait(chunk_of(e)), mid + chunks, gen)

            @pl.when((t == wide) | ((t >= turn - 1) & (t + 1 < turn + n_late)))
            def _():
                ntl, _ = late_task((t + 1 - turn) // groups)
                nl = jnp.where(t == wide, EARLY - 1, ntl)
                ng = jnp.where(t == wide, groups - 1, (t + 1) % groups)

                def fetch(c, j):
                    @pl.when(t == wide)
                    def _():
                        s_wait(c)

                    start(wload(c, 1 - slot, j))

                each_chunk(first_of(nl, ng), width_of(ng), fetch)

            @pl.when(late & (l == first_late) & (g == 0))
            def _():
                with SC("hw"):
                    wait(h.at[hb], hr.at[b])

            with SC("mm"):
                group_part(slot, g, hb, b)

            @pl.when((l == last_late) & (g == groups - 1))
            def _():
              with SC("out"):
                pass
                @pl.when(b >= 2)
                def _():
                    put_wait(b - 2)

                for j in range(pieces):
                    cols = pl.ds(j * PIECE, PIECE)
                    rows_buf[b % 2, cols, :] = h[hb, :, cols].T
                    if j >= 1:
                        put(b, j - 1)
                put(b, pieces - 1)

            return 0

        lax.fori_loop(0, turn + n_late, visit, 0)
        with SC("tail_s"):
          for b in range(blocks - 2, blocks):
            put_wait(b)
        run(lambda b: wait(h.at[b], hs.at[b]), 0, blocks)
        with SC("tail_r"):
          for i in range(blocks * pieces):
            wait(out.at[piece_rows(flip_tp, i // pieces, i % pieces)], osem.at[i])
        for l in range(2 * EARLY):
            for i in range(5):
                if i == 4:
                    wait(wbuf.at[pl.ds(0, chunks), :, :, 0], ss.at[i, l])
                else:
                    es = range(l * chunks, (l + 1) * chunks)
                    n = sum(1 for e in es if i < 2 or e % 5 in ((0, 2), (1, 3))[i - 2])
                    wait(wbuf.at[pl.ds(0, n), :, 0, 0, 0], ss.at[i, l])


def finish_kernel(up, dn, rows, new_up, new_dn, out, buf, zbuf, lsem, ssem, zsem):
    layers = up.shape[0]
    n_rows = rows.shape[0]
    slots, band, hidden = buf.shape
    side = lax.axis_index("side")
    items = [(i, o, l) for l in range(layers) for i, o in ((up, new_up), (dn, new_dn))]
    piece = zbuf.shape[1]
    n_pieces = n_rows // piece
    n_slots = zbuf.shape[0]

    def pipeline(n, n_slots, load, store):
        for i in range(min(n_slots, n)):
            load(i).start()
        half = n_slots // 2
        for i in range(n):
            load(i).wait()
            store(i).start()
            nxt = i + half
            if i >= half and nxt < n:
                store(nxt - n_slots).wait()
                load(nxt).start()

    @pl.when(side == 0)
    def _():
        zbuf[0] = jnp.zeros(zbuf.shape[1:], zbuf.dtype)
        zeros = [
            pltpu.make_async_copy(zbuf.at[0], out.at[pl.ds(i * piece, piece)], zsem.at[i]) for i in range(n_pieces)
        ]
        for cp in zeros:
            cp.start()

        def load(i):
            src, _, l = items[i]
            return pltpu.make_async_copy(src.at[l], buf.at[i % slots], lsem.at[i % slots])

        def store(i):
            _, dst, l = items[i]
            return pltpu.make_async_copy(buf.at[i % slots], dst.at[l], ssem.at[i % slots])

        n = len(items)
        pipeline(n, slots, load, store)
        for i in range(max(n - slots, 0), n):
            store(i).wait()
        for cp in zeros:
            cp.wait()

    @pl.when(side == 1)
    def _():
        buf[0] = jnp.zeros(buf.shape[1:], buf.dtype)
        zeros = [pltpu.make_async_copy(buf.at[0], dst.at[l], zsem.at[i]) for i, (_, dst, l) in enumerate(items)]
        for cp in zeros:
            cp.start()

        def load(i):
            return pltpu.make_async_copy(rows.at[pl.ds(i * piece, piece)], zbuf.at[i % n_slots], lsem.at[i % n_slots])

        def store(i):
            return pltpu.make_async_copy(zbuf.at[i % n_slots], out.at[pl.ds(i * piece, piece)], ssem.at[i % n_slots])

        pipeline(n_pieces, n_slots, load, store)
        for i in range(max(n_pieces - n_slots, 0), n_pieces):
            store(i).wait()
        for cp in zeros:
            cp.wait()


def solution(mesh):
    up_spec = P("side", None, ("rep", "tp"), None)
    down_spec = P("side", None, None, ("rep", "tp"))
    tok_spec = P("side", "rep", None, None)

    def device_step(w_up, w_down, g_up, g_down, learn_rate, prompts):
        layers, band, hidden = w_up.shape[1:]
        n_rows, d = prompts.shape[2:]
        chunks = hidden // UNIT
        total = layers * chunks
        my_rows = n_rows // 2
        blocks, pieces = my_rows // BLOCK, BLOCK // PIECE
        weights = (w_up[0], jnp.swapaxes(w_down[0], 1, 2), g_up[0], jnp.swapaxes(g_down[0], 1, 2))
        smem = pl.BlockSpec(memory_space=pltpu.SMEM)
        hbm = pl.BlockSpec(memory_space=pl.ANY)
        bf16 = jnp.bfloat16
        relay = jax.ShapeDtypeStruct((pieces, PIECE, d), bf16)
        new_w = jax.ShapeDtypeStruct((layers, band, hidden), jnp.float32)
        rows = jax.ShapeDtypeStruct((n_rows, d), bf16)
        rows_mid, up_mid, dn_mid, _, _, _ = pl.pallas_call(
            sync_kernel,
            name="sync_and_forward",
            out_shape=(
                rows,
                new_w,
                new_w,
                jax.ShapeDtypeStruct((total, 2, 2, 2, 2, band, UNIT), bf16),
                relay,
                relay,
            ),
            in_specs=[smem] + [hbm] * 5,
            out_specs=(hbm,) * 6,
            scratch_shapes=[
                pltpu.VMEM((2 * blocks, d, BLOCK), bf16),
                pltpu.VMEM((blocks, d, BLOCK), jnp.float32),
                pltpu.VMEM((2, 2, 2, 2, 2, band, GROUP * UNIT), bf16),
                pltpu.VMEM((LOAD_SLOTS, 4, band, UNIT), jnp.float32),
                pltpu.VMEM((LOAD_SLOTS, 2, band, UNIT), jnp.float32),
                pltpu.VMEM((STAGE_SLOTS, 2, band, UNIT), bf16),
                pltpu.VMEM((2, BLOCK, d), bf16),
                pltpu.SemaphoreType.DMA((5, total)),
                pltpu.SemaphoreType.DMA((5, 2 * EARLY)),
                pltpu.SemaphoreType.DMA((LOAD_SLOTS, 4)),
                pltpu.SemaphoreType.DMA((2, GROUP, 2)),
                pltpu.SemaphoreType.DMA((STAGE_SLOTS, 2)),
                pltpu.SemaphoreType.DMA((STAGE_SLOTS,)),
                pltpu.SemaphoreType.DMA((2,)),
                pltpu.SemaphoreType.DMA((2, pieces, 2)),
                pltpu.SemaphoreType.DMA((blocks * pieces,)),
                pltpu.SemaphoreType.DMA((2, pieces)),
                pltpu.SemaphoreType.DMA((blocks,)),
                pltpu.SemaphoreType.DMA((blocks,)),
            ],
            compiler_params=pltpu.CompilerParams(has_side_effects=True, vmem_limit_bytes=60 * 1024 * 1024),
        )(learn_rate, *weights, prompts[0, 0])
        new_up, new_dn, gen_out = pl.pallas_call(
            finish_kernel,
            name="write_outputs",
            out_shape=(new_w, new_w, rows),
            in_specs=[hbm] * 3,
            out_specs=(hbm,) * 3,
            scratch_shapes=[
                pltpu.VMEM((8, band, hidden), jnp.float32),
                pltpu.VMEM((8, n_rows // 16, d), bf16),
                pltpu.SemaphoreType.DMA((8,)),
                pltpu.SemaphoreType.DMA((8,)),
                pltpu.SemaphoreType.DMA((max(16, 2 * layers),)),
            ],
            compiler_params=pltpu.CompilerParams(vmem_limit_bytes=62 * 1024 * 1024),
        )(up_mid, dn_mid, rows_mid)
        return new_up[None], jnp.swapaxes(new_dn, 1, 2)[None], gen_out[None, None]

    return jax.shard_map(
        device_step,
        mesh=mesh,
        in_specs=(up_spec, down_spec, up_spec, down_spec, P("side"), tok_spec),
        out_specs=(up_spec, down_spec, tok_spec),
        check_vma=False,
    )
```

```python
import jax
import jax.numpy as jnp
from jax import lax
from jax.experimental import pallas as pl
from jax.experimental.pallas import tpu as pltpu
from jax.sharding import PartitionSpec as P

MESH = pl.DeviceIdType.MESH
SC = jax.named_scope
UNIT = 256
GROUP = 5
BLOCK = 512
PIECE = 128
EARLY = 2
LOAD_SLOTS = 4
STAGE_SLOTS = 36
N_LAG, D_LAG = 3, 6
RELAY_LAG = 4
FIRST_LATE = 3
MORE = 2
RELAYED = ((4, 2), (5, 2), (6, 3), (7, 1))
FRONTS = ((10, 15, 1, 40), (8, 14, 1, 44), (6, 13, 3, 24))
GELU_A = 0.7978845608028654
GELU_B = 0.7978845608028654 * 0.044715


def gelu(a):
    return a * (0.5 * jnp.tanh(a * (GELU_A + GELU_B * (a * a))) + 0.5)


def sync_kernel(
    rate_ref, w_up, w_dn, g_up, g_dn, prompts, out, nu, nd, wbuf, rin, rx,
    h, p, wv, fin, fnew, stage, rows_buf,
    rs, ss, lsem, fsem, tss, csem, iosem, psem, osem, rsem, hs, hr,
):
    layers, band, hidden = w_up.shape
    chunks = hidden // UNIT
    n_relay = sum(n for _, n in RELAYED)
    groups = -(-chunks // GROUP)
    lead = chunks - (groups - 1) * GROUP
    mid = EARLY * chunks
    gen = 2 * mid
    n_rows, d = out.shape
    my_rows = n_rows // 2
    blocks = my_rows // BLOCK
    pieces = BLOCK // PIECE

    tp = lax.axis_index("tp")
    side = lax.axis_index("side")
    rep = lax.axis_index("rep")
    x, k = rep // 2, rep % 2
    flip_tp = 1 - tp
    flip_rep = (1 - x) * 2 + k
    sib_rep = x * 2 + (1 - k)

    own, znb, xnb, dia = (x, tp), (x, flip_tp), (1 - x, tp), (1 - x, flip_tp)

    def both(c, b):
        return wbuf.at[c, :, b[0], k, b[1]]

    def core_half(c, core):
        return wbuf.at[c, :, :, core]

    def chunk_of(e):
        return e + jnp.where(e >= mid, mid, 0)

    def relayed(e):
        return ((e % 6 == 5) & (e < mid)) | ((e % 3 == 2) & (e >= mid + chunks))

    def by_z(e):
        return (((e // 6 + e % 6) % 2 == 1) & (e < mid + chunks)) | ((e % 3 == 1) & (e >= mid + chunks))

    def count(e0, e1, fn):
        return sum(1 for e in range(e0, e1) if fn(e))

    Y, Z, X, DG, SB = range(5)

    def send(src, dst, ssem, rsem_, t, s, r):
        pltpu.make_async_remote_copy(
            src_ref=src, dst_ref=dst, send_sem=ssem, recv_sem=rsem_,
            device_id={"tp": t, "side": s, "rep": r}, device_id_type=MESH,
        ).start()

    def wait(ref, sem):
        pltpu.make_async_copy(ref, ref, sem).wait()

    def start(cps):
        for cp in cps:
            cp.start()

    def finish(cps):
        for cp in cps:
            cp.wait()

    def run(fn, lo, hi):
        def body(c, _):
            fn(c)
            return 0

        lax.fori_loop(lo, hi, body, 0)

    def piece_rows(t, b, j):
        return pl.ds(pl.multiple_of(t * my_rows + b * BLOCK + j * PIECE, PIECE), PIECE)

    def s_wait(c):
        wait(core_half(c, 1 - k), rs.at[SB, c])

    def wload(c, slot, j):
        cols = pl.ds(j * UNIT if isinstance(j, int) else pl.multiple_of(j * UNIT, UNIT), UNIT)
        return [
            pltpu.make_async_copy(wbuf.at[c, m], wv.at[slot, m, :, :, :, :, cols], fsem.at[slot, j, m])
            for m in range(2)
        ]

    def each_chunk(c0, width, fn):
        for j in range(GROUP):

            @pl.when(j < width)
            def _():
                fn(c0 + j, j)

    def width_of(g):
        return jnp.where(g == 0, lead, GROUP)

    def first_of(l, g):
        return l * chunks + jnp.where(g == 0, 0, lead + (g - 1) * GROUP)

    def matmuls(slot, hb, width):
        def weight(m):
            return wv[slot, m, :, :, :, :, : width * UNIT].reshape(d, width * UNIT)

        a = lax.dot_general(weight(0), h[hb], (((0,), (0,)), ((), ())), preferred_element_type=jnp.float32)
        u = gelu(a).astype(jnp.bfloat16)
        return jnp.dot(weight(1), u, preferred_element_type=jnp.float32)

    def group_part(slot, g, hb, pb):
        @pl.when(g == 0)
        def _():
            p[pb] = matmuls(slot, hb, lead)

        @pl.when((g > 0) & (g < groups - 1))
        def _():
            p[pb] = p[pb] + matmuls(slot, hb, GROUP)

        @pl.when(g == groups - 1)
        def _():
            s = p[pb] + matmuls(slot, hb, GROUP)
            h[hb] = (h[hb].astype(jnp.float32) + s).astype(jnp.bfloat16)

    @pl.when(side == 0)
    def _():
        rate = rate_ref[0]
        parts = ((w_up, g_up, nu), (w_dn, g_dn, nd))
        steps = gen + mid

        def chunk_at(s):
            return jnp.where(s % 3 == 2, mid + s // 3, chunk_of(2 * (s // 3) + s % 3))

        def cols_of(c):
            return c // chunks, pl.ds(pl.multiple_of((c % chunks) * UNIT, UNIT), UNIT)

        def loads(s):
            l, cols = cols_of(chunk_at(s))
            slot = s % LOAD_SLOTS
            return [
                pltpu.make_async_copy(r.at[l, :, cols], fin.at[slot, 2 * m + i], lsem.at[slot, 2 * m + i])
                for m in range(2)
                for i, r in enumerate(parts[m][:2])
            ]

        def stores(s):
            l, cols = cols_of(chunk_at(s))
            slot = s % LOAD_SLOTS
            return [
                pltpu.make_async_copy(fnew.at[slot, m], parts[m][2].at[l, :, cols], fsem.at[slot // 2, slot % 2, m])
                for m in range(2)
            ]

        def own_copy(s):
            slot = s % STAGE_SLOTS
            return pltpu.make_async_copy(stage.at[slot], both(chunk_at(s), own), csem.at[slot])

        def gathered_too(s):
            e = 2 * (s // 3) + s % 3
            return (s % 3 != 2) & (e >= mid) & (e < mid + chunks)

        def post(s):
            slot = s % STAGE_SLOTS
            src = stage.at[slot]
            start(stores(s))

            @pl.when(s % 3 != 2)
            def _():
                e = 2 * (s // 3) + s % 3
                c = chunk_of(e)
                send(src, both(c, own), tss.at[slot, 0], rs.at[Y, c], tp, 1, rep)

                @pl.when(gathered_too(s))
                def _():
                    own_copy(s).start()

                @pl.when(relayed(e))
                def _():
                    send(src, both(c, own), tss.at[slot, 1], rs.at[DG, c], flip_tp, 0, flip_rep)

                @pl.when(e >= RELAY_LAG)
                def _():
                    relay(e - RELAY_LAG)

            @pl.when(s % 3 == 2)
            def _():
                c = mid + s // 3
                own_copy(s).start()
                send(src, both(c, own), tss.at[slot, 0], rs.at[Z, c], flip_tp, 0, rep)
                send(src, both(c, own), tss.at[slot, 1], rs.at[X, c], tp, 0, flip_rep)

        def relay(e):
            @pl.when(relayed(e))
            def _():
                c = chunk_of(e)
                wait(both(c, dia), rs.at[DG, c])
                send(both(c, dia), both(c, dia), ss.at[0, e // chunks], rs.at[DG, c], tp, 1, rep)

        def wait_sent(s):
            slot = s % STAGE_SLOTS
            is_mid = s % 3 == 2
            wait(stage.at[slot], tss.at[slot, 0])

            @pl.when(is_mid | relayed(2 * (s // 3) + s % 3))
            def _():
                wait(stage.at[slot], tss.at[slot, 1])

        def own_stage(f):
            c = mid + f
            send(both(c, own), both(c, own), ss.at[1, 0], rs.at[Z, c], flip_tp, 0, rep)
            send(both(c, own), both(c, own), ss.at[1, 1], rs.at[X, c], tp, 0, flip_rep)

        def n_stage(f):
            c = mid + f
            wait(both(c, znb), rs.at[Z, c])
            wait(both(c, xnb), rs.at[X, c])

            @pl.when(f % 2 == 0)
            def _():
                send(both(c, znb), both(c, znb), ss.at[2, f // chunks], rs.at[DG, c], tp, 0, flip_rep)

            @pl.when(f % 2 == 1)
            def _():
                send(both(c, xnb), both(c, xnb), ss.at[3, f // chunks], rs.at[DG, c], flip_tp, 0, rep)

        def d_stage(f):
            c = mid + f
            wait(both(c, dia), rs.at[DG, c])

            @pl.when(f < mid)
            def _():
                own_copy(3 * f + 2).wait()

            send(core_half(c, k), core_half(c, k), ss.at[4, f // chunks], rs.at[SB, c], tp, 0, sib_rep)

        for s in range(LOAD_SLOTS - 1):
            start(loads(s))

        def body(s, _):
            @pl.when(s + LOAD_SLOTS - 1 < steps)
            def _():
                start(loads(s + LOAD_SLOTS - 1))

            finish(loads(s))
            slot, lslot = s % STAGE_SLOTS, s % LOAD_SLOTS

            @pl.when(s >= STAGE_SLOTS)
            def _():
                wait_sent(s - STAGE_SLOTS)

                @pl.when(gathered_too(s - STAGE_SLOTS))
                def _():
                    own_copy(s - STAGE_SLOTS).wait()

            @pl.when(s >= LOAD_SLOTS)
            def _():
                finish(stores(s - LOAD_SLOTS))

            for m in range(2):
                new = fin[lslot, 2 * m] - rate * fin[lslot, 2 * m + 1]
                fnew[lslot, m] = new
                stage[slot, m] = new.astype(jnp.bfloat16)

            @pl.when(s >= 1)
            def _():
                post(s - 1)

            @pl.when(s % 3 == 2)
            def _():
                f = s // 3

                @pl.when(f >= N_LAG)
                def _():
                    n_stage(f - N_LAG)

                @pl.when(f >= D_LAG)
                def _():
                    d_stage(f - D_LAG)

            return 0

        with SC("t_cast"):
            lax.fori_loop(0, steps, body, 0)
        post(steps - 1)
        run(relay, gen - RELAY_LAG, gen)
        run(n_stage, mid - N_LAG, mid)
        run(d_stage, mid - D_LAG, mid)
        for s in range(steps - LOAD_SLOTS, steps):
            finish(stores(s))
        for s in range(steps - STAGE_SLOTS, steps):
            if s % 3 != 2 and mid <= 2 * (s // 3) + s % 3 < mid + chunks:
                own_copy(s).wait()
        with SC("t_sw"):
            run(s_wait, mid, 2 * mid)

        def load_group(c, j, slot):
            start(wload(c, slot, j))

        each_chunk(mid, lead, lambda c, j: load_group(c, j, 0))
        per_block = EARLY * groups
        few = (blocks - MORE) * per_block
        n_visits = few + MORE * (per_block + groups)

        def place(t):
            u = t - few
            more = jnp.where(u >= per_block + groups, 1, 0)
            b = jnp.where(t < few, t // per_block, blocks - MORE + more)
            return b, jnp.where(t < few, t % per_block, u - more * (per_block + groups))

        def give_back(b):
            send(h.at[b], h.at[blocks + b], hs.at[b], hr.at[b], tp, 1, rep)

        def visit(t, _):
            b, q = place(t)
            g, slot = q % groups, q % 2
            with SC("t_ld"):
                each_chunk(0, width_of(g), lambda c, j: finish(wload(c, slot, j)))

            for fn, after in ((own_stage, 0), (n_stage, 4), (d_stage, 8)):

                @pl.when((t >= after) & (t < after + chunks))
                def _():
                    with SC(f"t_fw{after}"):
                        fn(mid + t - after)

            @pl.when(t == few)
            def _():
                run(s_wait, 2 * mid, 2 * mid + chunks)

            @pl.when(t + 1 < n_visits)
            def _():
                _, nq = place(t + 1)
                ng = nq % groups
                each_chunk(
                    first_of(EARLY + nq // groups, ng), width_of(ng), lambda c, j: load_group(c, j, 1 - slot)
                )

            @pl.when(q == 0)
            def _():
                @pl.when(b > 0)
                def _():
                    give_back(b - 1)

                with SC("t_hw"):
                    wait(h.at[b], hr.at[b])

            with SC("t_mm"):
                group_part(slot, g, b, 0)
            return 0

        lax.fori_loop(0, n_visits, visit, 0)
        run(lambda b: wait(h.at[b], hs.at[b]), 0, blocks - 2)
        give_back(blocks - 1)

        def relay_out(i, _):
            @pl.when(i < n_relay)
            def _():
                wait(rin.at[i], rsem.at[0, i])
                send(rin.at[i], rx.at[i], psem.at[0, 0, 0], rsem.at[1, i], flip_tp, 0, rep)

            @pl.when(i >= 1)
            def _():
                q = i - 1
                wait(rx.at[q], rsem.at[1, q])
                b, j, first = 0, 0, 0
                for rb, n in RELAYED:
                    b = jnp.where(q >= first, rb, b)
                    j = jnp.where(q >= first, q - first, j)
                    first += n
                send(rx.at[q], out.at[piece_rows(flip_tp, b, j)], psem.at[0, 0, 1],
                     osem.at[b * pieces + j], tp, 1, rep)

            return 0

        with SC("t_relay"):
            lax.fori_loop(0, n_relay + 1, relay_out, 0)
        wait(rin, psem.at[0, 0, 0])
        wait(rx, psem.at[0, 0, 1])
        run(wait_sent, steps - STAGE_SLOTS, steps)
        run(lambda b: wait(h.at[b], hs.at[b]), blocks - 2, blocks)
        for l in range(2 * EARLY):
            n = count(l * chunks, (l + 1) * chunks, relayed)
            if n:
                wait(wbuf.at[pl.ds(0, n), :, 0, 0, 0], ss.at[0, l])
        for i in range(2):
            wait(wbuf.at[pl.ds(0, chunks), :, 0, 0, 0], ss.at[1, i])
        for l in range(EARLY + 1):
            for m in range(2):
                n = count(l * chunks, (l + 1) * chunks, lambda f: f % 2 == m)
                wait(wbuf.at[pl.ds(0, n), :, 0, 0, 0], ss.at[2 + m, l])
            wait(wbuf.at[pl.ds(0, chunks), :, :, 0], ss.at[4, l])

    @pl.when(side == 1)
    def _():
        def y_stage(e):
            c, l = chunk_of(e), e // chunks
            wait(both(c, own), rs.at[Y, c])
            send(both(c, own), both(c, own), ss.at[0, l], rs.at[Z, c], flip_tp, 1, rep)
            send(both(c, own), both(c, own), ss.at[1, l], rs.at[X, c], tp, 1, flip_rep)

        def n_stage(e):
            c, l = chunk_of(e), e // chunks
            wait(both(c, znb), rs.at[Z, c])
            wait(both(c, xnb), rs.at[X, c])
            direct = jnp.logical_not(relayed(e))

            @pl.when(direct & jnp.logical_not(by_z(e)))
            def _():
                send(both(c, znb), both(c, znb), ss.at[2, l], rs.at[DG, c], tp, 1, flip_rep)

            @pl.when(direct & by_z(e))
            def _():
                send(both(c, xnb), both(c, xnb), ss.at[3, l], rs.at[DG, c], flip_tp, 1, rep)

        def d_stage(e):
            c = chunk_of(e)
            wait(both(c, dia), rs.at[DG, c])
            send(core_half(c, k), core_half(c, k), ss.at[4, e // chunks], rs.at[SB, c], tp, 1, sib_rep)

        turn = EARLY * groups * blocks

        def front(i, t):
            a, s1, jump, s2 = FRONTS[i]
            late = 16 * jump + s1 * turn + s2 * (t - turn)
            return jnp.minimum(gen, a + (jnp.where(t <= turn, s1 * t, late) >> 4))

        def pload(b):
            rows = pl.ds(pl.multiple_of(tp * my_rows + b * BLOCK, BLOCK), BLOCK)
            return pltpu.make_async_copy(prompts.at[rows], rows_buf.at[b % 2], iosem.at[b % 2])

        pload(0).start()
        for b in range(blocks):
            if b + 1 < blocks:
                pload(b + 1).start()
            pload(b).wait()
            for j in range(pieces):
                h[b, :, pl.ds(j * PIECE, PIECE)] = rows_buf[b % 2, pl.ds(j * PIECE, PIECE), :].T

        n_pro = FRONTS[0][0]
        for e in range(n_pro):
            y_stage(e)
            for i, fn in ((1, n_stage), (2, d_stage)):
                if e >= n_pro - FRONTS[i][0]:
                    fn(e - (n_pro - FRONTS[i][0]))
            j = e - (n_pro - lead)
            if j >= 0:
                s_wait(j)
                start(wload(j, 0, j))

        def put(b, j):
            src = rows_buf.at[b % 2, pl.ds(j * PIECE, PIECE), :]
            rows = piece_rows(tp, b, j)
            pltpu.make_async_copy(src, out.at[rows], psem.at[b % 2, j, 0]).start()
            n, i, first = 0, 0, 0
            for rb, m in RELAYED:
                n = jnp.where(b == rb, m, n)
                i = jnp.where(b == rb, first + min(j, m - 1), i)
                first += m

            @pl.when(j < n)
            def _():
                send(src, rin.at[i], psem.at[b % 2, j, 1], rsem.at[0, i], tp, 0, rep)

            @pl.when(j >= n)
            def _():
                send(src, out.at[rows], psem.at[b % 2, j, 1], osem.at[b * pieces + j], flip_tp, 1, rep)

        def put_wait(b):
            for j in range(pieces):
                src = rows_buf.at[b % 2, pl.ds(j * PIECE, PIECE), :]
                wait(src, psem.at[b % 2, j, 0])
                wait(src, psem.at[b % 2, j, 1])

        n_rest = groups - 1
        wide = turn - n_rest * blocks
        n_first = blocks - MORE
        n_tasks = n_first + blocks
        n_visits = turn + n_tasks * groups
        paired = FIRST_LATE + 2 * (n_first - FIRST_LATE)
        first_late, last_late = 2 * EARLY, 2 * EARLY + 1
        arrived = turn + FIRST_LATE * groups - 1

        def late_task(q):
            u = q - FIRST_LATE
            in_pairs = (q >= FIRST_LATE) & (q < paired)
            last = jnp.where(in_pairs, (u & 1) == 0, q >= paired)
            j = u >> 1
            b = jnp.where(in_pairs, jnp.where(last, j, j + FIRST_LATE), jnp.where(q < FIRST_LATE, q, q - n_first))
            return jnp.where(last, last_late, first_late), b

        def rest(t):
            u = t - wide
            b = (u * (128 // n_rest + 1)) >> 7
            return b, 1 + u - n_rest * b

        def give(b):
            send(h.at[b], h.at[b], hs.at[b], hr.at[b], tp, 0, rep)

        def visit(t, _):
            late = t >= turn
            split = (t >= wide) & (t < turn)
            tl, tb = late_task((t - turn) >> 2)
            rb, rg = rest(t)
            l = jnp.where(late, tl, jnp.where(split, EARLY - 1, t // (groups * blocks)))
            g = jnp.where(late, t % groups, jnp.where(split, rg, (t // blocks) % groups))
            b = jnp.where(late, tb, jnp.where(split, rb, t % blocks))
            slot = jnp.where(t < wide, (t // blocks) % 2, (t - wide + 1) % 2)
            hb = jnp.where(late, blocks + b, b)
            width = width_of(g)

            @pl.when((t >= wide) | (b == 0))
            def _():
                with SC("ld"):
                    each_chunk(0, width, lambda c, j: finish(wload(c, slot, j)))

            @pl.when(t <= arrived)
            def _():
                for i, fn in enumerate((y_stage, n_stage, d_stage)):
                    with SC("fw" + "ynd"[i]):
                        run(fn, front(i, t), front(i, t + 1))

            @pl.when((t > wide) & (t <= turn) & ((rg == 1) | late))
            def _():
                give(rb - 1)

            @pl.when(t < wide)
            def _():
                @pl.when(b < jnp.where(g == groups - 1, lead, GROUP))
                def _():
                    c = first_of(l, g) + width + b
                    with SC("sw"):
                        s_wait(c)
                    start(wload(c, 1 - slot, b))

            @pl.when(t == wide)
            def _():
                with SC("sw1"):
                    run(s_wait, (EARLY - 1) * chunks + lead + GROUP, EARLY * chunks)

            @pl.when(t == turn - 1)
            def _():
                with SC("sw4"):
                    run(lambda e: s_wait(chunk_of(e)), mid, mid + chunks)

            @pl.when(t == arrived)
            def _():
              with SC("sw5"):
                for i, fn in enumerate((y_stage, n_stage, d_stage)):
                    run(fn, front(i, t + 1), gen)
                run(lambda e: s_wait(chunk_of(e)), mid + chunks, gen)

            @pl.when((t >= wide) & (t + 1 < n_visits))
            def _():
                ntl, _ = late_task((t + 1 - turn) >> 2)
                _, nrg = rest(t + 1)
                next_late = t + 1 >= turn
                nl = jnp.where(next_late, ntl, EARLY - 1)
                ng = jnp.where(next_late, (t + 1) % groups, nrg)
                each_chunk(first_of(nl, ng), width_of(ng), lambda c, j: start(wload(c, 1 - slot, j)))

            @pl.when((g == 0) & late & ((l == first_late) | (b >= n_first)))
            def _():
                with SC("hw"):
                    wait(h.at[hb], hr.at[b])

            with SC("mm"):
                group_part(slot, g, hb, b)

            @pl.when((l == last_late) & (g == groups - 1))
            def _():
                @pl.when(b >= 2)
                def _():
                    put_wait(b - 2)

                for j in range(pieces):
                    cols = pl.ds(j * PIECE, PIECE)
                    rows_buf[b % 2, cols, :] = h[hb, :, cols].T
                    if j >= 1:
                        put(b, j - 1)
                put(b, pieces - 1)

            return 0

        lax.fori_loop(0, n_visits, visit, 0)
        with SC("tail_s"):
          for b in range(blocks - 2, blocks):
            put_wait(b)
        run(lambda b: wait(h.at[b], hs.at[b]), 0, blocks)
        with SC("tail_r"):
          for i in range(blocks * pieces):
            wait(out.at[piece_rows(flip_tp, i // pieces, i % pieces)], osem.at[i])
        for l in range(2 * EARLY):
            for i in range(5):
                if i == 4:
                    wait(wbuf.at[pl.ds(0, chunks), :, :, 0], ss.at[i, l])
                else:
                    kinds = (None, None, lambda e: not relayed(e) and not by_z(e), lambda e: not relayed(e) and by_z(e))
                    n = chunks if i < 2 else count(l * chunks, (l + 1) * chunks, kinds[i])
                    wait(wbuf.at[pl.ds(0, n), :, 0, 0, 0], ss.at[i, l])


def finish_kernel(up, dn, rows, new_up, new_dn, out, buf, zbuf, lsem, ssem, zsem):
    layers = up.shape[0]
    n_rows = rows.shape[0]
    slots, band, hidden = buf.shape
    side = lax.axis_index("side")
    items = [(i, o, l) for l in range(layers) for i, o in ((up, new_up), (dn, new_dn))]
    piece = zbuf.shape[1]
    n_pieces = n_rows // piece
    n_slots = zbuf.shape[0]

    def pipeline(n, n_slots, load, store):
        for i in range(min(n_slots, n)):
            load(i).start()
        half = n_slots // 2
        for i in range(n):
            load(i).wait()
            store(i).start()
            nxt = i + half
            if i >= half and nxt < n:
                store(nxt - n_slots).wait()
                load(nxt).start()

    @pl.when(side == 0)
    def _():
        zbuf[0] = jnp.zeros(zbuf.shape[1:], zbuf.dtype)
        zeros = [
            pltpu.make_async_copy(zbuf.at[0], out.at[pl.ds(i * piece, piece)], zsem.at[i]) for i in range(n_pieces)
        ]
        for cp in zeros:
            cp.start()

        def load(i):
            src, _, l = items[i]
            return pltpu.make_async_copy(src.at[l], buf.at[i % slots], lsem.at[i % slots])

        def store(i):
            _, dst, l = items[i]
            return pltpu.make_async_copy(buf.at[i % slots], dst.at[l], ssem.at[i % slots])

        n = len(items)
        pipeline(n, slots, load, store)
        for i in range(max(n - slots, 0), n):
            store(i).wait()
        for cp in zeros:
            cp.wait()

    @pl.when(side == 1)
    def _():
        buf[0] = jnp.zeros(buf.shape[1:], buf.dtype)
        zeros = [pltpu.make_async_copy(buf.at[0], dst.at[l], zsem.at[i]) for i, (_, dst, l) in enumerate(items)]
        for cp in zeros:
            cp.start()

        def load(i):
            return pltpu.make_async_copy(rows.at[pl.ds(i * piece, piece)], zbuf.at[i % n_slots], lsem.at[i % n_slots])

        def store(i):
            return pltpu.make_async_copy(zbuf.at[i % n_slots], out.at[pl.ds(i * piece, piece)], ssem.at[i % n_slots])

        pipeline(n_pieces, n_slots, load, store)
        for i in range(max(n_pieces - n_slots, 0), n_pieces):
            store(i).wait()
        for cp in zeros:
            cp.wait()


def solution(mesh):
    up_spec = P("side", None, ("rep", "tp"), None)
    down_spec = P("side", None, None, ("rep", "tp"))
    tok_spec = P("side", "rep", None, None)

    def device_step(w_up, w_down, g_up, g_down, learn_rate, prompts):
        layers, band, hidden = w_up.shape[1:]
        n_rows, d = prompts.shape[2:]
        chunks = hidden // UNIT
        total = layers * chunks
        my_rows = n_rows // 2
        blocks, pieces = my_rows // BLOCK, BLOCK // PIECE
        weights = (w_up[0], jnp.swapaxes(w_down[0], 1, 2), g_up[0], jnp.swapaxes(g_down[0], 1, 2))
        smem = pl.BlockSpec(memory_space=pltpu.SMEM)
        hbm = pl.BlockSpec(memory_space=pl.ANY)
        bf16 = jnp.bfloat16
        relay = jax.ShapeDtypeStruct((sum(n for _, n in RELAYED), PIECE, d), bf16)
        new_w = jax.ShapeDtypeStruct((layers, band, hidden), jnp.float32)
        rows = jax.ShapeDtypeStruct((n_rows, d), bf16)
        rows_mid, up_mid, dn_mid, _, _, _ = pl.pallas_call(
            sync_kernel,
            name="sync_and_forward",
            out_shape=(
                rows,
                new_w,
                new_w,
                jax.ShapeDtypeStruct((total, 2, 2, 2, 2, band, UNIT), bf16),
                relay,
                relay,
            ),
            in_specs=[smem] + [hbm] * 5,
            out_specs=(hbm,) * 6,
            scratch_shapes=[
                pltpu.VMEM((2 * blocks, d, BLOCK), bf16),
                pltpu.VMEM((blocks, d, BLOCK), jnp.float32),
                pltpu.VMEM((2, 2, 2, 2, 2, band, GROUP * UNIT), bf16),
                pltpu.VMEM((LOAD_SLOTS, 4, band, UNIT), jnp.float32),
                pltpu.VMEM((LOAD_SLOTS, 2, band, UNIT), jnp.float32),
                pltpu.VMEM((STAGE_SLOTS, 2, band, UNIT), bf16),
                pltpu.VMEM((2, BLOCK, d), bf16),
                pltpu.SemaphoreType.DMA((5, total)),
                pltpu.SemaphoreType.DMA((5, 2 * EARLY)),
                pltpu.SemaphoreType.DMA((LOAD_SLOTS, 4)),
                pltpu.SemaphoreType.DMA((2, GROUP, 2)),
                pltpu.SemaphoreType.DMA((STAGE_SLOTS, 2)),
                pltpu.SemaphoreType.DMA((STAGE_SLOTS,)),
                pltpu.SemaphoreType.DMA((2,)),
                pltpu.SemaphoreType.DMA((2, pieces, 2)),
                pltpu.SemaphoreType.DMA((blocks * pieces,)),
                pltpu.SemaphoreType.DMA((2, sum(n for _, n in RELAYED))),
                pltpu.SemaphoreType.DMA((blocks,)),
                pltpu.SemaphoreType.DMA((blocks,)),
            ],
            compiler_params=pltpu.CompilerParams(has_side_effects=True, vmem_limit_bytes=60 * 1024 * 1024),
        )(learn_rate, *weights, prompts[0, 0])
        new_up, new_dn, gen_out = pl.pallas_call(
            finish_kernel,
            name="write_outputs",
            out_shape=(new_w, new_w, rows),
            in_specs=[hbm] * 3,
            out_specs=(hbm,) * 3,
            scratch_shapes=[
                pltpu.VMEM((8, band, hidden), jnp.float32),
                pltpu.VMEM((8, n_rows // 16, d), bf16),
                pltpu.SemaphoreType.DMA((8,)),
                pltpu.SemaphoreType.DMA((8,)),
                pltpu.SemaphoreType.DMA((max(16, 2 * layers),)),
            ],
            compiler_params=pltpu.CompilerParams(vmem_limit_bytes=62 * 1024 * 1024),
        )(up_mid, dn_mid, rows_mid)
        return new_up[None], jnp.swapaxes(new_dn, 1, 2)[None], gen_out[None, None]

    return jax.shard_map(
        device_step,
        mesh=mesh,
        in_specs=(up_spec, down_spec, up_spec, down_spec, P("side"), tok_spec),
        out_specs=(up_spec, down_spec, tok_spec),
        check_vma=False,
    )
```

```python
import jax
import jax.numpy as jnp
from jax import lax
from jax.experimental import pallas as pl
from jax.experimental.pallas import tpu as pltpu
from jax.sharding import PartitionSpec as P

MESH = pl.DeviceIdType.MESH
SC = jax.named_scope
UNIT = 256
GROUP = 5
BLOCK = 512
PIECE = 128
EARLY = 2
LOAD_SLOTS = 4
STAGE_SLOTS = 36
N_LAG, D_LAG = 3, 6
RELAY_LAG = 4
FIRST_LATE = 3
MORE = 2
RELAYED = ((4, 2), (5, 3), (6, 3))
FRONTS = ((10, 15, 1, 40), (8, 14, 1, 44), (6, 13, 3, 24))
GELU_A = 0.7978845608028654
GELU_B = 0.7978845608028654 * 0.044715


def div(a, n):
    if isinstance(a, int):
        return a // n
    if n & (n - 1) == 0:
        return a >> (n.bit_length() - 1)
    return (a * ((1 << 16) // n + 1)) >> 16


def mod(a, n):
    return a - n * div(a, n)


def gelu(a):
    return a * (0.5 * jnp.tanh(a * (GELU_A + GELU_B * (a * a))) + 0.5)


def sync_kernel(
    rate_ref, w_up, w_dn, g_up, g_dn, prompts, out, nu, nd, wbuf, rin, rx,
    h, p, wv, fin, fnew, stage, rows_buf,
    rs, ss, lsem, fsem, tss, csem, iosem, psem, osem, rsem, hs, hr,
):
    layers, band, hidden = w_up.shape
    chunks = hidden // UNIT
    n_relay = sum(n for _, n in RELAYED)
    groups = -(-chunks // GROUP)
    lead = chunks - (groups - 1) * GROUP
    mid = EARLY * chunks
    gen = 2 * mid
    n_rows, d = out.shape
    my_rows = n_rows // 2
    blocks = my_rows // BLOCK
    pieces = BLOCK // PIECE

    tp = lax.axis_index("tp")
    side = lax.axis_index("side")
    rep = lax.axis_index("rep")
    x, k = rep // 2, rep % 2
    flip_tp = 1 - tp
    flip_rep = (1 - x) * 2 + k
    sib_rep = x * 2 + (1 - k)

    own, znb, xnb, dia = (x, tp), (x, flip_tp), (1 - x, tp), (1 - x, flip_tp)

    def both(c, b):
        return wbuf.at[c, :, b[0], k, b[1]]

    def core_half(c, core):
        return wbuf.at[c, :, :, core]

    def chunk_of(e):
        return e + jnp.where(e >= mid, mid, 0)

    def relayed(e):
        return ((mod(e, 6) == 5) & (e < mid)) | ((mod(e, 3) == 2) & (e >= mid + chunks))

    def by_z(e):
        return ((mod(div(e, 6) + mod(e, 6), 2) == 1) & (e < mid + chunks)) | ((mod(e, 3) == 1) & (e >= mid + chunks))

    def count(e0, e1, fn):
        return sum(1 for e in range(e0, e1) if fn(e))

    Y, Z, X, DG, SB = range(5)

    def send(src, dst, ssem, rsem_, t, s, r):
        pltpu.make_async_remote_copy(
            src_ref=src, dst_ref=dst, send_sem=ssem, recv_sem=rsem_,
            device_id={"tp": t, "side": s, "rep": r}, device_id_type=MESH,
        ).start()

    def wait(ref, sem):
        pltpu.make_async_copy(ref, ref, sem).wait()

    def start(cps):
        for cp in cps:
            cp.start()

    def finish(cps):
        for cp in cps:
            cp.wait()

    def run(fn, lo, hi):
        def body(c, _):
            fn(c)
            return 0

        lax.fori_loop(lo, hi, body, 0)

    def piece_rows(t, b, j):
        return pl.ds(pl.multiple_of(t * my_rows + b * BLOCK + j * PIECE, PIECE), PIECE)

    def s_wait(c):
        wait(core_half(c, 1 - k), rs.at[SB, c])

    def wload(c, slot, j):
        cols = pl.ds(j * UNIT if isinstance(j, int) else pl.multiple_of(j * UNIT, UNIT), UNIT)
        return [
            pltpu.make_async_copy(wbuf.at[c, m], wv.at[slot, m, :, :, :, :, cols], fsem.at[slot, j, m])
            for m in range(2)
        ]

    def each_chunk(c0, width, fn):
        for j in range(GROUP):

            @pl.when(j < width)
            def _():
                fn(c0 + j, j)

    def width_of(g):
        return jnp.where(g == 0, lead, GROUP)

    def first_of(l, g):
        return l * chunks + jnp.where(g == 0, 0, lead + (g - 1) * GROUP)

    def matmuls(slot, hb, width):
        def weight(m):
            return wv[slot, m, :, :, :, :, : width * UNIT].reshape(d, width * UNIT)

        a = lax.dot_general(weight(0), h[hb], (((0,), (0,)), ((), ())), preferred_element_type=jnp.float32)
        u = gelu(a).astype(jnp.bfloat16)
        return jnp.dot(weight(1), u, preferred_element_type=jnp.float32)

    def group_part(slot, g, hb, pb):
        @pl.when(g == 0)
        def _():
            p[pb] = matmuls(slot, hb, lead)

        @pl.when((g > 0) & (g < groups - 1))
        def _():
            p[pb] = p[pb] + matmuls(slot, hb, GROUP)

        @pl.when(g == groups - 1)
        def _():
            s = p[pb] + matmuls(slot, hb, GROUP)
            h[hb] = (h[hb].astype(jnp.float32) + s).astype(jnp.bfloat16)

    @pl.when(side == 0)
    def _():
        rate = rate_ref[0]
        parts = ((w_up, g_up, nu), (w_dn, g_dn, nd))
        steps = gen + mid

        def chunk_at(s):
            return jnp.where(mod(s, 3) == 2, mid + div(s, 3), chunk_of(2 * div(s, 3) + mod(s, 3)))

        def cols_of(c):
            return div(c, chunks), pl.ds(pl.multiple_of(mod(c, chunks) * UNIT, UNIT), UNIT)

        def loads(s):
            l, cols = cols_of(chunk_at(s))
            slot = s % LOAD_SLOTS
            return [
                pltpu.make_async_copy(r.at[l, :, cols], fin.at[slot, 2 * m + i], lsem.at[slot, 2 * m + i])
                for m in range(2)
                for i, r in enumerate(parts[m][:2])
            ]

        def stores(s):
            l, cols = cols_of(chunk_at(s))
            slot = s % LOAD_SLOTS
            return [
                pltpu.make_async_copy(fnew.at[slot, m], parts[m][2].at[l, :, cols], fsem.at[slot // 2, slot % 2, m])
                for m in range(2)
            ]

        def own_copy(s):
            slot = s % STAGE_SLOTS
            return pltpu.make_async_copy(stage.at[slot], both(chunk_at(s), own), csem.at[slot])

        def gathered_too(s):
            e = 2 * (s // 3) + s % 3
            return (s % 3 != 2) & (e >= mid) & (e < mid + chunks)

        def post(s):
            slot = s % STAGE_SLOTS
            src = stage.at[slot]
            start(stores(s))

            @pl.when(s % 3 != 2)
            def _():
                e = 2 * (s // 3) + s % 3
                c = chunk_of(e)
                send(src, both(c, own), tss.at[slot, 0], rs.at[Y, c], tp, 1, rep)

                @pl.when(gathered_too(s))
                def _():
                    own_copy(s).start()

                @pl.when(relayed(e))
                def _():
                    send(src, both(c, own), tss.at[slot, 1], rs.at[DG, c], flip_tp, 0, flip_rep)

                @pl.when(e >= RELAY_LAG)
                def _():
                    relay(e - RELAY_LAG)

            @pl.when(s % 3 == 2)
            def _():
                c = mid + s // 3
                own_copy(s).start()
                send(src, both(c, own), tss.at[slot, 0], rs.at[Z, c], flip_tp, 0, rep)
                send(src, both(c, own), tss.at[slot, 1], rs.at[X, c], tp, 0, flip_rep)

        def relay(e):
            @pl.when(relayed(e))
            def _():
                c = chunk_of(e)
                wait(both(c, dia), rs.at[DG, c])
                send(both(c, dia), both(c, dia), ss.at[0, e // chunks], rs.at[DG, c], tp, 1, rep)

        def wait_sent(s):
            slot = s % STAGE_SLOTS
            is_mid = s % 3 == 2
            wait(stage.at[slot], tss.at[slot, 0])

            @pl.when(is_mid | relayed(2 * (s // 3) + s % 3))
            def _():
                wait(stage.at[slot], tss.at[slot, 1])

        def own_stage(f):
            c = mid + f
            send(both(c, own), both(c, own), ss.at[1, 0], rs.at[Z, c], flip_tp, 0, rep)
            send(both(c, own), both(c, own), ss.at[1, 1], rs.at[X, c], tp, 0, flip_rep)

        def n_stage(f):
            c = mid + f
            wait(both(c, znb), rs.at[Z, c])
            wait(both(c, xnb), rs.at[X, c])

            @pl.when(mod(f, 2) == 0)
            def _():
                send(both(c, znb), both(c, znb), ss.at[2, div(f, chunks)], rs.at[DG, c], tp, 0, flip_rep)

            @pl.when(mod(f, 2) == 1)
            def _():
                send(both(c, xnb), both(c, xnb), ss.at[3, div(f, chunks)], rs.at[DG, c], flip_tp, 0, rep)

        def d_stage(f):
            c = mid + f
            wait(both(c, dia), rs.at[DG, c])

            @pl.when(f < mid)
            def _():
                own_copy(3 * f + 2).wait()

            send(core_half(c, k), core_half(c, k), ss.at[4, div(f, chunks)], rs.at[SB, c], tp, 0, sib_rep)

        for s in range(LOAD_SLOTS - 1):
            start(loads(s))

        def body(s, _):
            @pl.when(s + LOAD_SLOTS - 1 < steps)
            def _():
                start(loads(s + LOAD_SLOTS - 1))

            finish(loads(s))
            slot, lslot = s % STAGE_SLOTS, s % LOAD_SLOTS

            @pl.when(s >= STAGE_SLOTS)
            def _():
                wait_sent(s - STAGE_SLOTS)

                @pl.when(gathered_too(s - STAGE_SLOTS))
                def _():
                    own_copy(s - STAGE_SLOTS).wait()

            @pl.when(s >= LOAD_SLOTS)
            def _():
                finish(stores(s - LOAD_SLOTS))

            for m in range(2):
                new = fin[lslot, 2 * m] - rate * fin[lslot, 2 * m + 1]
                fnew[lslot, m] = new
                stage[slot, m] = new.astype(jnp.bfloat16)

            @pl.when(s >= 1)
            def _():
                post(s - 1)

            @pl.when(s % 3 == 2)
            def _():
                f = s // 3

                @pl.when(f >= N_LAG)
                def _():
                    n_stage(f - N_LAG)

                @pl.when(f >= D_LAG)
                def _():
                    d_stage(f - D_LAG)

            return 0

        with SC("t_cast"):
            lax.fori_loop(0, steps, body, 0)
        post(steps - 1)
        run(relay, gen - RELAY_LAG, gen)
        run(n_stage, mid - N_LAG, mid)
        run(d_stage, mid - D_LAG, mid)
        for s in range(steps - LOAD_SLOTS, steps):
            finish(stores(s))
        for s in range(steps - STAGE_SLOTS, steps):
            if s % 3 != 2 and mid <= 2 * (s // 3) + s % 3 < mid + chunks:
                own_copy(s).wait()
        with SC("t_sw"):
            run(s_wait, mid, 2 * mid)

        def load_group(c, j, slot):
            start(wload(c, slot, j))

        each_chunk(mid, lead, lambda c, j: load_group(c, j, 0))
        per_block = EARLY * groups
        few = (blocks - MORE) * per_block
        n_visits = few + MORE * (per_block + groups)

        def place(t):
            u = t - few
            more = jnp.where(u >= per_block + groups, 1, 0)
            b = jnp.where(t < few, div(t, per_block), blocks - MORE + more)
            return b, jnp.where(t < few, mod(t, per_block), u - more * (per_block + groups))

        def give_back(b):
            send(h.at[b], h.at[blocks + b], hs.at[b], hr.at[b], tp, 1, rep)

        def visit(t, _):
            b, q = place(t)
            g, slot = mod(q, groups), mod(q, 2)
            with SC("t_ld"):
                each_chunk(0, width_of(g), lambda c, j: finish(wload(c, slot, j)))

            for fn, after in ((own_stage, 0), (n_stage, 8), (d_stage, 18)):

                @pl.when((t >= after) & (t < after + chunks))
                def _():
                    fn(mid + t - after)

            @pl.when(t == few)
            def _():
                run(s_wait, 2 * mid, 2 * mid + chunks)

            @pl.when(t + 1 < n_visits)
            def _():
                _, nq = place(t + 1)
                ng = mod(nq, groups)
                each_chunk(
                    first_of(EARLY + div(nq, groups), ng), width_of(ng), lambda c, j: load_group(c, j, 1 - slot)
                )

            @pl.when(q == 0)
            def _():
                @pl.when(b > 0)
                def _():
                    give_back(b - 1)

                with SC("t_hw"):
                    wait(h.at[b], hr.at[b])

            with SC("t_mm"):
                group_part(slot, g, b, 0)
            return 0

        lax.fori_loop(0, n_visits, visit, 0)
        run(lambda b: wait(h.at[b], hs.at[b]), 0, blocks - 2)
        give_back(blocks - 1)

        def relay_out(i, _):
            @pl.when(i < n_relay)
            def _():
                wait(rin.at[i], rsem.at[0, i])
                send(rin.at[i], rx.at[i], psem.at[0, 0, 0], rsem.at[1, i], flip_tp, 0, rep)

            @pl.when(i >= 1)
            def _():
                q = i - 1
                wait(rx.at[q], rsem.at[1, q])
                b, j, first = 0, 0, 0
                for rb, n in RELAYED:
                    b = jnp.where(q >= first, rb, b)
                    j = jnp.where(q >= first, q - first, j)
                    first += n
                send(rx.at[q], out.at[piece_rows(flip_tp, b, j)], psem.at[0, 0, 1],
                     osem.at[b * pieces + j], tp, 1, rep)

            return 0

        with SC("t_relay"):
            lax.fori_loop(0, n_relay + 1, relay_out, 0)
        wait(rin, psem.at[0, 0, 0])
        wait(rx, psem.at[0, 0, 1])
        run(wait_sent, steps - STAGE_SLOTS, steps)
        run(lambda b: wait(h.at[b], hs.at[b]), blocks - 2, blocks)
        for l in range(2 * EARLY):
            n = count(l * chunks, (l + 1) * chunks, relayed)
            if n:
                wait(wbuf.at[pl.ds(0, n), :, 0, 0, 0], ss.at[0, l])
        for i in range(2):
            wait(wbuf.at[pl.ds(0, chunks), :, 0, 0, 0], ss.at[1, i])
        for l in range(EARLY + 1):
            for m in range(2):
                n = count(l * chunks, (l + 1) * chunks, lambda f: f % 2 == m)
                wait(wbuf.at[pl.ds(0, n), :, 0, 0, 0], ss.at[2 + m, l])
            wait(wbuf.at[pl.ds(0, chunks), :, :, 0], ss.at[4, l])

    @pl.when(side == 1)
    def _():
        def y_stage(e):
            c, l = chunk_of(e), div(e, chunks)
            wait(both(c, own), rs.at[Y, c])
            send(both(c, own), both(c, own), ss.at[0, l], rs.at[Z, c], flip_tp, 1, rep)
            send(both(c, own), both(c, own), ss.at[1, l], rs.at[X, c], tp, 1, flip_rep)

        def n_stage(e):
            c, l = chunk_of(e), div(e, chunks)
            wait(both(c, znb), rs.at[Z, c])
            wait(both(c, xnb), rs.at[X, c])
            direct = jnp.logical_not(relayed(e))

            @pl.when(direct & jnp.logical_not(by_z(e)))
            def _():
                send(both(c, znb), both(c, znb), ss.at[2, l], rs.at[DG, c], tp, 1, flip_rep)

            @pl.when(direct & by_z(e))
            def _():
                send(both(c, xnb), both(c, xnb), ss.at[3, l], rs.at[DG, c], flip_tp, 1, rep)

        def d_stage(e):
            c = chunk_of(e)
            wait(both(c, dia), rs.at[DG, c])
            send(core_half(c, k), core_half(c, k), ss.at[4, div(e, chunks)], rs.at[SB, c], tp, 1, sib_rep)

        turn = EARLY * groups * blocks

        def front(i, t):
            a, s1, jump, s2 = FRONTS[i]
            late = 16 * jump + s1 * turn + s2 * (t - turn)
            return jnp.minimum(gen, a + (jnp.where(t <= turn, s1 * t, late) >> 4))

        def pload(b):
            rows = pl.ds(pl.multiple_of(tp * my_rows + b * BLOCK, BLOCK), BLOCK)
            return pltpu.make_async_copy(prompts.at[rows], rows_buf.at[b % 2], iosem.at[b % 2])

        pload(0).start()
        for b in range(blocks):
            if b + 1 < blocks:
                pload(b + 1).start()
            pload(b).wait()
            for j in range(pieces):
                h[b, :, pl.ds(j * PIECE, PIECE)] = rows_buf[b % 2, pl.ds(j * PIECE, PIECE), :].T

        n_pro = FRONTS[0][0]
        for e in range(n_pro):
            y_stage(e)
            for i, fn in ((1, n_stage), (2, d_stage)):
                if e >= n_pro - FRONTS[i][0]:
                    fn(e - (n_pro - FRONTS[i][0]))
            j = e - (n_pro - lead)
            if j >= 0:
                s_wait(j)
                start(wload(j, 0, j))

        def put(b, j):
            src = rows_buf.at[b % 2, pl.ds(j * PIECE, PIECE), :]
            rows = piece_rows(tp, b, j)
            pltpu.make_async_copy(src, out.at[rows], psem.at[b % 2, j, 0]).start()
            n, i, first = 0, 0, 0
            for rb, m in RELAYED:
                n = jnp.where(b == rb, m, n)
                i = jnp.where(b == rb, first + min(j, m - 1), i)
                first += m

            @pl.when(j < n)
            def _():
                send(src, rin.at[i], psem.at[b % 2, j, 1], rsem.at[0, i], tp, 0, rep)

            @pl.when(j >= n)
            def _():
                send(src, out.at[rows], psem.at[b % 2, j, 1], osem.at[b * pieces + j], flip_tp, 1, rep)

        def put_wait(b):
            for j in range(pieces):
                src = rows_buf.at[b % 2, pl.ds(j * PIECE, PIECE), :]
                wait(src, psem.at[b % 2, j, 0])
                wait(src, psem.at[b % 2, j, 1])

        n_rest = groups - 1
        wide = turn - n_rest * blocks
        n_first = blocks - MORE
        n_tasks = n_first + blocks
        n_visits = turn + n_tasks * groups
        paired = FIRST_LATE + 2 * (n_first - FIRST_LATE)
        first_late, last_late = 2 * EARLY, 2 * EARLY + 1
        arrived = turn + FIRST_LATE * groups - 1

        def late_task(q):
            u = q - FIRST_LATE
            in_pairs = (q >= FIRST_LATE) & (q < paired)
            last = jnp.where(in_pairs, (u & 1) == 0, q >= paired)
            j = u >> 1
            b = jnp.where(in_pairs, jnp.where(last, j, j + FIRST_LATE), jnp.where(q < FIRST_LATE, q, q - n_first))
            return jnp.where(last, last_late, first_late), b

        def rest(t):
            u = t - wide
            b = (u * (128 // n_rest + 1)) >> 7
            return b, 1 + u - n_rest * b

        def give(b):
            send(h.at[b], h.at[b], hs.at[b], hr.at[b], tp, 0, rep)

        def visit(t, _):
            late = t >= turn
            split = (t >= wide) & (t < turn)
            tl, tb = late_task((t - turn) >> 2)
            rb, rg = rest(t)
            l = jnp.where(late, tl, jnp.where(split, EARLY - 1, div(t, groups * blocks)))
            g = jnp.where(late, mod(t, groups), jnp.where(split, rg, mod(div(t, blocks), groups)))
            b = jnp.where(late, tb, jnp.where(split, rb, mod(t, blocks)))
            slot = mod(jnp.where(t < wide, div(t, blocks), t - wide + 1), 2)
            hb = jnp.where(late, blocks + b, b)
            width = width_of(g)

            @pl.when((t >= wide) | (b == 0))
            def _():
                with SC("ld"):
                    each_chunk(0, width, lambda c, j: finish(wload(c, slot, j)))

            @pl.when(t <= arrived)
            def _():
                for i, fn in enumerate((y_stage, n_stage, d_stage)):
                    with SC("fw" + "ynd"[i]):
                        run(fn, front(i, t), front(i, t + 1))

            @pl.when((t > wide) & (t <= turn) & ((rg == 1) | late))
            def _():
                give(rb - 1)

            @pl.when(t < wide)
            def _():
                @pl.when(b < jnp.where(g == groups - 1, lead, GROUP))
                def _():
                    c = first_of(l, g) + width + b
                    with SC("sw"):
                        s_wait(c)
                    start(wload(c, 1 - slot, b))

            @pl.when(t == wide)
            def _():
                with SC("sw1"):
                    run(s_wait, (EARLY - 1) * chunks + lead + GROUP, EARLY * chunks)

            @pl.when(t == turn - 1)
            def _():
                with SC("sw4"):
                    run(lambda e: s_wait(chunk_of(e)), mid, mid + chunks)

            @pl.when(t == arrived)
            def _():
              with SC("sw5"):
                for i, fn in enumerate((y_stage, n_stage, d_stage)):
                    run(fn, front(i, t + 1), gen)
                run(lambda e: s_wait(chunk_of(e)), mid + chunks, gen)

            @pl.when((t >= wide) & (t + 1 < n_visits))
            def _():
                ntl, _ = late_task((t + 1 - turn) >> 2)
                _, nrg = rest(t + 1)
                next_late = t + 1 >= turn
                nl = jnp.where(next_late, ntl, EARLY - 1)
                ng = jnp.where(next_late, mod(t + 1, groups), nrg)
                each_chunk(first_of(nl, ng), width_of(ng), lambda c, j: start(wload(c, 1 - slot, j)))

            @pl.when((g == 0) & late & ((l == first_late) | (b >= n_first)))
            def _():
                with SC("hw"):
                    wait(h.at[hb], hr.at[b])

            with SC("mm"):
                group_part(slot, g, hb, b)

            @pl.when((l == last_late) & (g == groups - 1))
            def _():
                @pl.when(b >= 2)
                def _():
                    put_wait(b - 2)

                for j in range(pieces):
                    cols = pl.ds(j * PIECE, PIECE)
                    rows_buf[mod(b, 2), cols, :] = h[hb, :, cols].T
                    if j >= 1:
                        put(b, j - 1)
                put(b, pieces - 1)

            return 0

        lax.fori_loop(0, n_visits, visit, 0)
        with SC("tail_s"):
          for b in range(blocks - 2, blocks):
            put_wait(b)
        run(lambda b: wait(h.at[b], hs.at[b]), 0, blocks)
        with SC("tail_r"):
          for i in range(blocks * pieces):
            wait(out.at[piece_rows(flip_tp, i // pieces, i % pieces)], osem.at[i])
        for l in range(2 * EARLY):
            for i in range(5):
                if i == 4:
                    wait(wbuf.at[pl.ds(0, chunks), :, :, 0], ss.at[i, l])
                else:
                    kinds = (None, None, lambda e: not relayed(e) and not by_z(e), lambda e: not relayed(e) and by_z(e))
                    n = chunks if i < 2 else count(l * chunks, (l + 1) * chunks, kinds[i])
                    wait(wbuf.at[pl.ds(0, n), :, 0, 0, 0], ss.at[i, l])


def finish_kernel(up, dn, rows, new_up, new_dn, out, buf, zbuf, lsem, ssem, zsem):
    layers = up.shape[0]
    n_rows = rows.shape[0]
    slots, band, hidden = buf.shape
    side = lax.axis_index("side")
    items = [(i, o, l) for l in range(layers) for i, o in ((up, new_up), (dn, new_dn))]
    piece = zbuf.shape[1]
    n_pieces = n_rows // piece
    n_slots = zbuf.shape[0]

    def pipeline(n, n_slots, load, store):
        for i in range(min(n_slots, n)):
            load(i).start()
        half = n_slots // 2
        for i in range(n):
            load(i).wait()
            store(i).start()
            nxt = i + half
            if i >= half and nxt < n:
                store(nxt - n_slots).wait()
                load(nxt).start()

    @pl.when(side == 0)
    def _():
        zbuf[0] = jnp.zeros(zbuf.shape[1:], zbuf.dtype)
        zeros = [
            pltpu.make_async_copy(zbuf.at[0], out.at[pl.ds(i * piece, piece)], zsem.at[i]) for i in range(n_pieces)
        ]
        for cp in zeros:
            cp.start()

        def load(i):
            src, _, l = items[i]
            return pltpu.make_async_copy(src.at[l], buf.at[i % slots], lsem.at[i % slots])

        def store(i):
            _, dst, l = items[i]
            return pltpu.make_async_copy(buf.at[i % slots], dst.at[l], ssem.at[i % slots])

        n = len(items)
        pipeline(n, slots, load, store)
        for i in range(max(n - slots, 0), n):
            store(i).wait()
        for cp in zeros:
            cp.wait()

    @pl.when(side == 1)
    def _():
        buf[0] = jnp.zeros(buf.shape[1:], buf.dtype)
        zeros = [pltpu.make_async_copy(buf.at[0], dst.at[l], zsem.at[i]) for i, (_, dst, l) in enumerate(items)]
        for cp in zeros:
            cp.start()

        def load(i):
            return pltpu.make_async_copy(rows.at[pl.ds(i * piece, piece)], zbuf.at[i % n_slots], lsem.at[i % n_slots])

        def store(i):
            return pltpu.make_async_copy(zbuf.at[i % n_slots], out.at[pl.ds(i * piece, piece)], ssem.at[i % n_slots])

        pipeline(n_pieces, n_slots, load, store)
        for i in range(max(n_pieces - n_slots, 0), n_pieces):
            store(i).wait()
        for cp in zeros:
            cp.wait()


def solution(mesh):
    up_spec = P("side", None, ("rep", "tp"), None)
    down_spec = P("side", None, None, ("rep", "tp"))
    tok_spec = P("side", "rep", None, None)

    def device_step(w_up, w_down, g_up, g_down, learn_rate, prompts):
        layers, band, hidden = w_up.shape[1:]
        n_rows, d = prompts.shape[2:]
        chunks = hidden // UNIT
        total = layers * chunks
        my_rows = n_rows // 2
        blocks, pieces = my_rows // BLOCK, BLOCK // PIECE
        weights = (w_up[0], jnp.swapaxes(w_down[0], 1, 2), g_up[0], jnp.swapaxes(g_down[0], 1, 2))
        smem = pl.BlockSpec(memory_space=pltpu.SMEM)
        hbm = pl.BlockSpec(memory_space=pl.ANY)
        bf16 = jnp.bfloat16
        relay = jax.ShapeDtypeStruct((sum(n for _, n in RELAYED), PIECE, d), bf16)
        new_w = jax.ShapeDtypeStruct((layers, band, hidden), jnp.float32)
        rows = jax.ShapeDtypeStruct((n_rows, d), bf16)
        rows_mid, up_mid, dn_mid, _, _, _ = pl.pallas_call(
            sync_kernel,
            name="sync_and_forward",
            out_shape=(
                rows,
                new_w,
                new_w,
                jax.ShapeDtypeStruct((total, 2, 2, 2, 2, band, UNIT), bf16),
                relay,
                relay,
            ),
            in_specs=[smem] + [hbm] * 5,
            out_specs=(hbm,) * 6,
            scratch_shapes=[
                pltpu.VMEM((2 * blocks, d, BLOCK), bf16),
                pltpu.VMEM((blocks, d, BLOCK), jnp.float32),
                pltpu.VMEM((2, 2, 2, 2, 2, band, GROUP * UNIT), bf16),
                pltpu.VMEM((LOAD_SLOTS, 4, band, UNIT), jnp.float32),
                pltpu.VMEM((LOAD_SLOTS, 2, band, UNIT), jnp.float32),
                pltpu.VMEM((STAGE_SLOTS, 2, band, UNIT), bf16),
                pltpu.VMEM((2, BLOCK, d), bf16),
                pltpu.SemaphoreType.DMA((5, total)),
                pltpu.SemaphoreType.DMA((5, 2 * EARLY)),
                pltpu.SemaphoreType.DMA((LOAD_SLOTS, 4)),
                pltpu.SemaphoreType.DMA((2, GROUP, 2)),
                pltpu.SemaphoreType.DMA((STAGE_SLOTS, 2)),
                pltpu.SemaphoreType.DMA((STAGE_SLOTS,)),
                pltpu.SemaphoreType.DMA((2,)),
                pltpu.SemaphoreType.DMA((2, pieces, 2)),
                pltpu.SemaphoreType.DMA((blocks * pieces,)),
                pltpu.SemaphoreType.DMA((2, sum(n for _, n in RELAYED))),
                pltpu.SemaphoreType.DMA((blocks,)),
                pltpu.SemaphoreType.DMA((blocks,)),
            ],
            compiler_params=pltpu.CompilerParams(has_side_effects=True, vmem_limit_bytes=60 * 1024 * 1024),
        )(learn_rate, *weights, prompts[0, 0])
        new_up, new_dn, gen_out = pl.pallas_call(
            finish_kernel,
            name="write_outputs",
            out_shape=(new_w, new_w, rows),
            in_specs=[hbm] * 3,
            out_specs=(hbm,) * 3,
            scratch_shapes=[
                pltpu.VMEM((8, band, hidden), jnp.float32),
                pltpu.VMEM((8, n_rows // 16, d), bf16),
                pltpu.SemaphoreType.DMA((8,)),
                pltpu.SemaphoreType.DMA((8,)),
                pltpu.SemaphoreType.DMA((max(16, 2 * layers),)),
            ],
            compiler_params=pltpu.CompilerParams(vmem_limit_bytes=62 * 1024 * 1024),
        )(up_mid, dn_mid, rows_mid)
        return new_up[None], jnp.swapaxes(new_dn, 1, 2)[None], gen_out[None, None]

    return jax.shard_map(
        device_step,
        mesh=mesh,
        in_specs=(up_spec, down_spec, up_spec, down_spec, P("side"), tok_spec),
        out_specs=(up_spec, down_spec, tok_spec),
        check_vma=False,
    )
```

```python
import jax
import jax.numpy as jnp
from jax import lax
from jax.experimental import pallas as pl
from jax.experimental.pallas import tpu as pltpu
from jax.sharding import PartitionSpec as P

MESH = pl.DeviceIdType.MESH
SC = jax.named_scope
UNIT = 256
GROUP = 5
BLOCK = 512
PIECE = 128
EARLY = 2
LOAD_SLOTS = 4
STAGE_SLOTS = 36
RING = 32
N_LAG, D_LAG = 3, 6
RELAY_LAG = 4
FIRST_LATE = 3
MORE = 2
RELAYED = ((4, 2), (5, 3), (6, 2))
FRONTS = ((10, 15, 1, 40), (8, 14, 1, 44), (6, 13, 3, 24))
GELU_A = 0.7978845608028654
GELU_B = 0.7978845608028654 * 0.044715


def div(a, n):
    if isinstance(a, int):
        return a // n
    if n & (n - 1) == 0:
        return a >> (n.bit_length() - 1)
    return (a * ((1 << 16) // n + 1)) >> 16


def mod(a, n):
    return a - n * div(a, n)


def gelu(a):
    return a * (0.5 * jnp.tanh(a * (GELU_A + GELU_B * (a * a))) + 0.5)


def sync_kernel(
    rate_ref, w_up, w_dn, g_up, g_dn, prompts, out, nu, nd, wbuf, rin, rx,
    h, p, wv, fin, fnew, stage, rows_buf,
    ysem, rs, rlsem, sbsem, ss, lsem, stsem, fsem, tss, csem, iosem, psem, osem, rsem, hs, hr,
):
    layers, band, hidden = w_up.shape
    chunks = hidden // UNIT
    n_relay = sum(n for _, n in RELAYED)
    groups = -(-chunks // GROUP)
    lead = chunks - (groups - 1) * GROUP
    mid = EARLY * chunks
    gen = 2 * mid
    n_rows, d = out.shape
    my_rows = n_rows // 2
    blocks = my_rows // BLOCK
    pieces = BLOCK // PIECE

    tp = lax.axis_index("tp")
    side = lax.axis_index("side")
    rep = lax.axis_index("rep")
    x, k = rep // 2, rep % 2
    flip_tp = 1 - tp
    flip_rep = (1 - x) * 2 + k
    sib_rep = x * 2 + (1 - k)

    own, znb, xnb, dia = (x, tp), (x, flip_tp), (1 - x, tp), (1 - x, flip_tp)

    def both(c, b):
        return wbuf.at[c, :, b[0], k, b[1]]

    def core_half(c, core):
        return wbuf.at[c, :, :, core]

    def chunk_of(e):
        return e + jnp.where(e >= mid, mid, 0)

    def relayed(e):
        return ((mod(e, 6) == 5) & (e < mid)) | ((mod(e, 3) == 2) & (e >= mid + chunks))

    def by_z(e):
        return ((mod(div(e, 6) + mod(e, 6), 2) == 1) & (e < mid + chunks)) | ((mod(e, 3) == 1) & (e >= mid + chunks))

    def count(e0, e1, fn):
        return sum(1 for e in range(e0, e1) if fn(e))

    n_early = count(0, mid, relayed)

    def relay_index(e):
        return jnp.where(e < mid, div(e, 6), n_early + div(e - mid - chunks, 3))

    def zsem(e):
        return rs.at[0, mod(e, RING)]

    def xsem(e):
        return rs.at[1, mod(e, RING)]

    def dsem(e):
        return rs.at[2, mod(e, RING)]

    def sb_of(e):
        l = div(e, chunks)
        j = e - l * chunks
        g = jnp.where(j < lead, 0, 1 + div(j - lead, GROUP))
        return sbsem.at[jnp.where(e < mid, l * groups + g, EARLY * groups + l - EARLY)]

    def sb_mid(f):
        return sbsem.at[EARLY * groups + EARLY + div(f, chunks)]

    def send(src, dst, ssem, rsem_, t, s, r):
        pltpu.make_async_remote_copy(
            src_ref=src, dst_ref=dst, send_sem=ssem, recv_sem=rsem_,
            device_id={"tp": t, "side": s, "rep": r}, device_id_type=MESH,
        ).start()

    def wait(ref, sem):
        pltpu.make_async_copy(ref, ref, sem).wait()

    def run(fn, lo, hi):
        def body(c, _):
            fn(c)
            return 0

        lax.fori_loop(lo, hi, body, 0)

    def piece_rows(t, b, j):
        return pl.ds(pl.multiple_of(t * my_rows + b * BLOCK + j * PIECE, PIECE), PIECE)

    def sb_wait(c0, width, sem):
        wait(wbuf.at[pl.ds(c0, width), :, :, 1 - k], sem)

    def load_group(c0, g, slot):
        def load(j):
            pltpu.make_async_copy(wbuf.at[c0 + j], wv.at[slot, j], fsem.at[slot]).start()

        for j in range(lead):
            load(j)

        @pl.when(g > 0)
        def _():
            for j in range(lead, GROUP):
                load(j)

    def wait_group(g, slot):
        @pl.when(g == 0)
        def _():
            wait(wv.at[slot, pl.ds(0, lead)], fsem.at[slot])

        @pl.when(g > 0)
        def _():
            wait(wv.at[slot], fsem.at[slot])

    def width_of(g):
        return jnp.where(g == 0, lead, GROUP)

    def first_of(l, g):
        return l * chunks + jnp.where(g == 0, 0, lead + (g - 1) * GROUP)

    def matmuls(slot, hb, width):
        def weight(m):
            return jnp.concatenate([wv[slot, j, m].reshape(d, UNIT) for j in range(width)], axis=1)

        a = lax.dot_general(weight(0), h[hb], (((0,), (0,)), ((), ())), preferred_element_type=jnp.float32)
        u = gelu(a).astype(jnp.bfloat16)
        return jnp.dot(weight(1), u, preferred_element_type=jnp.float32)

    def group_part(slot, g, hb, pb):
        @pl.when(g == 0)
        def _():
            p[pb] = matmuls(slot, hb, lead)

        @pl.when((g > 0) & (g < groups - 1))
        def _():
            p[pb] = p[pb] + matmuls(slot, hb, GROUP)

        @pl.when(g == groups - 1)
        def _():
            s = p[pb] + matmuls(slot, hb, GROUP)
            h[hb] = (h[hb].astype(jnp.float32) + s).astype(jnp.bfloat16)

    @pl.when(side == 0)
    def _():
        rate = rate_ref[0]
        parts = ((w_up, g_up, nu), (w_dn, g_dn, nd))
        steps = gen + mid

        def chunk_at(s):
            return jnp.where(mod(s, 3) == 2, mid + div(s, 3), chunk_of(2 * div(s, 3) + mod(s, 3)))

        def cols_of(c):
            return div(c, chunks), pl.ds(pl.multiple_of(mod(c, chunks) * UNIT, UNIT), UNIT)

        def loads(s):
            l, cols = cols_of(chunk_at(s))
            slot = mod(s, LOAD_SLOTS)
            for m in range(2):
                for i, r in enumerate(parts[m][:2]):
                    pltpu.make_async_copy(r.at[l, :, cols], fin.at[slot, 2 * m + i], lsem.at[slot]).start()

        def stores(s):
            l, cols = cols_of(chunk_at(s))
            slot = mod(s, LOAD_SLOTS)
            for m in range(2):
                pltpu.make_async_copy(fnew.at[slot, m], parts[m][2].at[l, :, cols], stsem.at[slot]).start()

        def wait_stored(s):
            slot = mod(s, LOAD_SLOTS)
            wait(fnew.at[slot], stsem.at[slot])

        def own_copy(s):
            slot = s % STAGE_SLOTS
            return pltpu.make_async_copy(stage.at[slot], both(chunk_at(s), own), csem.at[slot])

        def gathered_too(s):
            e = 2 * (s // 3) + s % 3
            return (s % 3 != 2) & (e >= mid) & (e < mid + chunks)

        def post(s):
            slot = s % STAGE_SLOTS
            src = stage.at[slot]
            stores(s)

            @pl.when(s % 3 != 2)
            def _():
                e = 2 * (s // 3) + s % 3
                c = chunk_of(e)
                send(src, both(c, own), tss.at[slot, 0], ysem.at[e], tp, 1, rep)

                @pl.when(gathered_too(s))
                def _():
                    own_copy(s).start()

                @pl.when(relayed(e))
                def _():
                    send(src, both(c, own), tss.at[slot, 1], rlsem.at[relay_index(e)], flip_tp, 0, flip_rep)

                @pl.when(e >= RELAY_LAG)
                def _():
                    relay(e - RELAY_LAG)

            @pl.when(s % 3 == 2)
            def _():
                f = div(s, 3)
                c = mid + f
                own_copy(s).start()
                send(src, both(c, own), tss.at[slot, 0], zsem(f), flip_tp, 0, rep)
                send(src, both(c, own), tss.at[slot, 1], xsem(f), tp, 0, flip_rep)

        def relay(e):
            @pl.when(relayed(e))
            def _():
                c = chunk_of(e)
                sem = rlsem.at[relay_index(e)]
                wait(both(c, dia), sem)
                send(both(c, dia), both(c, dia), ss.at[0, div(e, chunks)], sem, tp, 1, rep)

        def wait_sent(s):
            slot = s % STAGE_SLOTS
            is_mid = s % 3 == 2
            wait(stage.at[slot], tss.at[slot, 0])

            @pl.when(is_mid | relayed(2 * (s // 3) + s % 3))
            def _():
                wait(stage.at[slot], tss.at[slot, 1])

        def own_stage(f):
            c = mid + f
            send(both(c, own), both(c, own), ss.at[1, 0], zsem(f), flip_tp, 0, rep)
            send(both(c, own), both(c, own), ss.at[1, 1], xsem(f), tp, 0, flip_rep)

        def n_stage(f):
            c = mid + f
            wait(both(c, znb), zsem(f))
            wait(both(c, xnb), xsem(f))

            @pl.when(mod(f, 2) == 0)
            def _():
                send(both(c, znb), both(c, znb), ss.at[2, div(f, chunks)], dsem(f), tp, 0, flip_rep)

            @pl.when(mod(f, 2) == 1)
            def _():
                send(both(c, xnb), both(c, xnb), ss.at[3, div(f, chunks)], dsem(f), flip_tp, 0, rep)

        def d_stage(f):
            c = mid + f
            wait(both(c, dia), dsem(f))

            @pl.when(f < mid)
            def _():
                own_copy(3 * f + 2).wait()

            send(core_half(c, k), core_half(c, k), ss.at[4, div(f, chunks)], sb_mid(f), tp, 0, sib_rep)

        for s in range(LOAD_SLOTS - 1):
            loads(s)

        def body(s, _):
            @pl.when(s + LOAD_SLOTS - 1 < steps)
            def _():
                loads(s + LOAD_SLOTS - 1)

            slot, lslot = s % STAGE_SLOTS, mod(s, LOAD_SLOTS)
            wait(fin.at[lslot], lsem.at[lslot])

            @pl.when(s >= STAGE_SLOTS)
            def _():
                wait_sent(s - STAGE_SLOTS)

                @pl.when(gathered_too(s - STAGE_SLOTS))
                def _():
                    own_copy(s - STAGE_SLOTS).wait()

            @pl.when(s >= LOAD_SLOTS)
            def _():
                wait_stored(s - LOAD_SLOTS)

            for m in range(2):
                new = fin[lslot, 2 * m] - rate * fin[lslot, 2 * m + 1]
                fnew[lslot, m] = new
                stage[slot, m] = new.astype(jnp.bfloat16)

            @pl.when(s >= 1)
            def _():
                post(s - 1)

            @pl.when(s % 3 == 2)
            def _():
                f = s // 3

                @pl.when(f >= N_LAG)
                def _():
                    n_stage(f - N_LAG)

                @pl.when(f >= D_LAG)
                def _():
                    d_stage(f - D_LAG)

            return 0

        with SC("t_cast"):
            lax.fori_loop(0, steps, body, 0)
        post(steps - 1)
        run(relay, gen - RELAY_LAG, gen)
        run(n_stage, mid - N_LAG, mid)
        run(d_stage, mid - D_LAG, mid)
        for s in range(steps - LOAD_SLOTS, steps):
            wait_stored(s)
        for s in range(steps - STAGE_SLOTS, steps):
            if s % 3 != 2 and mid <= 2 * (s // 3) + s % 3 < mid + chunks:
                own_copy(s).wait()
        for l in range(EARLY):
            sb_wait(mid + l * chunks, chunks, sb_mid(l * chunks))

        load_group(mid, 0, 0)
        per_block = EARLY * groups
        few = (blocks - MORE) * per_block
        n_visits = few + MORE * (per_block + groups)

        def place(t):
            u = t - few
            more = jnp.where(u >= per_block + groups, 1, 0)
            b = jnp.where(t < few, div(t, per_block), blocks - MORE + more)
            return b, jnp.where(t < few, mod(t, per_block), u - more * (per_block + groups))

        def give_back(b):
            send(h.at[b], h.at[blocks + b], hs.at[b], hr.at[b], tp, 1, rep)

        def visit(t, _):
            b, q = place(t)
            g, slot = mod(q, groups), mod(q, 2)
            with SC("t_ld"):
                wait_group(g, slot)

            for fn, after in ((own_stage, 0), (n_stage, 8), (d_stage, 18)):

                @pl.when((t >= after) & (t < after + chunks))
                def _():
                    fn(mid + t - after)

            @pl.when(t == few)
            def _():
                sb_wait(2 * mid, chunks, sb_mid(mid))

            @pl.when(t + 1 < n_visits)
            def _():
                _, nq = place(t + 1)
                ng = mod(nq, groups)
                load_group(first_of(EARLY + div(nq, groups), ng), ng, 1 - slot)

            @pl.when(q == 0)
            def _():
                @pl.when(b > 0)
                def _():
                    give_back(b - 1)

                with SC("t_hw"):
                    wait(h.at[b], hr.at[b])

            with SC("t_mm"):
                group_part(slot, g, b, 0)
            return 0

        lax.fori_loop(0, n_visits, visit, 0)
        run(lambda b: wait(h.at[b], hs.at[b]), 0, blocks - 2)
        give_back(blocks - 1)

        def relay_out(i, _):
            @pl.when(i < n_relay)
            def _():
                wait(rin.at[i], rsem.at[0, i])
                send(rin.at[i], rx.at[i], psem.at[0, 0], rsem.at[1, i], flip_tp, 0, rep)

            @pl.when(i >= 1)
            def _():
                q = i - 1
                wait(rx.at[q], rsem.at[1, q])
                b, j, first = 0, 0, 0
                for rb, n in RELAYED:
                    b = jnp.where(q >= first, rb, b)
                    j = jnp.where(q >= first, q - first, j)
                    first += n
                send(rx.at[q], out.at[piece_rows(flip_tp, b, j)], psem.at[0, 1], osem.at[0], tp, 1, rep)

            return 0

        with SC("t_relay"):
            lax.fori_loop(0, n_relay + 1, relay_out, 0)
        wait(rin, psem.at[0, 0])
        wait(rx, psem.at[0, 1])
        run(wait_sent, steps - STAGE_SLOTS, steps)
        run(lambda b: wait(h.at[b], hs.at[b]), blocks - 2, blocks)
        for l in range(2 * EARLY):
            n = count(l * chunks, (l + 1) * chunks, relayed)
            if n:
                wait(wbuf.at[pl.ds(0, n), :, 0, 0, 0], ss.at[0, l])
        for i in range(2):
            wait(wbuf.at[pl.ds(0, chunks), :, 0, 0, 0], ss.at[1, i])
        for l in range(EARLY + 1):
            for m in range(2):
                n = count(l * chunks, (l + 1) * chunks, lambda f: f % 2 == m)
                wait(wbuf.at[pl.ds(0, n), :, 0, 0, 0], ss.at[2 + m, l])
            wait(wbuf.at[pl.ds(0, chunks), :, :, 0], ss.at[4, l])

    @pl.when(side == 1)
    def _():
        def y_stage(e):
            c, l = chunk_of(e), div(e, chunks)
            wait(both(c, own), ysem.at[e])
            send(both(c, own), both(c, own), ss.at[0, l], zsem(e), flip_tp, 1, rep)
            send(both(c, own), both(c, own), ss.at[1, l], xsem(e), tp, 1, flip_rep)

        def n_stage(e):
            c, l = chunk_of(e), div(e, chunks)
            wait(both(c, znb), zsem(e))
            wait(both(c, xnb), xsem(e))
            direct = jnp.logical_not(relayed(e))

            @pl.when(direct & jnp.logical_not(by_z(e)))
            def _():
                send(both(c, znb), both(c, znb), ss.at[2, l], dsem(e), tp, 1, flip_rep)

            @pl.when(direct & by_z(e))
            def _():
                send(both(c, xnb), both(c, xnb), ss.at[3, l], dsem(e), flip_tp, 1, rep)

        def d_stage(e):
            c = chunk_of(e)

            @pl.when(relayed(e))
            def _():
                wait(both(c, dia), rlsem.at[relay_index(e)])

            @pl.when(jnp.logical_not(relayed(e)))
            def _():
                wait(both(c, dia), dsem(e))

            send(core_half(c, k), core_half(c, k), ss.at[4, div(e, chunks)], sb_of(e), tp, 1, sib_rep)

        turn = EARLY * groups * blocks

        def front(i, t):
            a, s1, jump, s2 = FRONTS[i]
            late = 16 * jump + s1 * turn + s2 * (t - turn)
            return jnp.minimum(gen, a + (jnp.where(t <= turn, s1 * t, late) >> 4))

        def pload(b):
            rows = pl.ds(pl.multiple_of(tp * my_rows + b * BLOCK, BLOCK), BLOCK)
            return pltpu.make_async_copy(prompts.at[rows], rows_buf.at[b % 2], iosem.at[b % 2])

        pload(0).start()
        for b in range(blocks):
            if b + 1 < blocks:
                pload(b + 1).start()
            pload(b).wait()
            for j in range(pieces):
                h[b, :, pl.ds(j * PIECE, PIECE)] = rows_buf[b % 2, pl.ds(j * PIECE, PIECE), :].T

        n_pro = FRONTS[0][0]
        for e in range(n_pro):
            y_stage(e)
            for i, fn in ((1, n_stage), (2, d_stage)):
                if e >= n_pro - FRONTS[i][0]:
                    fn(e - (n_pro - FRONTS[i][0]))
        sb_wait(0, lead, sbsem.at[0])
        load_group(0, 0, 0)

        def put(b, j):
            src = rows_buf.at[mod(b, 2), pl.ds(j * PIECE, PIECE), :]
            rows = piece_rows(tp, b, j)
            pltpu.make_async_copy(src, out.at[rows], psem.at[mod(b, 2), 0]).start()
            n, i, first = 0, 0, 0
            for rb, m in RELAYED:
                n = jnp.where(b == rb, m, n)
                i = jnp.where(b == rb, first + min(j, m - 1), i)
                first += m

            @pl.when(j < n)
            def _():
                send(src, rin.at[i], psem.at[mod(b, 2), 1], rsem.at[0, i], tp, 0, rep)

            @pl.when(j >= n)
            def _():
                send(src, out.at[rows], psem.at[mod(b, 2), 1], osem.at[0], flip_tp, 1, rep)

        def put_wait(b):
            for i in range(2):
                wait(rows_buf.at[mod(b, 2)], psem.at[mod(b, 2), i])

        n_rest = groups - 1
        wide = turn - n_rest * blocks
        n_first = blocks - MORE
        n_tasks = n_first + blocks
        n_visits = turn + n_tasks * groups
        paired = FIRST_LATE + 2 * (n_first - FIRST_LATE)
        first_late, last_late = 2 * EARLY, 2 * EARLY + 1
        arrived = turn + FIRST_LATE * groups - 1

        def late_task(q):
            u = q - FIRST_LATE
            in_pairs = (q >= FIRST_LATE) & (q < paired)
            last = jnp.where(in_pairs, (u & 1) == 0, q >= paired)
            j = u >> 1
            b = jnp.where(in_pairs, jnp.where(last, j, j + FIRST_LATE), jnp.where(q < FIRST_LATE, q, q - n_first))
            return jnp.where(last, last_late, first_late), b

        def rest(t):
            u = t - wide
            b = (u * (128 // n_rest + 1)) >> 7
            return b, 1 + u - n_rest * b

        def give(b):
            send(h.at[b], h.at[b], hs.at[b], hr.at[b], tp, 0, rep)

        def visit(t, _):
            late = t >= turn
            split = (t >= wide) & (t < turn)
            tl, tb = late_task((t - turn) >> 2)
            rb, rg = rest(t)
            l = jnp.where(late, tl, jnp.where(split, EARLY - 1, div(t, groups * blocks)))
            g = jnp.where(late, mod(t, groups), jnp.where(split, rg, mod(div(t, blocks), groups)))
            b = jnp.where(late, tb, jnp.where(split, rb, mod(t, blocks)))
            slot = mod(jnp.where(t < wide, div(t, blocks), t - wide + 1), 2)
            hb = jnp.where(late, blocks + b, b)
            @pl.when((t >= wide) | (b == 0))
            def _():
                with SC("ld"):
                    wait_group(g, slot)

            @pl.when(t <= arrived)
            def _():
                for i, fn in enumerate((y_stage, n_stage, d_stage)):
                    with SC("fw" + "ynd"[i]):
                        run(fn, front(i, t), front(i, t + 1))

            @pl.when((t > wide) & (t <= turn) & ((rg == 1) | late))
            def _():
                give(rb - 1)

            @pl.when((t < wide) & (b == blocks // 2))
            def _():
                c0 = first_of(l, g) + width_of(g)
                ng = mod(g + 1, groups)
                sem = sb_of(c0)

                @pl.when(ng == 0)
                def _():
                    sb_wait(c0, lead, sem)

                @pl.when(ng > 0)
                def _():
                    sb_wait(c0, GROUP, sem)

                load_group(c0, ng, 1 - slot)

            @pl.when(t == wide)
            def _():
                for g_ in range(2, groups):
                    c0 = (EARLY - 1) * chunks + lead + (g_ - 1) * GROUP
                    sb_wait(c0, GROUP, sb_of(c0))

            @pl.when(t == turn - 1)
            def _():
                with SC("sw4"):
                    sb_wait(2 * mid, chunks, sb_of(mid))

            @pl.when(t == arrived)
            def _():
              with SC("sw5"):
                for i, fn in enumerate((y_stage, n_stage, d_stage)):
                    run(fn, front(i, t + 1), gen)
                sb_wait(2 * mid + chunks, chunks, sb_of(mid + chunks))

            @pl.when((t >= wide) & (t + 1 < n_visits))
            def _():
                ntl, _ = late_task((t + 1 - turn) >> 2)
                _, nrg = rest(t + 1)
                next_late = t + 1 >= turn
                nl = jnp.where(next_late, ntl, EARLY - 1)
                ng = jnp.where(next_late, mod(t + 1, groups), nrg)
                load_group(first_of(nl, ng), ng, 1 - slot)

            @pl.when((g == 0) & late & ((l == first_late) | (b >= n_first)))
            def _():
                with SC("hw"):
                    wait(h.at[hb], hr.at[b])

            with SC("mm"):
                group_part(slot, g, hb, b)

            @pl.when((l == last_late) & (g == groups - 1))
            def _():
                @pl.when(b >= 2)
                def _():
                    put_wait(b - 2)

                for j in range(pieces):
                    cols = pl.ds(j * PIECE, PIECE)
                    rows_buf[mod(b, 2), cols, :] = h[hb, :, cols].T
                    if j >= 1:
                        put(b, j - 1)
                put(b, pieces - 1)

            return 0

        lax.fori_loop(0, n_visits, visit, 0)
        with SC("tail_s"):
          for b in range(blocks - 2, blocks):
            put_wait(b)
        run(lambda b: wait(h.at[b], hs.at[b]), 0, blocks)
        with SC("tail_r"):
            wait(out.at[pl.ds(pl.multiple_of(flip_tp * my_rows, BLOCK), my_rows)], osem.at[0])
        for l in range(2 * EARLY):
            for i in range(5):
                if i == 4:
                    wait(wbuf.at[pl.ds(0, chunks), :, :, 0], ss.at[i, l])
                else:
                    kinds = (None, None, lambda e: not relayed(e) and not by_z(e), lambda e: not relayed(e) and by_z(e))
                    n = chunks if i < 2 else count(l * chunks, (l + 1) * chunks, kinds[i])
                    wait(wbuf.at[pl.ds(0, n), :, 0, 0, 0], ss.at[i, l])


def finish_kernel(up, dn, rows, new_up, new_dn, out, buf, zbuf, lsem, ssem, zsem):
    layers = up.shape[0]
    n_rows = rows.shape[0]
    slots, band, hidden = buf.shape
    side = lax.axis_index("side")
    items = [(i, o, l) for l in range(layers) for i, o in ((up, new_up), (dn, new_dn))]
    piece = zbuf.shape[1]
    n_pieces = n_rows // piece
    n_slots = zbuf.shape[0]

    def pipeline(n, n_slots, load, store):
        for i in range(min(n_slots, n)):
            load(i).start()
        half = n_slots // 2
        for i in range(n):
            load(i).wait()
            store(i).start()
            nxt = i + half
            if i >= half and nxt < n:
                store(nxt - n_slots).wait()
                load(nxt).start()

    @pl.when(side == 0)
    def _():
        zbuf[0] = jnp.zeros(zbuf.shape[1:], zbuf.dtype)
        zeros = [
            pltpu.make_async_copy(zbuf.at[0], out.at[pl.ds(i * piece, piece)], zsem.at[i]) for i in range(n_pieces)
        ]
        for cp in zeros:
            cp.start()

        def load(i):
            src, _, l = items[i]
            return pltpu.make_async_copy(src.at[l], buf.at[i % slots], lsem.at[i % slots])

        def store(i):
            _, dst, l = items[i]
            return pltpu.make_async_copy(buf.at[i % slots], dst.at[l], ssem.at[i % slots])

        n = len(items)
        pipeline(n, slots, load, store)
        for i in range(max(n - slots, 0), n):
            store(i).wait()
        for cp in zeros:
            cp.wait()

    @pl.when(side == 1)
    def _():
        buf[0] = jnp.zeros(buf.shape[1:], buf.dtype)
        zeros = [pltpu.make_async_copy(buf.at[0], dst.at[l], zsem.at[i]) for i, (_, dst, l) in enumerate(items)]
        for cp in zeros:
            cp.start()

        def load(i):
            return pltpu.make_async_copy(rows.at[pl.ds(i * piece, piece)], zbuf.at[i % n_slots], lsem.at[i % n_slots])

        def store(i):
            return pltpu.make_async_copy(zbuf.at[i % n_slots], out.at[pl.ds(i * piece, piece)], ssem.at[i % n_slots])

        pipeline(n_pieces, n_slots, load, store)
        for i in range(max(n_pieces - n_slots, 0), n_pieces):
            store(i).wait()
        for cp in zeros:
            cp.wait()


def solution(mesh):
    up_spec = P("side", None, ("rep", "tp"), None)
    down_spec = P("side", None, None, ("rep", "tp"))
    tok_spec = P("side", "rep", None, None)

    def device_step(w_up, w_down, g_up, g_down, learn_rate, prompts):
        layers, band, hidden = w_up.shape[1:]
        n_rows, d = prompts.shape[2:]
        chunks = hidden // UNIT
        total = layers * chunks
        my_rows = n_rows // 2
        blocks, pieces = my_rows // BLOCK, BLOCK // PIECE
        weights = (w_up[0], jnp.swapaxes(w_down[0], 1, 2), g_up[0], jnp.swapaxes(g_down[0], 1, 2))
        smem = pl.BlockSpec(memory_space=pltpu.SMEM)
        hbm = pl.BlockSpec(memory_space=pl.ANY)
        bf16 = jnp.bfloat16
        relay = jax.ShapeDtypeStruct((sum(n for _, n in RELAYED), PIECE, d), bf16)
        new_w = jax.ShapeDtypeStruct((layers, band, hidden), jnp.float32)
        rows = jax.ShapeDtypeStruct((n_rows, d), bf16)
        rows_mid, up_mid, dn_mid, _, _, _ = pl.pallas_call(
            sync_kernel,
            name="sync_and_forward",
            out_shape=(
                rows,
                new_w,
                new_w,
                jax.ShapeDtypeStruct((total, 2, 2, 2, 2, band, UNIT), bf16),
                relay,
                relay,
            ),
            in_specs=[smem] + [hbm] * 5,
            out_specs=(hbm,) * 6,
            scratch_shapes=[
                pltpu.VMEM((2 * blocks, d, BLOCK), bf16),
                pltpu.VMEM((blocks, d, BLOCK), jnp.float32),
                pltpu.VMEM((2, GROUP, 2, 2, 2, 2, band, UNIT), bf16),
                pltpu.VMEM((LOAD_SLOTS, 4, band, UNIT), jnp.float32),
                pltpu.VMEM((LOAD_SLOTS, 2, band, UNIT), jnp.float32),
                pltpu.VMEM((STAGE_SLOTS, 2, band, UNIT), bf16),
                pltpu.VMEM((2, BLOCK, d), bf16),
                pltpu.SemaphoreType.DMA((2 * EARLY * chunks,)),
                pltpu.SemaphoreType.DMA((3, RING)),
                pltpu.SemaphoreType.DMA((EARLY * chunks // 6 + chunks // 3 + 1,)),
                pltpu.SemaphoreType.DMA((EARLY * (-(-chunks // GROUP)) + 2 * EARLY + 1,)),
                pltpu.SemaphoreType.DMA((5, 2 * EARLY)),
                pltpu.SemaphoreType.DMA((LOAD_SLOTS,)),
                pltpu.SemaphoreType.DMA((LOAD_SLOTS,)),
                pltpu.SemaphoreType.DMA((2,)),
                pltpu.SemaphoreType.DMA((STAGE_SLOTS, 2)),
                pltpu.SemaphoreType.DMA((STAGE_SLOTS,)),
                pltpu.SemaphoreType.DMA((2,)),
                pltpu.SemaphoreType.DMA((2, 2)),
                pltpu.SemaphoreType.DMA((1,)),
                pltpu.SemaphoreType.DMA((2, sum(n for _, n in RELAYED))),
                pltpu.SemaphoreType.DMA((blocks,)),
                pltpu.SemaphoreType.DMA((blocks,)),
            ],
            compiler_params=pltpu.CompilerParams(has_side_effects=True, vmem_limit_bytes=60 * 1024 * 1024),
        )(learn_rate, *weights, prompts[0, 0])
        new_up, new_dn, gen_out = pl.pallas_call(
            finish_kernel,
            name="write_outputs",
            out_shape=(new_w, new_w, rows),
            in_specs=[hbm] * 3,
            out_specs=(hbm,) * 3,
            scratch_shapes=[
                pltpu.VMEM((8, band, hidden), jnp.float32),
                pltpu.VMEM((8, n_rows // 16, d), bf16),
                pltpu.SemaphoreType.DMA((8,)),
                pltpu.SemaphoreType.DMA((8,)),
                pltpu.SemaphoreType.DMA((max(16, 2 * layers),)),
            ],
            compiler_params=pltpu.CompilerParams(vmem_limit_bytes=62 * 1024 * 1024),
        )(up_mid, dn_mid, rows_mid)
        return new_up[None], jnp.swapaxes(new_dn, 1, 2)[None], gen_out[None, None]

    return jax.shard_map(
        device_step,
        mesh=mesh,
        in_specs=(up_spec, down_spec, up_spec, down_spec, P("side"), tok_spec),
        out_specs=(up_spec, down_spec, tok_spec),
        check_vma=False,
    )
```

```python
import jax
import jax.numpy as jnp
from jax import lax
from jax.experimental import pallas as pl
from jax.experimental.pallas import tpu as pltpu
from jax.sharding import PartitionSpec as P

MESH = pl.DeviceIdType.MESH
SC = jax.named_scope
UNIT = 256
GROUP = 5
BLOCK = 512
PIECE = 128
EARLY = 2
LOAD_SLOTS = 4
STAGE_SLOTS = 36
RING = 32
N_LAG, D_LAG = 3, 6
RELAY_LAG = 4
FIRST_LATE = 3
MORE = 2
RELAYED = ((4, 2), (5, 2), (6, 2))
FRONTS = ((10, 15, 1, 40), (8, 14, 1, 44), (6, 13, 3, 24))
GELU_A = 0.7978845608028654
GELU_B = 0.7978845608028654 * 0.044715


def div(a, n):
    if isinstance(a, int):
        return a // n
    if n & (n - 1) == 0:
        return a >> (n.bit_length() - 1)
    return (a * ((1 << 16) // n + 1)) >> 16


def mod(a, n):
    return a - n * div(a, n)


def gelu(a):
    return a * (0.5 * jnp.tanh(a * (GELU_A + GELU_B * (a * a))) + 0.5)


def sync_kernel(
    rate_ref, w_up, w_dn, g_up, g_dn, prompts, out, nu, nd, wbuf, rin, rx,
    h, p, wv, fin, fnew, stage, rows_buf,
    ysem, rs, rlsem, sbsem, ss, lsem, stsem, fsem, tss, csem, iosem, psem, osem, rsem, hs, hr,
):
    layers, band, hidden = w_up.shape
    chunks = hidden // UNIT
    n_relay = sum(n for _, n in RELAYED)
    groups = -(-chunks // GROUP)
    lead = chunks - (groups - 1) * GROUP
    mid = EARLY * chunks
    gen = 2 * mid
    n_rows, d = out.shape
    my_rows = n_rows // 2
    blocks = my_rows // BLOCK
    pieces = BLOCK // PIECE

    tp = lax.axis_index("tp")
    side = lax.axis_index("side")
    rep = lax.axis_index("rep")
    x, k = rep // 2, rep % 2
    flip_tp = 1 - tp
    flip_rep = (1 - x) * 2 + k
    sib_rep = x * 2 + (1 - k)

    barrier = pltpu.get_barrier_semaphore()
    peers = [(tp, 1 - side, rep)] + [
        (t, side, r) for t, r in ((flip_tp, rep), (tp, flip_rep), (flip_tp, flip_rep), (tp, sib_rep))
    ]
    for t, s_, r in peers:
        pl.semaphore_signal(
            barrier, inc=1, device_id={"tp": t, "side": s_, "rep": r}, device_id_type=MESH
        )
    with SC("bar"):
        pl.semaphore_wait(barrier, len(peers))

    own, znb, xnb, dia = (x, tp), (x, flip_tp), (1 - x, tp), (1 - x, flip_tp)

    def both(c, b):
        return wbuf.at[c, :, b[0], k, b[1]]

    def core_half(c, core):
        return wbuf.at[c, :, :, core]

    def chunk_of(e):
        return e + jnp.where(e >= mid, mid, 0)

    def relayed(e):
        return ((mod(e, 6) == 5) & (e < mid)) | ((mod(e, 3) == 2) & (e >= mid + chunks))

    def by_z(e):
        return ((mod(div(e, 6) + mod(e, 6), 2) == 1) & (e < mid + chunks)) | ((mod(e, 3) == 1) & (e >= mid + chunks))

    def count(e0, e1, fn):
        return sum(1 for e in range(e0, e1) if fn(e))

    n_early = count(0, mid, relayed)

    def relay_index(e):
        return jnp.where(e < mid, div(e, 6), n_early + div(e - mid - chunks, 3))

    def zsem(e):
        return rs.at[0, mod(e, RING)]

    def xsem(e):
        return rs.at[1, mod(e, RING)]

    def dsem(e):
        return rs.at[2, mod(e, RING)]

    def sb_of(e):
        l = div(e, chunks)
        j = e - l * chunks
        g = jnp.where(j < lead, 0, 1 + div(j - lead, GROUP))
        return sbsem.at[jnp.where(e < mid, l * groups + g, EARLY * groups + l - EARLY)]

    def sb_mid(f):
        return sbsem.at[EARLY * groups + EARLY + div(f, chunks)]

    def send(src, dst, ssem, rsem_, t, s, r):
        pltpu.make_async_remote_copy(
            src_ref=src, dst_ref=dst, send_sem=ssem, recv_sem=rsem_,
            device_id={"tp": t, "side": s, "rep": r}, device_id_type=MESH,
        ).start()

    def wait(ref, sem):
        pltpu.make_async_copy(ref, ref, sem).wait()

    def run(fn, lo, hi):
        def body(c, _):
            fn(c)
            return 0

        lax.fori_loop(lo, hi, body, 0)

    def piece_rows(t, b, j):
        return pl.ds(pl.multiple_of(t * my_rows + b * BLOCK + j * PIECE, PIECE), PIECE)

    def sb_wait(c0, width, sem):
        wait(wbuf.at[pl.ds(c0, width), :, :, 1 - k], sem)

    def load_group(c0, g, slot):
        def load(j):
            pltpu.make_async_copy(wbuf.at[c0 + j], wv.at[slot, j], fsem.at[slot]).start()

        for j in range(lead):
            load(j)

        @pl.when(g > 0)
        def _():
            for j in range(lead, GROUP):
                load(j)

    def wait_group(g, slot):
        @pl.when(g == 0)
        def _():
            wait(wv.at[slot, pl.ds(0, lead)], fsem.at[slot])

        @pl.when(g > 0)
        def _():
            wait(wv.at[slot], fsem.at[slot])

    def width_of(g):
        return jnp.where(g == 0, lead, GROUP)

    def first_of(l, g):
        return l * chunks + jnp.where(g == 0, 0, lead + (g - 1) * GROUP)

    def matmuls(slot, hb, width):
        def weight(m):
            return jnp.concatenate([wv[slot, j, m].reshape(d, UNIT) for j in range(width)], axis=1)

        a = lax.dot_general(weight(0), h[hb], (((0,), (0,)), ((), ())), preferred_element_type=jnp.float32)
        u = gelu(a).astype(jnp.bfloat16)
        return jnp.dot(weight(1), u, preferred_element_type=jnp.float32)

    def group_part(slot, g, hb, pb):
        @pl.when(g == 0)
        def _():
            p[pb] = matmuls(slot, hb, lead)

        @pl.when((g > 0) & (g < groups - 1))
        def _():
            p[pb] = p[pb] + matmuls(slot, hb, GROUP)

        @pl.when(g == groups - 1)
        def _():
            s = p[pb] + matmuls(slot, hb, GROUP)
            h[hb] = (h[hb].astype(jnp.float32) + s).astype(jnp.bfloat16)

    @pl.when(side == 0)
    def _():
        rate = rate_ref[0]
        parts = ((w_up, g_up, nu), (w_dn, g_dn, nd))
        steps = gen + mid

        def chunk_at(s):
            return jnp.where(mod(s, 3) == 2, mid + div(s, 3), chunk_of(2 * div(s, 3) + mod(s, 3)))

        def cols_of(c):
            return div(c, chunks), pl.ds(pl.multiple_of(mod(c, chunks) * UNIT, UNIT), UNIT)

        def loads(s):
            l, cols = cols_of(chunk_at(s))
            slot = mod(s, LOAD_SLOTS)
            for m in range(2):
                for i, r in enumerate(parts[m][:2]):
                    pltpu.make_async_copy(r.at[l, :, cols], fin.at[slot, 2 * m + i], lsem.at[slot]).start()

        def stores(s):
            l, cols = cols_of(chunk_at(s))
            slot = mod(s, LOAD_SLOTS)
            for m in range(2):
                pltpu.make_async_copy(fnew.at[slot, m], parts[m][2].at[l, :, cols], stsem.at[slot]).start()

        def wait_stored(s):
            slot = mod(s, LOAD_SLOTS)
            wait(fnew.at[slot], stsem.at[slot])

        def own_copy(s):
            slot = s % STAGE_SLOTS
            return pltpu.make_async_copy(stage.at[slot], both(chunk_at(s), own), csem.at[slot])

        def gathered_too(s):
            e = 2 * (s // 3) + s % 3
            return (s % 3 != 2) & (e >= mid) & (e < mid + chunks)

        def post(s):
            slot = s % STAGE_SLOTS
            src = stage.at[slot]
            stores(s)

            @pl.when(s % 3 != 2)
            def _():
                e = 2 * (s // 3) + s % 3
                c = chunk_of(e)
                send(src, both(c, own), tss.at[slot, 0], ysem.at[e], tp, 1, rep)

                @pl.when(gathered_too(s))
                def _():
                    own_copy(s).start()

                @pl.when(relayed(e))
                def _():
                    send(src, both(c, own), tss.at[slot, 1], rlsem.at[relay_index(e)], flip_tp, 0, flip_rep)

                @pl.when(e >= RELAY_LAG)
                def _():
                    relay(e - RELAY_LAG)

            @pl.when(s % 3 == 2)
            def _():
                f = div(s, 3)
                c = mid + f
                own_copy(s).start()
                send(src, both(c, own), tss.at[slot, 0], zsem(f), flip_tp, 0, rep)
                send(src, both(c, own), tss.at[slot, 1], xsem(f), tp, 0, flip_rep)

        def relay(e):
            @pl.when(relayed(e))
            def _():
                c = chunk_of(e)
                sem = rlsem.at[relay_index(e)]
                wait(both(c, dia), sem)
                send(both(c, dia), both(c, dia), ss.at[0, div(e, chunks)], sem, tp, 1, rep)

        def wait_sent(s):
            slot = s % STAGE_SLOTS
            is_mid = s % 3 == 2
            wait(stage.at[slot], tss.at[slot, 0])

            @pl.when(is_mid | relayed(2 * (s // 3) + s % 3))
            def _():
                wait(stage.at[slot], tss.at[slot, 1])

        def own_stage(f):
            c = mid + f
            send(both(c, own), both(c, own), ss.at[1, 0], zsem(f), flip_tp, 0, rep)
            send(both(c, own), both(c, own), ss.at[1, 1], xsem(f), tp, 0, flip_rep)

        def n_stage(f):
            c = mid + f
            wait(both(c, znb), zsem(f))
            wait(both(c, xnb), xsem(f))

            @pl.when(mod(f, 2) == 0)
            def _():
                send(both(c, znb), both(c, znb), ss.at[2, div(f, chunks)], dsem(f), tp, 0, flip_rep)

            @pl.when(mod(f, 2) == 1)
            def _():
                send(both(c, xnb), both(c, xnb), ss.at[3, div(f, chunks)], dsem(f), flip_tp, 0, rep)

        def d_stage(f):
            c = mid + f
            wait(both(c, dia), dsem(f))

            @pl.when(f < mid)
            def _():
                own_copy(3 * f + 2).wait()

            send(core_half(c, k), core_half(c, k), ss.at[4, div(f, chunks)], sb_mid(f), tp, 0, sib_rep)

        for s in range(LOAD_SLOTS - 1):
            loads(s)

        def body(s, _):
            @pl.when(s + LOAD_SLOTS - 1 < steps)
            def _():
                loads(s + LOAD_SLOTS - 1)

            slot, lslot = s % STAGE_SLOTS, mod(s, LOAD_SLOTS)
            wait(fin.at[lslot], lsem.at[lslot])

            @pl.when(s >= STAGE_SLOTS)
            def _():
                wait_sent(s - STAGE_SLOTS)

                @pl.when(gathered_too(s - STAGE_SLOTS))
                def _():
                    own_copy(s - STAGE_SLOTS).wait()

            @pl.when(s >= LOAD_SLOTS)
            def _():
                wait_stored(s - LOAD_SLOTS)

            for m in range(2):
                new = fin[lslot, 2 * m] - rate * fin[lslot, 2 * m + 1]
                fnew[lslot, m] = new
                stage[slot, m] = new.astype(jnp.bfloat16)

            @pl.when(s >= 1)
            def _():
                post(s - 1)

            @pl.when(s % 3 == 2)
            def _():
                f = s // 3

                @pl.when(f >= N_LAG)
                def _():
                    n_stage(f - N_LAG)

                @pl.when(f >= D_LAG)
                def _():
                    d_stage(f - D_LAG)

            return 0

        with SC("t_cast"):
            lax.fori_loop(0, steps, body, 0)
        post(steps - 1)
        run(relay, gen - RELAY_LAG, gen)
        run(n_stage, mid - N_LAG, mid)
        run(d_stage, mid - D_LAG, mid)
        for s in range(steps - LOAD_SLOTS, steps):
            wait_stored(s)
        for s in range(steps - STAGE_SLOTS, steps):
            if s % 3 != 2 and mid <= 2 * (s // 3) + s % 3 < mid + chunks:
                own_copy(s).wait()
        for l in range(EARLY):
            sb_wait(mid + l * chunks, chunks, sb_mid(l * chunks))

        load_group(mid, 0, 0)
        per_block = EARLY * groups
        few = (blocks - MORE) * per_block
        n_visits = few + MORE * (per_block + groups)

        def place(t):
            u = t - few
            more = jnp.where(u >= per_block + groups, 1, 0)
            b = jnp.where(t < few, div(t, per_block), blocks - MORE + more)
            return b, jnp.where(t < few, mod(t, per_block), u - more * (per_block + groups))

        def give_back(b):
            send(h.at[b], h.at[blocks + b], hs.at[b], hr.at[b], tp, 1, rep)

        def visit(t, _):
            b, q = place(t)
            g, slot = mod(q, groups), mod(q, 2)
            with SC("t_ld"):
                wait_group(g, slot)

            for fn, after in ((own_stage, 0), (n_stage, 8), (d_stage, 18)):

                @pl.when((t >= after) & (t < after + chunks))
                def _():
                    fn(mid + t - after)

            @pl.when(t == few)
            def _():
                sb_wait(2 * mid, chunks, sb_mid(mid))

            @pl.when(t + 1 < n_visits)
            def _():
                _, nq = place(t + 1)
                ng = mod(nq, groups)
                load_group(first_of(EARLY + div(nq, groups), ng), ng, 1 - slot)

            @pl.when(q == 0)
            def _():
                @pl.when(b > 0)
                def _():
                    give_back(b - 1)

                with SC("t_hw"):
                    wait(h.at[b], hr.at[b])

            with SC("t_mm"):
                group_part(slot, g, b, 0)
            return 0

        lax.fori_loop(0, n_visits, visit, 0)
        run(lambda b: wait(h.at[b], hs.at[b]), 0, blocks - 2)
        give_back(blocks - 1)

        def relay_out(i, _):
            @pl.when(i < n_relay)
            def _():
                wait(rin.at[i], rsem.at[0, i])
                send(rin.at[i], rx.at[i], psem.at[0, 0], rsem.at[1, i], flip_tp, 0, rep)

            @pl.when(i >= 1)
            def _():
                q = i - 1
                wait(rx.at[q], rsem.at[1, q])
                b, j, first = 0, 0, 0
                for rb, n in RELAYED:
                    b = jnp.where(q >= first, rb, b)
                    j = jnp.where(q >= first, q - first, j)
                    first += n
                send(rx.at[q], out.at[piece_rows(flip_tp, b, j)], psem.at[0, 1], osem.at[0], tp, 1, rep)

            return 0

        with SC("t_relay"):
            lax.fori_loop(0, n_relay + 1, relay_out, 0)
        with SC("t_drain"):
            wait(rin, psem.at[0, 0])
            wait(rx, psem.at[0, 1])
        run(wait_sent, steps - STAGE_SLOTS, steps)
        run(lambda b: wait(h.at[b], hs.at[b]), blocks - 2, blocks)
        for l in range(2 * EARLY):
            n = count(l * chunks, (l + 1) * chunks, relayed)
            if n:
                wait(wbuf.at[pl.ds(0, n), :, 0, 0, 0], ss.at[0, l])
        for i in range(2):
            wait(wbuf.at[pl.ds(0, chunks), :, 0, 0, 0], ss.at[1, i])
        for l in range(EARLY + 1):
            for m in range(2):
                n = count(l * chunks, (l + 1) * chunks, lambda f: f % 2 == m)
                wait(wbuf.at[pl.ds(0, n), :, 0, 0, 0], ss.at[2 + m, l])
            wait(wbuf.at[pl.ds(0, chunks), :, :, 0], ss.at[4, l])

    @pl.when(side == 1)
    def _():
        def y_stage(e):
            c, l = chunk_of(e), div(e, chunks)
            wait(both(c, own), ysem.at[e])
            send(both(c, own), both(c, own), ss.at[0, l], zsem(e), flip_tp, 1, rep)
            send(both(c, own), both(c, own), ss.at[1, l], xsem(e), tp, 1, flip_rep)

        def n_stage(e):
            c, l = chunk_of(e), div(e, chunks)
            wait(both(c, znb), zsem(e))
            wait(both(c, xnb), xsem(e))
            direct = jnp.logical_not(relayed(e))

            @pl.when(direct & jnp.logical_not(by_z(e)))
            def _():
                send(both(c, znb), both(c, znb), ss.at[2, l], dsem(e), tp, 1, flip_rep)

            @pl.when(direct & by_z(e))
            def _():
                send(both(c, xnb), both(c, xnb), ss.at[3, l], dsem(e), flip_tp, 1, rep)

        def d_stage(e):
            c = chunk_of(e)

            @pl.when(relayed(e))
            def _():
                wait(both(c, dia), rlsem.at[relay_index(e)])

            @pl.when(jnp.logical_not(relayed(e)))
            def _():
                wait(both(c, dia), dsem(e))

            send(core_half(c, k), core_half(c, k), ss.at[4, div(e, chunks)], sb_of(e), tp, 1, sib_rep)

        turn = EARLY * groups * blocks

        def front(i, t):
            a, s1, jump, s2 = FRONTS[i]
            late = 16 * jump + s1 * turn + s2 * (t - turn)
            return jnp.minimum(gen, a + (jnp.where(t <= turn, s1 * t, late) >> 4))

        def pload(b):
            rows = pl.ds(pl.multiple_of(tp * my_rows + b * BLOCK, BLOCK), BLOCK)
            return pltpu.make_async_copy(prompts.at[rows], rows_buf.at[b % 2], iosem.at[b % 2])

        with SC("pro_h"):
          pload(0).start()
        for b in range(blocks):
            if b + 1 < blocks:
                pload(b + 1).start()
            pload(b).wait()
            for j in range(pieces):
                h[b, :, pl.ds(j * PIECE, PIECE)] = rows_buf[b % 2, pl.ds(j * PIECE, PIECE), :].T

        n_pro = FRONTS[0][0]
        for e in range(n_pro):
            y_stage(e)
            for i, fn in ((1, n_stage), (2, d_stage)):
                if e >= n_pro - FRONTS[i][0]:
                    fn(e - (n_pro - FRONTS[i][0]))
        sb_wait(0, lead, sbsem.at[0])
        load_group(0, 0, 0)

        def put(b, j):
            src = rows_buf.at[mod(b, 2), pl.ds(j * PIECE, PIECE), :]
            rows = piece_rows(tp, b, j)
            pltpu.make_async_copy(src, out.at[rows], psem.at[mod(b, 2), 0]).start()
            n, i, first = 0, 0, 0
            for rb, m in RELAYED:
                n = jnp.where(b == rb, m, n)
                i = jnp.where(b == rb, first + min(j, m - 1), i)
                first += m

            @pl.when(j < n)
            def _():
                send(src, rin.at[i], psem.at[mod(b, 2), 1], rsem.at[0, i], tp, 0, rep)

            @pl.when(j >= n)
            def _():
                send(src, out.at[rows], psem.at[mod(b, 2), 1], osem.at[0], flip_tp, 1, rep)

        def put_wait(b):
            for i in range(2):
                wait(rows_buf.at[mod(b, 2)], psem.at[mod(b, 2), i])

        n_rest = groups - 1
        wide = turn - n_rest * blocks
        n_first = blocks - MORE
        n_tasks = n_first + blocks
        paired = FIRST_LATE + 2 * (n_first - FIRST_LATE)
        first_late, last_late = 2 * EARLY, 2 * EARLY + 1

        def late_task(q):
            u = q - FIRST_LATE
            in_pairs = (q >= FIRST_LATE) & (q < paired)
            last = jnp.where(in_pairs, (u & 1) == 0, q >= paired)
            j = u >> 1
            b = jnp.where(in_pairs, jnp.where(last, j, j + FIRST_LATE), jnp.where(q < FIRST_LATE, q, q - n_first))
            return jnp.where(last, last_late, first_late), b

        def rest(t):
            u = t - wide
            b = (u * (128 // n_rest + 1)) >> 7
            return b, 1 + u - n_rest * b

        def give(b):
            send(h.at[b], h.at[b], hs.at[b], hr.at[b], tp, 0, rep)

        def forward(t):
            for i, fn in enumerate((y_stage, n_stage, d_stage)):
                with SC("fw" + "ynd"[i]):
                    run(fn, front(i, t), front(i, t + 1))

        def early_visit(t, _):
            split = t >= wide
            rb, rg = rest(t)
            l = jnp.where(split, EARLY - 1, div(t, groups * blocks))
            g = jnp.where(split, rg, mod(div(t, blocks), groups))
            b = jnp.where(split, rb, mod(t, blocks))
            slot = mod(jnp.where(split, t - wide + 1, div(t, blocks)), 2)

            @pl.when(split | (b == 0))
            def _():
                wait_group(g, slot)

            forward(t)

            @pl.when((t > wide) & (rg == 1))
            def _():
                give(rb - 1)

            @pl.when((t < wide) & (b == blocks // 2))
            def _():
                c0 = first_of(l, g) + width_of(g)
                ng = mod(g + 1, groups)
                sem = sb_of(c0)

                @pl.when(ng == 0)
                def _():
                    sb_wait(c0, lead, sem)

                @pl.when(ng > 0)
                def _():
                    sb_wait(c0, GROUP, sem)

                load_group(c0, ng, 1 - slot)

            @pl.when(t == wide)
            def _():
                for g_ in range(2, groups):
                    c0 = (EARLY - 1) * chunks + lead + (g_ - 1) * GROUP
                    sb_wait(c0, GROUP, sb_of(c0))

            @pl.when(split & (t + 1 < turn))
            def _():
                _, ng = rest(t + 1)
                load_group(first_of(EARLY - 1, ng), ng, 1 - slot)

            @pl.when(t == turn - 1)
            def _():
                sb_wait(2 * mid, chunks, sb_of(mid))
                load_group(2 * mid, 0, 1 - slot)

            with SC("mm"):
                group_part(slot, g, b, b)
            return 0

        def late_visit(u, _):
            l, b = late_task(div(u, groups))
            g = mod(u, groups)
            slot = mod(u + n_rest * blocks + 1, 2)
            hb = blocks + b
            with SC("ld"):
                wait_group(g, slot)

            @pl.when(u < FIRST_LATE * groups)
            def _():
                forward(turn + u)

                @pl.when(u == 0)
                def _():
                    give(blocks - 1)

                @pl.when(u == FIRST_LATE * groups - 1)
                def _():
                    for i, fn in enumerate((y_stage, n_stage, d_stage)):
                        run(fn, front(i, turn + u + 1), gen)
                    sb_wait(2 * mid + chunks, chunks, sb_of(mid + chunks))

            @pl.when(u + 1 < n_tasks * groups)
            def _():
                nl, _ = late_task(div(u + 1, groups))
                ng = mod(u + 1, groups)
                load_group(first_of(nl, ng), ng, 1 - slot)

            @pl.when((g == 0) & ((l == first_late) | (b >= n_first)))
            def _():
                with SC("hw"):
                    wait(h.at[hb], hr.at[b])

            with SC("mm"):
                group_part(slot, g, hb, b)

            @pl.when((l == last_late) & (g == groups - 1))
            def _():
                @pl.when(b >= 2)
                def _():
                    put_wait(b - 2)

                for j in range(pieces):
                    cols = pl.ds(j * PIECE, PIECE)
                    rows_buf[mod(b, 2), cols, :] = h[hb, :, cols].T
                    if j >= 1:
                        put(b, j - 1)
                put(b, pieces - 1)

            return 0

        lax.fori_loop(0, turn, early_visit, 0)
        lax.fori_loop(0, n_tasks * groups, late_visit, 0)
        with SC("tail_s"):
          for b in range(blocks - 2, blocks):
            put_wait(b)
        run(lambda b: wait(h.at[b], hs.at[b]), 0, blocks)
        with SC("tail_r"):
            wait(out.at[pl.ds(pl.multiple_of(flip_tp * my_rows, BLOCK), my_rows)], osem.at[0])
        for l in range(2 * EARLY):
            for i in range(5):
                if i == 4:
                    wait(wbuf.at[pl.ds(0, chunks), :, :, 0], ss.at[i, l])
                else:
                    kinds = (None, None, lambda e: not relayed(e) and not by_z(e), lambda e: not relayed(e) and by_z(e))
                    n = chunks if i < 2 else count(l * chunks, (l + 1) * chunks, kinds[i])
                    wait(wbuf.at[pl.ds(0, n), :, 0, 0, 0], ss.at[i, l])


def finish_kernel(up, dn, rows, new_up, new_dn, out, buf, zbuf, lsem, ssem, zsem):
    layers = up.shape[0]
    n_rows = rows.shape[0]
    slots, band, hidden = buf.shape
    side = lax.axis_index("side")
    items = [(i, o, l) for l in range(layers) for i, o in ((up, new_up), (dn, new_dn))]
    piece = zbuf.shape[1]
    n_pieces = n_rows // piece
    n_slots = zbuf.shape[0]

    def pipeline(n, n_slots, load, store, zeros):
        for i in range(min(n_slots, n)):
            load(i).start()
        half = n_slots // 2
        done = 0
        for i in range(n):
            load(i).wait()
            store(i).start()
            upto = len(zeros) * (i + 1) // n
            for cp in zeros[done:upto]:
                cp.start()
            done = upto
            nxt = i + half
            if i >= half and nxt < n:
                store(nxt - n_slots).wait()
                load(nxt).start()
        for i in range(max(n - n_slots, 0), n):
            store(i).wait()
        for cp in zeros:
            cp.wait()

    @pl.when(side == 0)
    def _():
        zbuf[0] = jnp.zeros(zbuf.shape[1:], zbuf.dtype)
        zeros = [
            pltpu.make_async_copy(zbuf.at[0], out.at[pl.ds(i * piece, piece)], zsem.at[i]) for i in range(n_pieces)
        ]

        def load(i):
            src, _, l = items[i]
            return pltpu.make_async_copy(src.at[l], buf.at[i % slots], lsem.at[i % slots])

        def store(i):
            _, dst, l = items[i]
            return pltpu.make_async_copy(buf.at[i % slots], dst.at[l], ssem.at[i % slots])

        pipeline(len(items), slots, load, store, zeros)

    @pl.when(side == 1)
    def _():
        buf[0] = jnp.zeros(buf.shape[1:], buf.dtype)
        zeros = [pltpu.make_async_copy(buf.at[0], dst.at[l], zsem.at[i]) for i, (_, dst, l) in enumerate(items)]

        def load(i):
            return pltpu.make_async_copy(rows.at[pl.ds(i * piece, piece)], zbuf.at[i % n_slots], lsem.at[i % n_slots])

        def store(i):
            return pltpu.make_async_copy(zbuf.at[i % n_slots], out.at[pl.ds(i * piece, piece)], ssem.at[i % n_slots])

        pipeline(n_pieces, n_slots, load, store, zeros)


def solution(mesh):
    up_spec = P("side", None, ("rep", "tp"), None)
    down_spec = P("side", None, None, ("rep", "tp"))
    tok_spec = P("side", "rep", None, None)

    def device_step(w_up, w_down, g_up, g_down, learn_rate, prompts):
        layers, band, hidden = w_up.shape[1:]
        n_rows, d = prompts.shape[2:]
        chunks = hidden // UNIT
        total = layers * chunks
        my_rows = n_rows // 2
        blocks, pieces = my_rows // BLOCK, BLOCK // PIECE
        weights = (w_up[0], jnp.swapaxes(w_down[0], 1, 2), g_up[0], jnp.swapaxes(g_down[0], 1, 2))
        smem = pl.BlockSpec(memory_space=pltpu.SMEM)
        hbm = pl.BlockSpec(memory_space=pl.ANY)
        bf16 = jnp.bfloat16
        relay = jax.ShapeDtypeStruct((sum(n for _, n in RELAYED), PIECE, d), bf16)
        new_w = jax.ShapeDtypeStruct((layers, band, hidden), jnp.float32)
        rows = jax.ShapeDtypeStruct((n_rows, d), bf16)
        rows_mid, up_mid, dn_mid, _, _, _ = pl.pallas_call(
            sync_kernel,
            name="sync_and_forward",
            out_shape=(
                rows,
                new_w,
                new_w,
                jax.ShapeDtypeStruct((total, 2, 2, 2, 2, band, UNIT), bf16),
                relay,
                relay,
            ),
            in_specs=[smem] + [hbm] * 5,
            out_specs=(hbm,) * 6,
            scratch_shapes=[
                pltpu.VMEM((2 * blocks, d, BLOCK), bf16),
                pltpu.VMEM((blocks, d, BLOCK), jnp.float32),
                pltpu.VMEM((2, GROUP, 2, 2, 2, 2, band, UNIT), bf16),
                pltpu.VMEM((LOAD_SLOTS, 4, band, UNIT), jnp.float32),
                pltpu.VMEM((LOAD_SLOTS, 2, band, UNIT), jnp.float32),
                pltpu.VMEM((STAGE_SLOTS, 2, band, UNIT), bf16),
                pltpu.VMEM((2, BLOCK, d), bf16),
                pltpu.SemaphoreType.DMA((2 * EARLY * chunks,)),
                pltpu.SemaphoreType.DMA((3, RING)),
                pltpu.SemaphoreType.DMA((EARLY * chunks // 6 + chunks // 3 + 1,)),
                pltpu.SemaphoreType.DMA((EARLY * (-(-chunks // GROUP)) + 2 * EARLY + 1,)),
                pltpu.SemaphoreType.DMA((5, 2 * EARLY)),
                pltpu.SemaphoreType.DMA((LOAD_SLOTS,)),
                pltpu.SemaphoreType.DMA((LOAD_SLOTS,)),
                pltpu.SemaphoreType.DMA((2,)),
                pltpu.SemaphoreType.DMA((STAGE_SLOTS, 2)),
                pltpu.SemaphoreType.DMA((STAGE_SLOTS,)),
                pltpu.SemaphoreType.DMA((2,)),
                pltpu.SemaphoreType.DMA((2, 2)),
                pltpu.SemaphoreType.DMA((1,)),
                pltpu.SemaphoreType.DMA((2, sum(n for _, n in RELAYED))),
                pltpu.SemaphoreType.DMA((blocks,)),
                pltpu.SemaphoreType.DMA((blocks,)),
            ],
            compiler_params=pltpu.CompilerParams(
                collective_id=0, has_side_effects=True, vmem_limit_bytes=60 * 1024 * 1024
            ),
        )(learn_rate, *weights, prompts[0, 0])
        new_up, new_dn, gen_out = pl.pallas_call(
            finish_kernel,
            name="write_outputs",
            out_shape=(new_w, new_w, rows),
            in_specs=[hbm] * 3,
            out_specs=(hbm,) * 3,
            scratch_shapes=[
                pltpu.VMEM((8, band, hidden), jnp.float32),
                pltpu.VMEM((8, n_rows // 16, d), bf16),
                pltpu.SemaphoreType.DMA((8,)),
                pltpu.SemaphoreType.DMA((8,)),
                pltpu.SemaphoreType.DMA((max(16, 2 * layers),)),
            ],
            compiler_params=pltpu.CompilerParams(vmem_limit_bytes=62 * 1024 * 1024),
        )(up_mid, dn_mid, rows_mid)
        return new_up[None], jnp.swapaxes(new_dn, 1, 2)[None], gen_out[None, None]

    return jax.shard_map(
        device_step,
        mesh=mesh,
        in_specs=(up_spec, down_spec, up_spec, down_spec, P("side"), tok_spec),
        out_specs=(up_spec, down_spec, tok_spec),
        check_vma=False,
    )
```

```python
import jax
import jax.numpy as jnp
from jax import lax
from jax.experimental import pallas as pl
from jax.experimental.pallas import tpu as pltpu
from jax.sharding import PartitionSpec as P

MESH = pl.DeviceIdType.MESH
SC = jax.named_scope
UNIT = 256
GROUP = 5
BLOCK = 512
PIECE = 128
EARLY = 2
LOAD_SLOTS = 4
STAGE_SLOTS = 36
RING = 32
N_LAG, D_LAG = 3, 6
RELAY_LAG = 4
FIRST_LATE = 3
MORE = 2
RELAYED = ((4, 2), (5, 2), (6, 2))
FRONTS = ((10, 15, 1, 40), (8, 14, 1, 44), (6, 13, 3, 24))
GELU_A = 0.7978845608028654
GELU_B = 0.7978845608028654 * 0.044715


def div(a, n):
    if isinstance(a, int):
        return a // n
    if n & (n - 1) == 0:
        return a >> (n.bit_length() - 1)
    return (a * ((1 << 16) // n + 1)) >> 16


def mod(a, n):
    return a - n * div(a, n)


def gelu(a):
    return a * (0.5 * jnp.tanh(a * (GELU_A + GELU_B * (a * a))) + 0.5)


def sync_kernel(
    rate_ref, w_up, w_dn, g_up, g_dn, prompts, out, nu, nd, wbuf, rin, rx,
    h, p, wv, fin, fnew, stage, rows_buf,
    ysem, rs, rlsem, sbsem, ss, lsem, stsem, fsem, tss, csem, iosem, psem, osem, rsem, hs, hr,
):
    layers, band, hidden = w_up.shape
    chunks = hidden // UNIT
    n_relay = sum(n for _, n in RELAYED)
    groups = -(-chunks // GROUP)
    lead = chunks - (groups - 1) * GROUP
    mid = EARLY * chunks
    gen = 2 * mid
    n_rows, d = out.shape
    my_rows = n_rows // 2
    blocks = my_rows // BLOCK
    pieces = BLOCK // PIECE

    tp = lax.axis_index("tp")
    side = lax.axis_index("side")
    rep = lax.axis_index("rep")
    x, k = rep // 2, rep % 2
    flip_tp = 1 - tp
    flip_rep = (1 - x) * 2 + k
    sib_rep = x * 2 + (1 - k)

    own, znb, xnb, dia = (x, tp), (x, flip_tp), (1 - x, tp), (1 - x, flip_tp)

    def both(c, b):
        return wbuf.at[c, :, b[0], k, b[1]]

    def core_half(c, core):
        return wbuf.at[c, :, :, core]

    def chunk_of(e):
        return e + jnp.where(e >= mid, mid, 0)

    def relayed(e):
        return ((mod(e, 6) == 5) & (e < mid)) | ((mod(e, 3) == 2) & (e >= mid + chunks))

    def by_z(e):
        return ((mod(div(e, 6) + mod(e, 6), 2) == 1) & (e < mid + chunks)) | ((mod(e, 3) == 1) & (e >= mid + chunks))

    def count(e0, e1, fn):
        return sum(1 for e in range(e0, e1) if fn(e))

    n_early = count(0, mid, relayed)

    def relay_index(e):
        return jnp.where(e < mid, div(e, 6), n_early + div(e - mid - chunks, 3))

    def zsem(e):
        return rs.at[0, mod(e, RING)]

    def xsem(e):
        return rs.at[1, mod(e, RING)]

    def dsem(e):
        return rs.at[2, mod(e, RING)]

    def sb_of(e):
        l = div(e, chunks)
        j = e - l * chunks
        g = jnp.where(j < lead, 0, 1 + div(j - lead, GROUP))
        return sbsem.at[jnp.where(e < mid, l * groups + g, EARLY * groups + l - EARLY)]

    def sb_mid(f):
        return sbsem.at[EARLY * groups + EARLY + div(f, chunks)]

    def send(src, dst, ssem, rsem_, t, s, r):
        pltpu.make_async_remote_copy(
            src_ref=src, dst_ref=dst, send_sem=ssem, recv_sem=rsem_,
            device_id={"tp": t, "side": s, "rep": r}, device_id_type=MESH,
        ).start()

    def wait(ref, sem):
        pltpu.make_async_copy(ref, ref, sem).wait()

    def run(fn, lo, hi):
        def body(c, _):
            fn(c)
            return 0

        lax.fori_loop(lo, hi, body, 0)

    def piece_rows(t, b, j):
        return pl.ds(pl.multiple_of(t * my_rows + b * BLOCK + j * PIECE, PIECE), PIECE)

    def sb_wait(c0, width, sem):
        wait(wbuf.at[pl.ds(c0, width), :, :, 1 - k], sem)

    def load_group(c0, g, slot):
        def load(j):
            pltpu.make_async_copy(wbuf.at[c0 + j], wv.at[slot, j], fsem.at[slot]).start()

        for j in range(lead):
            load(j)

        @pl.when(g > 0)
        def _():
            for j in range(lead, GROUP):
                load(j)

    def wait_group(g, slot):
        @pl.when(g == 0)
        def _():
            wait(wv.at[slot, pl.ds(0, lead)], fsem.at[slot])

        @pl.when(g > 0)
        def _():
            wait(wv.at[slot], fsem.at[slot])

    def width_of(g):
        return jnp.where(g == 0, lead, GROUP)

    def first_of(l, g):
        return l * chunks + jnp.where(g == 0, 0, lead + (g - 1) * GROUP)

    def matmuls(slot, hb, width):
        def weight(j, m):
            return wv[slot, j, m].reshape(d, UNIT)

        rows = h[hb]
        acts = []
        for j in range(width):
            a = lax.dot_general(weight(j, 0), rows, (((0,), (0,)), ((), ())), preferred_element_type=jnp.float32)
            acts.append(gelu(a).astype(jnp.bfloat16))
        down = jnp.concatenate([weight(j, 1) for j in range(width)], axis=1)
        return jnp.dot(down, jnp.concatenate(acts, axis=0), preferred_element_type=jnp.float32)

    def group_part(slot, g, hb, pb):
        @pl.when(g == 0)
        def _():
            p[pb] = matmuls(slot, hb, lead)

        @pl.when((g > 0) & (g < groups - 1))
        def _():
            p[pb] = p[pb] + matmuls(slot, hb, GROUP)

        @pl.when(g == groups - 1)
        def _():
            s = p[pb] + matmuls(slot, hb, GROUP)
            h[hb] = (h[hb].astype(jnp.float32) + s).astype(jnp.bfloat16)

    parts = ((w_up, g_up, nu), (w_dn, g_dn, nd))
    steps = gen + mid

    def chunk_at(s):
        return jnp.where(mod(s, 3) == 2, mid + div(s, 3), chunk_of(2 * div(s, 3) + mod(s, 3)))

    def cols_of(c):
        return div(c, chunks), pl.ds(pl.multiple_of(mod(c, chunks) * UNIT, UNIT), UNIT)

    def loads(s):
        l, cols = cols_of(chunk_at(s))
        slot = mod(s, LOAD_SLOTS)
        for m in range(2):
            for i, r in enumerate(parts[m][:2]):
                pltpu.make_async_copy(r.at[l, :, cols], fin.at[slot, 2 * m + i], lsem.at[slot]).start()

    def cast(s):
        slot, lslot = mod(s, STAGE_SLOTS), mod(s, LOAD_SLOTS)
        wait(fin.at[lslot], lsem.at[lslot])
        rate = rate_ref[0]
        for m in range(2):
            new = fin[lslot, 2 * m] - rate * fin[lslot, 2 * m + 1]
            fnew[lslot, m] = new
            stage[slot, m] = new.astype(jnp.bfloat16)

    @pl.when(side == 0)
    def _():
        for s in range(LOAD_SLOTS):
            loads(s)
        cast(0)

    barrier = pltpu.get_barrier_semaphore()
    peers = [(tp, 1 - side, rep)] + [
        (t, side, r) for t, r in ((flip_tp, rep), (tp, flip_rep), (flip_tp, flip_rep), (tp, sib_rep))
    ]
    for t, s_, r in peers:
        pl.semaphore_signal(
            barrier, inc=1, device_id={"tp": t, "side": s_, "rep": r}, device_id_type=MESH
        )
    with SC("bar"):
        pl.semaphore_wait(barrier, len(peers))

    @pl.when(side == 0)
    def _():
        def stores(s):
            l, cols = cols_of(chunk_at(s))
            slot = mod(s, LOAD_SLOTS)
            for m in range(2):
                pltpu.make_async_copy(fnew.at[slot, m], parts[m][2].at[l, :, cols], stsem.at[slot]).start()

        def wait_stored(s):
            slot = mod(s, LOAD_SLOTS)
            wait(fnew.at[slot], stsem.at[slot])

        def own_copy(s):
            slot = s % STAGE_SLOTS
            return pltpu.make_async_copy(stage.at[slot], both(chunk_at(s), own), csem.at[slot])

        def gathered_too(s):
            e = 2 * (s // 3) + s % 3
            return (s % 3 != 2) & (e >= mid) & (e < mid + chunks)

        def post(s):
            slot = s % STAGE_SLOTS
            src = stage.at[slot]
            stores(s)

            @pl.when(s % 3 != 2)
            def _():
                e = 2 * (s // 3) + s % 3
                c = chunk_of(e)
                send(src, both(c, own), tss.at[slot, 0], ysem.at[e], tp, 1, rep)

                @pl.when(gathered_too(s))
                def _():
                    own_copy(s).start()

                @pl.when(relayed(e))
                def _():
                    send(src, both(c, own), tss.at[slot, 1], rlsem.at[relay_index(e)], flip_tp, 0, flip_rep)

                @pl.when(e >= RELAY_LAG)
                def _():
                    relay(e - RELAY_LAG)

            @pl.when(s % 3 == 2)
            def _():
                f = div(s, 3)
                c = mid + f
                own_copy(s).start()
                send(src, both(c, own), tss.at[slot, 0], zsem(f), flip_tp, 0, rep)
                send(src, both(c, own), tss.at[slot, 1], xsem(f), tp, 0, flip_rep)

        def relay(e):
            @pl.when(relayed(e))
            def _():
                c = chunk_of(e)
                sem = rlsem.at[relay_index(e)]
                wait(both(c, dia), sem)
                send(both(c, dia), both(c, dia), ss.at[0, div(e, chunks)], sem, tp, 1, rep)

        def wait_sent(s):
            slot = s % STAGE_SLOTS
            is_mid = s % 3 == 2
            wait(stage.at[slot], tss.at[slot, 0])

            @pl.when(is_mid | relayed(2 * (s // 3) + s % 3))
            def _():
                wait(stage.at[slot], tss.at[slot, 1])

        def own_stage(f):
            c = mid + f
            send(both(c, own), both(c, own), ss.at[1, 0], zsem(f), flip_tp, 0, rep)
            send(both(c, own), both(c, own), ss.at[1, 1], xsem(f), tp, 0, flip_rep)

        def n_stage(f):
            c = mid + f
            wait(both(c, znb), zsem(f))
            wait(both(c, xnb), xsem(f))

            @pl.when(mod(f, 2) == 0)
            def _():
                send(both(c, znb), both(c, znb), ss.at[2, div(f, chunks)], dsem(f), tp, 0, flip_rep)

            @pl.when(mod(f, 2) == 1)
            def _():
                send(both(c, xnb), both(c, xnb), ss.at[3, div(f, chunks)], dsem(f), flip_tp, 0, rep)

        def d_stage(f):
            c = mid + f
            wait(both(c, dia), dsem(f))

            @pl.when(f < mid)
            def _():
                own_copy(3 * f + 2).wait()

            send(core_half(c, k), core_half(c, k), ss.at[4, div(f, chunks)], sb_mid(f), tp, 0, sib_rep)

        def body(s, _):
            @pl.when(s + LOAD_SLOTS - 1 < steps)
            def _():
                loads(s + LOAD_SLOTS - 1)

            @pl.when(s >= STAGE_SLOTS)
            def _():
                wait_sent(s - STAGE_SLOTS)

                @pl.when(gathered_too(s - STAGE_SLOTS))
                def _():
                    own_copy(s - STAGE_SLOTS).wait()

            @pl.when(s >= LOAD_SLOTS)
            def _():
                wait_stored(s - LOAD_SLOTS)

            cast(s)
            @pl.when(s >= 2)
            def _():
                post(s - 1)

            @pl.when(s % 3 == 2)
            def _():
                f = s // 3

                @pl.when(f >= N_LAG)
                def _():
                    n_stage(f - N_LAG)

                @pl.when(f >= D_LAG)
                def _():
                    d_stage(f - D_LAG)

            return 0

        post(0)
        with SC("t_cast"):
            lax.fori_loop(1, steps, body, 0)
        post(steps - 1)
        run(relay, gen - RELAY_LAG, gen)
        run(n_stage, mid - N_LAG, mid)
        run(d_stage, mid - D_LAG, mid)
        for s in range(steps - LOAD_SLOTS, steps):
            wait_stored(s)
        for s in range(steps - STAGE_SLOTS, steps):
            if s % 3 != 2 and mid <= 2 * (s // 3) + s % 3 < mid + chunks:
                own_copy(s).wait()
        for l in range(EARLY):
            sb_wait(mid + l * chunks, chunks, sb_mid(l * chunks))

        load_group(mid, 0, 0)
        per_block = EARLY * groups
        few = (blocks - MORE) * per_block
        n_visits = few + MORE * (per_block + groups)

        def place(t):
            u = t - few
            more = jnp.where(u >= per_block + groups, 1, 0)
            b = jnp.where(t < few, div(t, per_block), blocks - MORE + more)
            return b, jnp.where(t < few, mod(t, per_block), u - more * (per_block + groups))

        def give_back(b):
            send(h.at[b], h.at[blocks + b], hs.at[b], hr.at[b], tp, 1, rep)

        def visit(t, _):
            b, q = place(t)
            g, slot = mod(q, groups), mod(q, 2)
            with SC("t_ld"):
                wait_group(g, slot)

            for fn, after in ((own_stage, 0), (n_stage, 8), (d_stage, 18)):

                @pl.when((t >= after) & (t < after + chunks))
                def _():
                    fn(mid + t - after)

            @pl.when(t == few)
            def _():
                sb_wait(2 * mid, chunks, sb_mid(mid))

            @pl.when(t + 1 < n_visits)
            def _():
                _, nq = place(t + 1)
                ng = mod(nq, groups)
                load_group(first_of(EARLY + div(nq, groups), ng), ng, 1 - slot)

            @pl.when(q == 0)
            def _():
                @pl.when(b > 0)
                def _():
                    give_back(b - 1)

                with SC("t_hw"):
                    wait(h.at[b], hr.at[b])

            with SC("t_mm"):
                group_part(slot, g, b, 0)
            return 0

        lax.fori_loop(0, n_visits, visit, 0)
        run(lambda b: wait(h.at[b], hs.at[b]), 0, blocks - 2)
        give_back(blocks - 1)

        def relay_out(i, _):
            @pl.when(i < n_relay)
            def _():
                wait(rin.at[i], rsem.at[0, i])
                send(rin.at[i], rx.at[i], psem.at[0, 0], rsem.at[1, i], flip_tp, 0, rep)

            @pl.when(i >= 1)
            def _():
                q = i - 1
                wait(rx.at[q], rsem.at[1, q])
                b, j, first = 0, 0, 0
                for rb, n in RELAYED:
                    b = jnp.where(q >= first, rb, b)
                    j = jnp.where(q >= first, q - first, j)
                    first += n
                send(rx.at[q], out.at[piece_rows(flip_tp, b, j)], psem.at[0, 1], osem.at[0], tp, 1, rep)

            return 0

        with SC("t_relay"):
            lax.fori_loop(0, n_relay + 1, relay_out, 0)
        with SC("t_drain"):
            wait(rin, psem.at[0, 0])
            wait(rx, psem.at[0, 1])
        run(wait_sent, steps - STAGE_SLOTS, steps)
        run(lambda b: wait(h.at[b], hs.at[b]), blocks - 2, blocks)
        for l in range(2 * EARLY):
            n = count(l * chunks, (l + 1) * chunks, relayed)
            if n:
                wait(wbuf.at[pl.ds(0, n), :, 0, 0, 0], ss.at[0, l])
        for i in range(2):
            wait(wbuf.at[pl.ds(0, chunks), :, 0, 0, 0], ss.at[1, i])
        for l in range(EARLY + 1):
            for m in range(2):
                n = count(l * chunks, (l + 1) * chunks, lambda f: f % 2 == m)
                wait(wbuf.at[pl.ds(0, n), :, 0, 0, 0], ss.at[2 + m, l])
            wait(wbuf.at[pl.ds(0, chunks), :, :, 0], ss.at[4, l])

    @pl.when(side == 1)
    def _():
        def y_stage(e):
            c, l = chunk_of(e), div(e, chunks)
            wait(both(c, own), ysem.at[e])
            send(both(c, own), both(c, own), ss.at[0, l], zsem(e), flip_tp, 1, rep)
            send(both(c, own), both(c, own), ss.at[1, l], xsem(e), tp, 1, flip_rep)

        def n_stage(e):
            c, l = chunk_of(e), div(e, chunks)
            wait(both(c, znb), zsem(e))
            wait(both(c, xnb), xsem(e))
            direct = jnp.logical_not(relayed(e))

            @pl.when(direct & jnp.logical_not(by_z(e)))
            def _():
                send(both(c, znb), both(c, znb), ss.at[2, l], dsem(e), tp, 1, flip_rep)

            @pl.when(direct & by_z(e))
            def _():
                send(both(c, xnb), both(c, xnb), ss.at[3, l], dsem(e), flip_tp, 1, rep)

        def d_stage(e):
            c = chunk_of(e)

            @pl.when(relayed(e))
            def _():
                wait(both(c, dia), rlsem.at[relay_index(e)])

            @pl.when(jnp.logical_not(relayed(e)))
            def _():
                wait(both(c, dia), dsem(e))

            send(core_half(c, k), core_half(c, k), ss.at[4, div(e, chunks)], sb_of(e), tp, 1, sib_rep)

        turn = EARLY * groups * blocks

        def front(i, t):
            a, s1, jump, s2 = FRONTS[i]
            late = 16 * jump + s1 * turn + s2 * (t - turn)
            return jnp.minimum(gen, a + (jnp.where(t <= turn, s1 * t, late) >> 4))

        def pload(b):
            rows = pl.ds(pl.multiple_of(tp * my_rows + b * BLOCK, BLOCK), BLOCK)
            return pltpu.make_async_copy(prompts.at[rows], rows_buf.at[b % 2], iosem.at[b % 2])

        with SC("pro_h"):
          pload(0).start()
        for b in range(blocks):
            if b + 1 < blocks:
                pload(b + 1).start()
            pload(b).wait()
            for j in range(pieces):
                h[b, :, pl.ds(j * PIECE, PIECE)] = rows_buf[b % 2, pl.ds(j * PIECE, PIECE), :].T

        n_pro = FRONTS[0][0]
        for e in range(n_pro):
            y_stage(e)
            for i, fn in ((1, n_stage), (2, d_stage)):
                if e >= n_pro - FRONTS[i][0]:
                    fn(e - (n_pro - FRONTS[i][0]))
        sb_wait(0, lead, sbsem.at[0])
        load_group(0, 0, 0)

        def put(b, j):
            src = rows_buf.at[mod(b, 2), pl.ds(j * PIECE, PIECE), :]
            rows = piece_rows(tp, b, j)
            pltpu.make_async_copy(src, out.at[rows], psem.at[mod(b, 2), 0]).start()
            n, i, first = 0, 0, 0
            for rb, m in RELAYED:
                n = jnp.where(b == rb, m, n)
                i = jnp.where(b == rb, first + min(j, m - 1), i)
                first += m

            @pl.when(j < n)
            def _():
                send(src, rin.at[i], psem.at[mod(b, 2), 1], rsem.at[0, i], tp, 0, rep)

            @pl.when(j >= n)
            def _():
                send(src, out.at[rows], psem.at[mod(b, 2), 1], osem.at[0], flip_tp, 1, rep)

        def put_wait(b):
            for i in range(2):
                wait(rows_buf.at[mod(b, 2)], psem.at[mod(b, 2), i])

        n_rest = groups - 1
        wide = turn - n_rest * blocks
        n_first = blocks - MORE
        n_tasks = n_first + blocks
        paired = FIRST_LATE + 2 * (n_first - FIRST_LATE)
        first_late, last_late = 2 * EARLY, 2 * EARLY + 1

        def late_task(q):
            u = q - FIRST_LATE
            in_pairs = (q >= FIRST_LATE) & (q < paired)
            last = jnp.where(in_pairs, (u & 1) == 0, q >= paired)
            j = u >> 1
            b = jnp.where(in_pairs, jnp.where(last, j, j + FIRST_LATE), jnp.where(q < FIRST_LATE, q, q - n_first))
            return jnp.where(last, last_late, first_late), b

        def rest(t):
            u = t - wide
            b = (u * (128 // n_rest + 1)) >> 7
            return b, 1 + u - n_rest * b

        def give(b):
            send(h.at[b], h.at[b], hs.at[b], hr.at[b], tp, 0, rep)

        def forward(t):
            for i, fn in enumerate((y_stage, n_stage, d_stage)):
                with SC("fw" + "ynd"[i]):
                    run(fn, front(i, t), front(i, t + 1))

        def early_visit(t, _):
            split = t >= wide
            rb, rg = rest(t)
            l = jnp.where(split, EARLY - 1, div(t, groups * blocks))
            g = jnp.where(split, rg, mod(div(t, blocks), groups))
            b = jnp.where(split, rb, mod(t, blocks))
            slot = mod(jnp.where(split, t - wide + 1, div(t, blocks)), 2)

            @pl.when(split | (b == 0))
            def _():
                wait_group(g, slot)

            forward(t)

            @pl.when((t > wide) & (rg == 1))
            def _():
                give(rb - 1)

            @pl.when((t < wide) & (b == blocks // 2))
            def _():
                c0 = first_of(l, g) + width_of(g)
                ng = mod(g + 1, groups)
                sem = sb_of(c0)

                @pl.when(ng == 0)
                def _():
                    sb_wait(c0, lead, sem)

                @pl.when(ng > 0)
                def _():
                    sb_wait(c0, GROUP, sem)

                load_group(c0, ng, 1 - slot)

            @pl.when(t == wide)
            def _():
                for g_ in range(2, groups):
                    c0 = (EARLY - 1) * chunks + lead + (g_ - 1) * GROUP
                    sb_wait(c0, GROUP, sb_of(c0))

            @pl.when(split & (t + 1 < turn))
            def _():
                _, ng = rest(t + 1)
                load_group(first_of(EARLY - 1, ng), ng, 1 - slot)

            @pl.when(t == turn - 1)
            def _():
                sb_wait(2 * mid, chunks, sb_of(mid))
                load_group(2 * mid, 0, 1 - slot)

            with SC("mm"):
                group_part(slot, g, b, b)
            return 0

        def late_visit(u, _):
            l, b = late_task(div(u, groups))
            g = mod(u, groups)
            slot = mod(u + n_rest * blocks + 1, 2)
            hb = blocks + b
            with SC("ld"):
                wait_group(g, slot)

            @pl.when(u < FIRST_LATE * groups)
            def _():
                forward(turn + u)

                @pl.when(u == 0)
                def _():
                    give(blocks - 1)

                @pl.when(u == FIRST_LATE * groups - 1)
                def _():
                    for i, fn in enumerate((y_stage, n_stage, d_stage)):
                        run(fn, front(i, turn + u + 1), gen)
                    sb_wait(2 * mid + chunks, chunks, sb_of(mid + chunks))

            @pl.when(u + 1 < n_tasks * groups)
            def _():
                nl, _ = late_task(div(u + 1, groups))
                ng = mod(u + 1, groups)
                load_group(first_of(nl, ng), ng, 1 - slot)

            @pl.when((g == 0) & ((l == first_late) | (b >= n_first)))
            def _():
                with SC("hw"):
                    wait(h.at[hb], hr.at[b])

            with SC("mm"):
                group_part(slot, g, hb, b)

            @pl.when((l == last_late) & (g == groups - 1))
            def _():
                @pl.when(b >= 2)
                def _():
                    put_wait(b - 2)

                for j in range(pieces):
                    cols = pl.ds(j * PIECE, PIECE)
                    rows_buf[mod(b, 2), cols, :] = h[hb, :, cols].T
                    if j >= 1:
                        put(b, j - 1)
                put(b, pieces - 1)

            return 0

        lax.fori_loop(0, turn, early_visit, 0)
        lax.fori_loop(0, n_tasks * groups, late_visit, 0)
        with SC("tail_s"):
          for b in range(blocks - 2, blocks):
            put_wait(b)
        run(lambda b: wait(h.at[b], hs.at[b]), 0, blocks)
        with SC("tail_r"):
            wait(out.at[pl.ds(pl.multiple_of(flip_tp * my_rows, BLOCK), my_rows)], osem.at[0])
        for l in range(2 * EARLY):
            for i in range(5):
                if i == 4:
                    wait(wbuf.at[pl.ds(0, chunks), :, :, 0], ss.at[i, l])
                else:
                    kinds = (None, None, lambda e: not relayed(e) and not by_z(e), lambda e: not relayed(e) and by_z(e))
                    n = chunks if i < 2 else count(l * chunks, (l + 1) * chunks, kinds[i])
                    wait(wbuf.at[pl.ds(0, n), :, 0, 0, 0], ss.at[i, l])


def finish_kernel(up, dn, rows, new_up, new_dn, out, buf, zbuf, lsem, ssem, zsem):
    layers = up.shape[0]
    n_rows = rows.shape[0]
    slots, band, hidden = buf.shape
    side = lax.axis_index("side")
    items = [(i, o, l) for l in range(layers) for i, o in ((up, new_up), (dn, new_dn))]
    piece = zbuf.shape[1]
    n_pieces = n_rows // piece
    n_slots = zbuf.shape[0]

    def pipeline(n, n_slots, load, store, zeros):
        for i in range(min(n_slots, n)):
            load(i).start()
        half = n_slots // 2
        done = 0
        for i in range(n):
            load(i).wait()
            store(i).start()
            upto = len(zeros) * (i + 1) // n
            for cp in zeros[done:upto]:
                cp.start()
            done = upto
            nxt = i + half
            if i >= half and nxt < n:
                store(nxt - n_slots).wait()
                load(nxt).start()
        for i in range(max(n - n_slots, 0), n):
            store(i).wait()
        for cp in zeros:
            cp.wait()

    @pl.when(side == 0)
    def _():
        zbuf[0] = jnp.zeros(zbuf.shape[1:], zbuf.dtype)
        zeros = [
            pltpu.make_async_copy(zbuf.at[0], out.at[pl.ds(i * piece, piece)], zsem.at[i]) for i in range(n_pieces)
        ]

        def load(i):
            src, _, l = items[i]
            return pltpu.make_async_copy(src.at[l], buf.at[i % slots], lsem.at[i % slots])

        def store(i):
            _, dst, l = items[i]
            return pltpu.make_async_copy(buf.at[i % slots], dst.at[l], ssem.at[i % slots])

        pipeline(len(items), slots, load, store, zeros)

    @pl.when(side == 1)
    def _():
        buf[0] = jnp.zeros(buf.shape[1:], buf.dtype)
        zeros = [pltpu.make_async_copy(buf.at[0], dst.at[l], zsem.at[i]) for i, (_, dst, l) in enumerate(items)]

        def load(i):
            return pltpu.make_async_copy(rows.at[pl.ds(i * piece, piece)], zbuf.at[i % n_slots], lsem.at[i % n_slots])

        def store(i):
            return pltpu.make_async_copy(zbuf.at[i % n_slots], out.at[pl.ds(i * piece, piece)], ssem.at[i % n_slots])

        pipeline(n_pieces, n_slots, load, store, zeros)


def solution(mesh):
    up_spec = P("side", None, ("rep", "tp"), None)
    down_spec = P("side", None, None, ("rep", "tp"))
    tok_spec = P("side", "rep", None, None)

    def device_step(w_up, w_down, g_up, g_down, learn_rate, prompts):
        layers, band, hidden = w_up.shape[1:]
        n_rows, d = prompts.shape[2:]
        chunks = hidden // UNIT
        total = layers * chunks
        my_rows = n_rows // 2
        blocks, pieces = my_rows // BLOCK, BLOCK // PIECE
        weights = (w_up[0], jnp.swapaxes(w_down[0], 1, 2), g_up[0], jnp.swapaxes(g_down[0], 1, 2))
        smem = pl.BlockSpec(memory_space=pltpu.SMEM)
        hbm = pl.BlockSpec(memory_space=pl.ANY)
        bf16 = jnp.bfloat16
        relay = jax.ShapeDtypeStruct((sum(n for _, n in RELAYED), PIECE, d), bf16)
        new_w = jax.ShapeDtypeStruct((layers, band, hidden), jnp.float32)
        rows = jax.ShapeDtypeStruct((n_rows, d), bf16)
        rows_mid, up_mid, dn_mid, _, _, _ = pl.pallas_call(
            sync_kernel,
            name="sync_and_forward",
            out_shape=(
                rows,
                new_w,
                new_w,
                jax.ShapeDtypeStruct((total, 2, 2, 2, 2, band, UNIT), bf16),
                relay,
                relay,
            ),
            in_specs=[smem] + [hbm] * 5,
            out_specs=(hbm,) * 6,
            scratch_shapes=[
                pltpu.VMEM((2 * blocks, d, BLOCK), bf16),
                pltpu.VMEM((blocks, d, BLOCK), jnp.float32),
                pltpu.VMEM((2, GROUP, 2, 2, 2, 2, band, UNIT), bf16),
                pltpu.VMEM((LOAD_SLOTS, 4, band, UNIT), jnp.float32),
                pltpu.VMEM((LOAD_SLOTS, 2, band, UNIT), jnp.float32),
                pltpu.VMEM((STAGE_SLOTS, 2, band, UNIT), bf16),
                pltpu.VMEM((2, BLOCK, d), bf16),
                pltpu.SemaphoreType.DMA((2 * EARLY * chunks,)),
                pltpu.SemaphoreType.DMA((3, RING)),
                pltpu.SemaphoreType.DMA((EARLY * chunks // 6 + chunks // 3 + 1,)),
                pltpu.SemaphoreType.DMA((EARLY * (-(-chunks // GROUP)) + 2 * EARLY + 1,)),
                pltpu.SemaphoreType.DMA((5, 2 * EARLY)),
                pltpu.SemaphoreType.DMA((LOAD_SLOTS,)),
                pltpu.SemaphoreType.DMA((LOAD_SLOTS,)),
                pltpu.SemaphoreType.DMA((2,)),
                pltpu.SemaphoreType.DMA((STAGE_SLOTS, 2)),
                pltpu.SemaphoreType.DMA((STAGE_SLOTS,)),
                pltpu.SemaphoreType.DMA((2,)),
                pltpu.SemaphoreType.DMA((2, 2)),
                pltpu.SemaphoreType.DMA((1,)),
                pltpu.SemaphoreType.DMA((2, sum(n for _, n in RELAYED))),
                pltpu.SemaphoreType.DMA((blocks,)),
                pltpu.SemaphoreType.DMA((blocks,)),
            ],
            compiler_params=pltpu.CompilerParams(
                collective_id=0, has_side_effects=True, vmem_limit_bytes=60 * 1024 * 1024
            ),
        )(learn_rate, *weights, prompts[0, 0])
        new_up, new_dn, gen_out = pl.pallas_call(
            finish_kernel,
            name="write_outputs",
            out_shape=(new_w, new_w, rows),
            in_specs=[hbm] * 3,
            out_specs=(hbm,) * 3,
            scratch_shapes=[
                pltpu.VMEM((8, band, hidden), jnp.float32),
                pltpu.VMEM((8, n_rows // 16, d), bf16),
                pltpu.SemaphoreType.DMA((8,)),
                pltpu.SemaphoreType.DMA((8,)),
                pltpu.SemaphoreType.DMA((max(16, 2 * layers),)),
            ],
            compiler_params=pltpu.CompilerParams(vmem_limit_bytes=62 * 1024 * 1024),
        )(up_mid, dn_mid, rows_mid)
        return new_up[None], jnp.swapaxes(new_dn, 1, 2)[None], gen_out[None, None]

    return jax.shard_map(
        device_step,
        mesh=mesh,
        in_specs=(up_spec, down_spec, up_spec, down_spec, P("side"), tok_spec),
        out_specs=(up_spec, down_spec, tok_spec),
        check_vma=False,
    )
```

```python
import jax
import jax.numpy as jnp
from jax import lax
from jax.experimental import pallas as pl
from jax.experimental.pallas import tpu as pltpu
from jax.sharding import PartitionSpec as P

MESH = pl.DeviceIdType.MESH
UNIT = 256
GROUP = 5
BLOCK = 512
PIECE = 128
EARLY = 2
LOAD_SLOTS = 4
STAGE_SLOTS = 36
RING = 32
N_LAG, D_LAG = 3, 6
RELAY_LAG = 4
FIRST_LATE = 3
MORE = 2
RELAYED = ((5, 2), (6, 2))
FRONTS = ((10, 15, 1, 40), (8, 14, 1, 44), (6, 13, 3, 24))
GELU_A = 0.7978845608028654
GELU_B = 0.7978845608028654 * 0.044715


def div(a, n):
    if isinstance(a, int):
        return a // n
    if n & (n - 1) == 0:
        return a >> (n.bit_length() - 1)
    return (a * ((1 << 16) // n + 1)) >> 16


def mod(a, n):
    return a - n * div(a, n)


def gelu(a):
    return a * (0.5 * jnp.tanh(a * (GELU_A + GELU_B * (a * a))) + 0.5)


def sync_kernel(
    rate_ref, w_up, w_dn, g_up, g_dn, prompts, out, nu, nd, wbuf, rin, rx,
    h, p, wv, fin, fnew, stage, rows_buf,
    ysem, rs, rlsem, sbsem, ss, lsem, stsem, fsem, tss, csem, iosem, psem, osem, rsem, hs, hr,
):
    layers, band, hidden = w_up.shape
    chunks = hidden // UNIT
    n_relay = sum(n for _, n in RELAYED)
    groups = -(-chunks // GROUP)
    lead = chunks - (groups - 1) * GROUP
    mid = EARLY * chunks
    gen = 2 * mid
    n_rows, d = out.shape
    my_rows = n_rows // 2
    blocks = my_rows // BLOCK
    pieces = BLOCK // PIECE

    tp = lax.axis_index("tp")
    side = lax.axis_index("side")
    rep = lax.axis_index("rep")
    x, k = rep // 2, rep % 2
    flip_tp = 1 - tp
    flip_rep = (1 - x) * 2 + k
    sib_rep = x * 2 + (1 - k)

    own, znb, xnb, dia = (x, tp), (x, flip_tp), (1 - x, tp), (1 - x, flip_tp)

    def both(c, b):
        return wbuf.at[c, :, b[0], k, b[1]]

    def core_half(c, core):
        return wbuf.at[c, :, :, core]

    def chunk_of(e):
        return e + jnp.where(e >= mid, mid, 0)

    def relayed(e):
        return ((mod(e, 6) == 5) & (e < mid)) | ((mod(e, 3) == 2) & (e >= mid + chunks))

    def by_z(e):
        return ((mod(div(e, 6) + mod(e, 6), 2) == 1) & (e < mid + chunks)) | ((mod(e, 3) == 1) & (e >= mid + chunks))

    def count(e0, e1, fn):
        return sum(1 for e in range(e0, e1) if fn(e))

    n_early = count(0, mid, relayed)

    def relay_index(e):
        return jnp.where(e < mid, div(e, 6), n_early + div(e - mid - chunks, 3))

    def zsem(e):
        return rs.at[0, mod(e, RING)]

    def xsem(e):
        return rs.at[1, mod(e, RING)]

    def dsem(e):
        return rs.at[2, mod(e, RING)]

    def sb_of(e):
        l = div(e, chunks)
        j = e - l * chunks
        g = jnp.where(j < lead, 0, 1 + div(j - lead, GROUP))
        return sbsem.at[jnp.where(e < mid, l * groups + g, EARLY * groups + l - EARLY)]

    def sb_mid(f):
        return sbsem.at[EARLY * groups + EARLY + div(f, chunks)]

    def send(src, dst, ssem, rsem_, t, s, r):
        pltpu.make_async_remote_copy(
            src_ref=src, dst_ref=dst, send_sem=ssem, recv_sem=rsem_,
            device_id={"tp": t, "side": s, "rep": r}, device_id_type=MESH,
        ).start()

    def wait(ref, sem):
        pltpu.make_async_copy(ref, ref, sem).wait()

    def run(fn, lo, hi):
        def body(c, _):
            fn(c)
            return 0

        lax.fori_loop(lo, hi, body, 0)

    def piece_rows(t, b, j):
        return pl.ds(pl.multiple_of(t * my_rows + b * BLOCK + j * PIECE, PIECE), PIECE)

    def sb_wait(c0, width, sem):
        wait(wbuf.at[pl.ds(c0, width), :, :, 1 - k], sem)

    def load_group(c0, g, slot):
        def load(j):
            pltpu.make_async_copy(wbuf.at[c0 + j], wv.at[slot, j], fsem.at[slot]).start()

        for j in range(lead):
            load(j)

        @pl.when(g > 0)
        def _():
            for j in range(lead, GROUP):
                load(j)

    def wait_group(g, slot):
        @pl.when(g == 0)
        def _():
            wait(wv.at[slot, pl.ds(0, lead)], fsem.at[slot])

        @pl.when(g > 0)
        def _():
            wait(wv.at[slot], fsem.at[slot])

    def width_of(g):
        return jnp.where(g == 0, lead, GROUP)

    def first_of(l, g):
        return l * chunks + jnp.where(g == 0, 0, lead + (g - 1) * GROUP)

    def matmuls(slot, rows, width):
        def weight(j, m):
            return wv[slot, j, m].reshape(d, UNIT)

        acts = []
        for j in range(width):
            a = lax.dot_general(weight(j, 0), rows, (((0,), (0,)), ((), ())), preferred_element_type=jnp.float32)
            acts.append(gelu(a).astype(jnp.bfloat16))
        down = jnp.concatenate([weight(j, 1) for j in range(width)], axis=1)
        return jnp.dot(down, jnp.concatenate(acts, axis=0), preferred_element_type=jnp.float32)

    def group_part(slot, g, hb, pb):
        @pl.when(g == 0)
        def _():
            p[pb] = matmuls(slot, h[hb], lead)

        @pl.when((g > 0) & (g < groups - 1))
        def _():
            p[pb] = p[pb] + matmuls(slot, h[hb], GROUP)

        @pl.when(g == groups - 1)
        def _():
            s = p[pb] + matmuls(slot, h[hb], GROUP)
            h[hb] = (h[hb].astype(jnp.float32) + s).astype(jnp.bfloat16)

    parts = ((w_up, g_up, nu), (w_dn, g_dn, nd))
    steps = gen + mid

    def chunk_at(s):
        return jnp.where(mod(s, 3) == 2, mid + div(s, 3), chunk_of(2 * div(s, 3) + mod(s, 3)))

    def cols_of(c):
        return div(c, chunks), pl.ds(pl.multiple_of(mod(c, chunks) * UNIT, UNIT), UNIT)

    def loads(s):
        l, cols = cols_of(chunk_at(s))
        slot = mod(s, LOAD_SLOTS)
        for m in range(2):
            for i, r in enumerate(parts[m][:2]):
                pltpu.make_async_copy(r.at[l, :, cols], fin.at[slot, 2 * m + i], lsem.at[slot]).start()

    def cast(s):
        slot, lslot = mod(s, STAGE_SLOTS), mod(s, LOAD_SLOTS)
        wait(fin.at[lslot], lsem.at[lslot])
        rate = rate_ref[0]
        for m in range(2):
            new = fin[lslot, 2 * m] - rate * fin[lslot, 2 * m + 1]
            fnew[lslot, m] = new
            stage[slot, m] = new.astype(jnp.bfloat16)

    @pl.when(side == 0)
    def _():
        for s in range(LOAD_SLOTS):
            loads(s)
        cast(0)

    barrier = pltpu.get_barrier_semaphore()
    peers = [(tp, 1 - side, rep)] + [
        (t, side, r) for t, r in ((flip_tp, rep), (tp, flip_rep), (flip_tp, flip_rep), (tp, sib_rep))
    ]
    for t, s_, r in peers:
        pl.semaphore_signal(
            barrier, inc=1, device_id={"tp": t, "side": s_, "rep": r}, device_id_type=MESH
        )
    pl.semaphore_wait(barrier, len(peers))

    @pl.when(side == 0)
    def _():
        def stores(s):
            l, cols = cols_of(chunk_at(s))
            slot = mod(s, LOAD_SLOTS)
            for m in range(2):
                pltpu.make_async_copy(fnew.at[slot, m], parts[m][2].at[l, :, cols], stsem.at[slot]).start()

        def wait_stored(s):
            slot = mod(s, LOAD_SLOTS)
            wait(fnew.at[slot], stsem.at[slot])

        def own_copy(s):
            slot = s % STAGE_SLOTS
            return pltpu.make_async_copy(stage.at[slot], both(chunk_at(s), own), csem.at[slot])

        def gathered_too(s):
            e = 2 * (s // 3) + s % 3
            return (s % 3 != 2) & (e >= mid) & (e < mid + chunks)

        def post(s):
            slot = s % STAGE_SLOTS
            src = stage.at[slot]
            stores(s)

            @pl.when(s % 3 != 2)
            def _():
                e = 2 * (s // 3) + s % 3
                c = chunk_of(e)
                send(src, both(c, own), tss.at[slot, 0], ysem.at[e], tp, 1, rep)

                @pl.when(gathered_too(s))
                def _():
                    own_copy(s).start()

                @pl.when(relayed(e))
                def _():
                    send(src, both(c, own), tss.at[slot, 1], rlsem.at[relay_index(e)], flip_tp, 0, flip_rep)

                @pl.when(e >= RELAY_LAG)
                def _():
                    relay(e - RELAY_LAG)

            @pl.when(s % 3 == 2)
            def _():
                f = div(s, 3)
                c = mid + f
                own_copy(s).start()
                send(src, both(c, own), tss.at[slot, 0], zsem(f), flip_tp, 0, rep)
                send(src, both(c, own), tss.at[slot, 1], xsem(f), tp, 0, flip_rep)

        def relay(e):
            @pl.when(relayed(e))
            def _():
                c = chunk_of(e)
                sem = rlsem.at[relay_index(e)]
                wait(both(c, dia), sem)
                send(both(c, dia), both(c, dia), ss.at[0, div(e, chunks)], sem, tp, 1, rep)

        def wait_sent(s):
            slot = s % STAGE_SLOTS
            is_mid = s % 3 == 2
            wait(stage.at[slot], tss.at[slot, 0])

            @pl.when(is_mid | relayed(2 * (s // 3) + s % 3))
            def _():
                wait(stage.at[slot], tss.at[slot, 1])

        def own_stage(f):
            c = mid + f
            send(both(c, own), both(c, own), ss.at[1, 0], zsem(f), flip_tp, 0, rep)
            send(both(c, own), both(c, own), ss.at[1, 1], xsem(f), tp, 0, flip_rep)

        def n_stage(f):
            c = mid + f
            wait(both(c, znb), zsem(f))
            wait(both(c, xnb), xsem(f))

            @pl.when(mod(f, 2) == 0)
            def _():
                send(both(c, znb), both(c, znb), ss.at[2, div(f, chunks)], dsem(f), tp, 0, flip_rep)

            @pl.when(mod(f, 2) == 1)
            def _():
                send(both(c, xnb), both(c, xnb), ss.at[3, div(f, chunks)], dsem(f), flip_tp, 0, rep)

        def d_stage(f):
            c = mid + f
            wait(both(c, dia), dsem(f))

            @pl.when(f < mid)
            def _():
                own_copy(3 * f + 2).wait()

            send(core_half(c, k), core_half(c, k), ss.at[4, div(f, chunks)], sb_mid(f), tp, 0, sib_rep)

        def body(s, _):
            @pl.when(s + LOAD_SLOTS - 1 < steps)
            def _():
                loads(s + LOAD_SLOTS - 1)

            @pl.when(s >= STAGE_SLOTS)
            def _():
                wait_sent(s - STAGE_SLOTS)

                @pl.when(gathered_too(s - STAGE_SLOTS))
                def _():
                    own_copy(s - STAGE_SLOTS).wait()

            @pl.when(s >= LOAD_SLOTS)
            def _():
                wait_stored(s - LOAD_SLOTS)

            cast(s)
            @pl.when(s >= 2)
            def _():
                post(s - 1)

            @pl.when(s % 3 == 2)
            def _():
                f = s // 3

                @pl.when(f >= N_LAG)
                def _():
                    n_stage(f - N_LAG)

                @pl.when(f >= D_LAG)
                def _():
                    d_stage(f - D_LAG)

            return 0

        post(0)
        lax.fori_loop(1, steps, body, 0)
        post(steps - 1)
        run(relay, gen - RELAY_LAG, gen)
        run(n_stage, mid - N_LAG, mid)
        run(d_stage, mid - D_LAG, mid)
        for s in range(steps - LOAD_SLOTS, steps):
            wait_stored(s)
        for s in range(steps - STAGE_SLOTS, steps):
            if s % 3 != 2 and mid <= 2 * (s // 3) + s % 3 < mid + chunks:
                own_copy(s).wait()
        for l in range(EARLY):
            sb_wait(mid + l * chunks, chunks, sb_mid(l * chunks))

        load_group(mid, 0, 0)
        per_block = EARLY * groups
        few = (blocks - MORE) * per_block
        n_visits = few + MORE * (per_block + groups)

        def place(t):
            u = t - few
            more = jnp.where(u >= per_block + groups, 1, 0)
            b = jnp.where(t < few, div(t, per_block), blocks - MORE + more)
            return b, jnp.where(t < few, mod(t, per_block), u - more * (per_block + groups))

        def give_back(b):
            send(h.at[b], h.at[blocks + b], hs.at[b], hr.at[b], tp, 1, rep)

        def visit(t, _):
            b, q = place(t)
            g, slot = mod(q, groups), mod(q, 2)
            wait_group(g, slot)

            for fn, after in ((own_stage, 0), (n_stage, 8), (d_stage, 18)):

                @pl.when((t >= after) & (t < after + chunks))
                def _():
                    fn(mid + t - after)

            @pl.when(t == few)
            def _():
                sb_wait(2 * mid, chunks, sb_mid(mid))

            @pl.when(t + 1 < n_visits)
            def _():
                _, nq = place(t + 1)
                ng = mod(nq, groups)
                load_group(first_of(EARLY + div(nq, groups), ng), ng, 1 - slot)

            @pl.when(q == 0)
            def _():
                @pl.when(b > 0)
                def _():
                    give_back(b - 1)

                wait(h.at[b], hr.at[b])

            group_part(slot, g, b, 0)
            return 0

        lax.fori_loop(0, n_visits, visit, 0)
        run(lambda b: wait(h.at[b], hs.at[b]), 0, blocks - 2)
        give_back(blocks - 1)

        def relay_out(i, _):
            @pl.when(i < n_relay)
            def _():
                wait(rin.at[i], rsem.at[0, i])
                send(rin.at[i], rx.at[i], psem.at[0, 0], rsem.at[1, i], flip_tp, 0, rep)

            @pl.when(i >= 1)
            def _():
                q = i - 1
                wait(rx.at[q], rsem.at[1, q])
                b, j, first = 0, 0, 0
                for rb, n in RELAYED:
                    b = jnp.where(q >= first, rb, b)
                    j = jnp.where(q >= first, q - first, j)
                    first += n
                send(rx.at[q], out.at[piece_rows(flip_tp, b, j)], psem.at[0, 1], osem.at[0], tp, 1, rep)

            return 0

        lax.fori_loop(0, n_relay + 1, relay_out, 0)
        wait(rin, psem.at[0, 0])
        wait(rx, psem.at[0, 1])
        run(wait_sent, steps - STAGE_SLOTS, steps)
        run(lambda b: wait(h.at[b], hs.at[b]), blocks - 2, blocks)
        for l in range(2 * EARLY):
            n = count(l * chunks, (l + 1) * chunks, relayed)
            if n:
                wait(wbuf.at[pl.ds(0, n), :, 0, 0, 0], ss.at[0, l])
        for i in range(2):
            wait(wbuf.at[pl.ds(0, chunks), :, 0, 0, 0], ss.at[1, i])
        for l in range(EARLY + 1):
            for m in range(2):
                n = count(l * chunks, (l + 1) * chunks, lambda f: f % 2 == m)
                wait(wbuf.at[pl.ds(0, n), :, 0, 0, 0], ss.at[2 + m, l])
            wait(wbuf.at[pl.ds(0, chunks), :, :, 0], ss.at[4, l])

    @pl.when(side == 1)
    def _():
        def y_stage(e):
            c, l = chunk_of(e), div(e, chunks)
            wait(both(c, own), ysem.at[e])
            send(both(c, own), both(c, own), ss.at[0, l], zsem(e), flip_tp, 1, rep)
            send(both(c, own), both(c, own), ss.at[1, l], xsem(e), tp, 1, flip_rep)

        def n_stage(e):
            c, l = chunk_of(e), div(e, chunks)
            wait(both(c, znb), zsem(e))
            wait(both(c, xnb), xsem(e))
            direct = jnp.logical_not(relayed(e))

            @pl.when(direct & jnp.logical_not(by_z(e)))
            def _():
                send(both(c, znb), both(c, znb), ss.at[2, l], dsem(e), tp, 1, flip_rep)

            @pl.when(direct & by_z(e))
            def _():
                send(both(c, xnb), both(c, xnb), ss.at[3, l], dsem(e), flip_tp, 1, rep)

        def d_stage(e):
            c = chunk_of(e)

            @pl.when(relayed(e))
            def _():
                wait(both(c, dia), rlsem.at[relay_index(e)])

            @pl.when(jnp.logical_not(relayed(e)))
            def _():
                wait(both(c, dia), dsem(e))

            send(core_half(c, k), core_half(c, k), ss.at[4, div(e, chunks)], sb_of(e), tp, 1, sib_rep)

        turn = EARLY * groups * blocks

        def front(i, t):
            a, s1, jump, s2 = FRONTS[i]
            late = 16 * jump + s1 * turn + s2 * (t - turn)
            return jnp.minimum(gen, a + (jnp.where(t <= turn, s1 * t, late) >> 4))

        def pload(b):
            rows = pl.ds(pl.multiple_of(tp * my_rows + b * BLOCK, BLOCK), BLOCK)
            return pltpu.make_async_copy(prompts.at[rows], rows_buf.at[b % 2], iosem.at[b % 2])

        pload(0).start()
        for b in range(blocks):
            if b + 1 < blocks:
                pload(b + 1).start()
            pload(b).wait()
            for j in range(pieces):
                h[b, :, pl.ds(j * PIECE, PIECE)] = rows_buf[b % 2, pl.ds(j * PIECE, PIECE), :].T

        n_pro = FRONTS[0][0]
        for e in range(n_pro):
            y_stage(e)
            for i, fn in ((1, n_stage), (2, d_stage)):
                if e >= n_pro - FRONTS[i][0]:
                    fn(e - (n_pro - FRONTS[i][0]))
        sb_wait(0, lead, sbsem.at[0])
        load_group(0, 0, 0)

        def put(b, j):
            src = rows_buf.at[mod(b, 2), pl.ds(j * PIECE, PIECE), :]
            rows = piece_rows(tp, b, j)
            pltpu.make_async_copy(src, out.at[rows], psem.at[mod(b, 2), 0]).start()
            n, i, first = 0, 0, 0
            for rb, m in RELAYED:
                n = jnp.where(b == rb, m, n)
                i = jnp.where(b == rb, first + min(j, m - 1), i)
                first += m

            @pl.when(j < n)
            def _():
                send(src, rin.at[i], psem.at[mod(b, 2), 1], rsem.at[0, i], tp, 0, rep)

            @pl.when(j >= n)
            def _():
                send(src, out.at[rows], psem.at[mod(b, 2), 1], osem.at[0], flip_tp, 1, rep)

        def put_wait(b):
            for i in range(2):
                wait(rows_buf.at[mod(b, 2)], psem.at[mod(b, 2), i])

        n_rest = groups - 1
        wide = turn - n_rest * blocks
        n_first = blocks - MORE
        n_tasks = n_first + blocks
        first_late, last_late = 2 * EARLY, 2 * EARLY + 1

        def late_task(q):
            u = q - 2 * FIRST_LATE
            each = (u >= 0) & (u < 2 * (n_first - FIRST_LATE))
            first = (q < FIRST_LATE) | (each & ((u & 1) == 0))
            b = jnp.where(q < FIRST_LATE, q, jnp.where(u < 0, q - FIRST_LATE, jnp.where(each, FIRST_LATE + (u >> 1), q - n_first)))
            return jnp.where(first, first_late, last_late), b

        def rest(t):
            u = t - wide
            b = (u * (128 // n_rest + 1)) >> 7
            return b, 1 + u - n_rest * b

        def give(b):
            send(h.at[b], h.at[b], hs.at[b], hr.at[b], tp, 0, rep)

        def forward(t):
            for i, fn in enumerate((y_stage, n_stage, d_stage)):
                run(fn, front(i, t), front(i, t + 1))

        def early_visit(t, _):
            split = t >= wide
            rb, rg = rest(t)
            l = jnp.where(split, EARLY - 1, div(t, groups * blocks))
            g = jnp.where(split, rg, mod(div(t, blocks), groups))
            b = jnp.where(split, rb, mod(t, blocks))
            slot = mod(jnp.where(split, t - wide + 1, div(t, blocks)), 2)

            @pl.when(split | (b == 0))
            def _():
                wait_group(g, slot)

            forward(t)

            @pl.when((t > wide) & (rg == 1))
            def _():
                give(rb - 1)

            @pl.when((t < wide) & (b == blocks // 2))
            def _():
                c0 = first_of(l, g) + width_of(g)
                ng = mod(g + 1, groups)
                sem = sb_of(c0)

                @pl.when(ng == 0)
                def _():
                    sb_wait(c0, lead, sem)

                @pl.when(ng > 0)
                def _():
                    sb_wait(c0, GROUP, sem)

                load_group(c0, ng, 1 - slot)

            @pl.when(t == wide)
            def _():
                for g_ in range(2, groups):
                    c0 = (EARLY - 1) * chunks + lead + (g_ - 1) * GROUP
                    sb_wait(c0, GROUP, sb_of(c0))

            @pl.when(split & (t + 1 < turn))
            def _():
                _, ng = rest(t + 1)
                load_group(first_of(EARLY - 1, ng), ng, 1 - slot)

            @pl.when(t == turn - 1)
            def _():
                sb_wait(2 * mid, chunks, sb_of(mid))
                load_group(2 * mid, 0, 1 - slot)

            group_part(slot, g, b, b)
            return 0

        def late_visit(u, _):
            l, b = late_task(div(u, groups))
            g = mod(u, groups)
            slot = mod(u + n_rest * blocks + 1, 2)
            hb = blocks + b
            wait_group(g, slot)

            @pl.when(u < FIRST_LATE * groups)
            def _():
                forward(turn + u)

                @pl.when(u == 0)
                def _():
                    give(blocks - 1)

                @pl.when(u == FIRST_LATE * groups - 1)
                def _():
                    for i, fn in enumerate((y_stage, n_stage, d_stage)):
                        run(fn, front(i, turn + u + 1), gen)
                    sb_wait(2 * mid + chunks, chunks, sb_of(mid + chunks))

            @pl.when(u + 1 < n_tasks * groups)
            def _():
                nl, _ = late_task(div(u + 1, groups))
                ng = mod(u + 1, groups)
                load_group(first_of(nl, ng), ng, 1 - slot)

            @pl.when((g == 0) & ((l == first_late) | (b >= n_first)))
            def _():
                wait(h.at[hb], hr.at[b])

            group_part(slot, g, hb, b)

            @pl.when((l == last_late) & (g == groups - 1))
            def _():
                @pl.when(b >= 2)
                def _():
                    put_wait(b - 2)

                for j in range(pieces):
                    cols = pl.ds(j * PIECE, PIECE)
                    rows_buf[mod(b, 2), cols, :] = h[hb, :, cols].T
                    if j >= 1:
                        put(b, j - 1)
                put(b, pieces - 1)

            return 0

        lax.fori_loop(0, turn, early_visit, 0)
        lax.fori_loop(0, (n_tasks - 1) * groups, late_visit, 0)

        b, hb, half = blocks - 1, 2 * blocks - 1, BLOCK // 2
        wait(h.at[hb], hr.at[b])
        put_wait(b - 2)

        def half_visits(i, _):
            cols = pl.ds(pl.multiple_of(i * half, half), half)
            for g in range(groups):
                slot = ((n_tasks - 1) * groups + n_rest * blocks + 1 + g) % 2
                wait_group(g, slot)
                if g + 1 < groups:
                    load_group(first_of(last_late, g + 1), g + 1, 1 - slot)
                else:

                    @pl.when(i == 0)
                    def _():
                        load_group(first_of(last_late, 0), 0, 1 - slot)

                rows = h[hb, :, cols]
                t = matmuls(slot, rows, GROUP if g else lead)
                if g:
                    t = p[b, :, cols] + t
                if g + 1 < groups:
                    p[b, :, cols] = t
                else:
                    t = (rows.astype(jnp.float32) + t).astype(jnp.bfloat16)
                    for j in range(half // PIECE):
                        at = pl.multiple_of(i * half + j * PIECE, PIECE)
                        rows_buf[b % 2, pl.ds(at, PIECE), :] = t[:, j * PIECE : (j + 1) * PIECE].T
            for j in range(half // PIECE):
                at = i * half + j * PIECE
                src = rows_buf.at[b % 2, pl.ds(pl.multiple_of(at, PIECE), PIECE), :]
                to = pl.ds(pl.multiple_of(tp * my_rows + b * BLOCK + at, PIECE), PIECE)
                pltpu.make_async_copy(src, out.at[to], psem.at[b % 2, 0]).start()
                send(src, out.at[to], psem.at[b % 2, 1], osem.at[0], flip_tp, 1, rep)
            return 0

        lax.fori_loop(0, 2, half_visits, 0)
        for b in range(blocks - 2, blocks):
            put_wait(b)
        run(lambda b: wait(h.at[b], hs.at[b]), 0, blocks)
        wait(out.at[pl.ds(pl.multiple_of(flip_tp * my_rows, BLOCK), my_rows)], osem.at[0])
        for l in range(2 * EARLY):
            for i in range(5):
                if i == 4:
                    wait(wbuf.at[pl.ds(0, chunks), :, :, 0], ss.at[i, l])
                else:
                    kinds = (None, None, lambda e: not relayed(e) and not by_z(e), lambda e: not relayed(e) and by_z(e))
                    n = chunks if i < 2 else count(l * chunks, (l + 1) * chunks, kinds[i])
                    wait(wbuf.at[pl.ds(0, n), :, 0, 0, 0], ss.at[i, l])


def finish_kernel(up, dn, rows, new_up, new_dn, out, buf, zbuf, lsem, ssem, zsem):
    layers = up.shape[0]
    n_rows = rows.shape[0]
    slots, band, hidden = buf.shape
    side = lax.axis_index("side")
    items = [(i, o, l) for l in range(layers) for i, o in ((up, new_up), (dn, new_dn))]
    piece = zbuf.shape[1]
    n_pieces = n_rows // piece
    n_slots = zbuf.shape[0]

    def pipeline(n, n_slots, load, store, zeros):
        for i in range(min(n_slots, n)):
            load(i).start()
        half = n_slots // 2
        done = 0
        for i in range(n):
            load(i).wait()
            store(i).start()
            upto = len(zeros) * (i + 1) // n
            for cp in zeros[done:upto]:
                cp.start()
            done = upto
            nxt = i + half
            if i >= half and nxt < n:
                store(nxt - n_slots).wait()
                load(nxt).start()
        for i in range(max(n - n_slots, 0), n):
            store(i).wait()
        for cp in zeros:
            cp.wait()

    @pl.when(side == 0)
    def _():
        zbuf[0] = jnp.zeros(zbuf.shape[1:], zbuf.dtype)
        zeros = [
            pltpu.make_async_copy(zbuf.at[0], out.at[pl.ds(i * piece, piece)], zsem.at[i]) for i in range(n_pieces)
        ]

        def load(i):
            src, _, l = items[i]
            return pltpu.make_async_copy(src.at[l], buf.at[i % slots], lsem.at[i % slots])

        def store(i):
            _, dst, l = items[i]
            return pltpu.make_async_copy(buf.at[i % slots], dst.at[l], ssem.at[i % slots])

        pipeline(len(items), slots, load, store, zeros)

    @pl.when(side == 1)
    def _():
        buf[0] = jnp.zeros(buf.shape[1:], buf.dtype)
        zeros = [pltpu.make_async_copy(buf.at[0], dst.at[l], zsem.at[i]) for i, (_, dst, l) in enumerate(items)]

        def load(i):
            return pltpu.make_async_copy(rows.at[pl.ds(i * piece, piece)], zbuf.at[i % n_slots], lsem.at[i % n_slots])

        def store(i):
            return pltpu.make_async_copy(zbuf.at[i % n_slots], out.at[pl.ds(i * piece, piece)], ssem.at[i % n_slots])

        pipeline(n_pieces, n_slots, load, store, zeros)


def solution(mesh):
    up_spec = P("side", None, ("rep", "tp"), None)
    down_spec = P("side", None, None, ("rep", "tp"))
    tok_spec = P("side", "rep", None, None)

    def device_step(w_up, w_down, g_up, g_down, learn_rate, prompts):
        layers, band, hidden = w_up.shape[1:]
        n_rows, d = prompts.shape[2:]
        chunks = hidden // UNIT
        total = layers * chunks
        my_rows = n_rows // 2
        blocks, pieces = my_rows // BLOCK, BLOCK // PIECE
        weights = (w_up[0], jnp.swapaxes(w_down[0], 1, 2), g_up[0], jnp.swapaxes(g_down[0], 1, 2))
        smem = pl.BlockSpec(memory_space=pltpu.SMEM)
        hbm = pl.BlockSpec(memory_space=pl.ANY)
        bf16 = jnp.bfloat16
        relay = jax.ShapeDtypeStruct((sum(n for _, n in RELAYED), PIECE, d), bf16)
        new_w = jax.ShapeDtypeStruct((layers, band, hidden), jnp.float32)
        rows = jax.ShapeDtypeStruct((n_rows, d), bf16)
        rows_mid, up_mid, dn_mid, _, _, _ = pl.pallas_call(
            sync_kernel,
            name="sync_and_forward",
            out_shape=(
                rows,
                new_w,
                new_w,
                jax.ShapeDtypeStruct((total, 2, 2, 2, 2, band, UNIT), bf16),
                relay,
                relay,
            ),
            in_specs=[smem] + [hbm] * 5,
            out_specs=(hbm,) * 6,
            scratch_shapes=[
                pltpu.VMEM((2 * blocks, d, BLOCK), bf16),
                pltpu.VMEM((blocks, d, BLOCK), jnp.float32),
                pltpu.VMEM((2, GROUP, 2, 2, 2, 2, band, UNIT), bf16),
                pltpu.VMEM((LOAD_SLOTS, 4, band, UNIT), jnp.float32),
                pltpu.VMEM((LOAD_SLOTS, 2, band, UNIT), jnp.float32),
                pltpu.VMEM((STAGE_SLOTS, 2, band, UNIT), bf16),
                pltpu.VMEM((2, BLOCK, d), bf16),
                pltpu.SemaphoreType.DMA((2 * EARLY * chunks,)),
                pltpu.SemaphoreType.DMA((3, RING)),
                pltpu.SemaphoreType.DMA((EARLY * chunks // 6 + chunks // 3 + 1,)),
                pltpu.SemaphoreType.DMA((EARLY * (-(-chunks // GROUP)) + 2 * EARLY + 1,)),
                pltpu.SemaphoreType.DMA((5, 2 * EARLY)),
                pltpu.SemaphoreType.DMA((LOAD_SLOTS,)),
                pltpu.SemaphoreType.DMA((LOAD_SLOTS,)),
                pltpu.SemaphoreType.DMA((2,)),
                pltpu.SemaphoreType.DMA((STAGE_SLOTS, 2)),
                pltpu.SemaphoreType.DMA((STAGE_SLOTS,)),
                pltpu.SemaphoreType.DMA((2,)),
                pltpu.SemaphoreType.DMA((2, 2)),
                pltpu.SemaphoreType.DMA((1,)),
                pltpu.SemaphoreType.DMA((2, sum(n for _, n in RELAYED))),
                pltpu.SemaphoreType.DMA((blocks,)),
                pltpu.SemaphoreType.DMA((blocks,)),
            ],
            compiler_params=pltpu.CompilerParams(
                collective_id=0, has_side_effects=True, vmem_limit_bytes=60 * 1024 * 1024
            ),
        )(learn_rate, *weights, prompts[0, 0])
        new_up, new_dn, gen_out = pl.pallas_call(
            finish_kernel,
            name="write_outputs",
            out_shape=(new_w, new_w, rows),
            in_specs=[hbm] * 3,
            out_specs=(hbm,) * 3,
            scratch_shapes=[
                pltpu.VMEM((8, band, hidden), jnp.float32),
                pltpu.VMEM((8, n_rows // 16, d), bf16),
                pltpu.SemaphoreType.DMA((8,)),
                pltpu.SemaphoreType.DMA((8,)),
                pltpu.SemaphoreType.DMA((max(16, 2 * layers),)),
            ],
            compiler_params=pltpu.CompilerParams(vmem_limit_bytes=62 * 1024 * 1024),
        )(up_mid, dn_mid, rows_mid)
        return new_up[None], jnp.swapaxes(new_dn, 1, 2)[None], gen_out[None, None]

    return jax.shard_map(
        device_step,
        mesh=mesh,
        in_specs=(up_spec, down_spec, up_spec, down_spec, P("side"), tok_spec),
        out_specs=(up_spec, down_spec, tok_spec),
        check_vma=False,
    )
```

```python
import jax
import jax.numpy as jnp
from jax import lax
from jax.experimental import pallas as pl
from jax.experimental.pallas import tpu as pltpu
from jax.sharding import PartitionSpec as P

MESH = pl.DeviceIdType.MESH
UNIT = 256
GROUP = 5
BLOCK = 512
PIECE = 128
EARLY = 2
LOAD_SLOTS = 4
STAGE_SLOTS = 36
RING = 32
N_LAG, D_LAG = 3, 6
RELAY_LAG = 4
FIRST_LATE = 3
MORE = 2
RELAYED = ((5, 2), (6, 2))
FRONTS = ((10, 15, 1, 40), (8, 14, 1, 44), (6, 13, 3, 24))
GELU_A = 0.7978845608028654
GELU_B = 0.7978845608028654 * 0.044715


def div(a, n):
    if isinstance(a, int):
        return a // n
    if n & (n - 1) == 0:
        return a >> (n.bit_length() - 1)
    return (a * ((1 << 16) // n + 1)) >> 16


def mod(a, n):
    return a - n * div(a, n)


def gelu(a):
    return a * (0.5 * jnp.tanh(a * (GELU_A + GELU_B * (a * a))) + 0.5)


def sync_kernel(
    rate_ref, w_up, w_dn, g_up, g_dn, prompts, out, nu, nd, wbuf, rin, rx,
    h, p, wv, fin, fnew, stage, rows_buf,
    ysem, rs, rlsem, sbsem, ss, lsem, stsem, fsem, tss, csem, iosem, psem, osem, rsem, hs, hr,
):
    layers, band, hidden = w_up.shape
    chunks = hidden // UNIT
    n_relay = sum(n for _, n in RELAYED)
    groups = -(-chunks // GROUP)
    lead = chunks - (groups - 1) * GROUP
    mid = EARLY * chunks
    gen = 2 * mid
    n_rows, d = out.shape
    my_rows = n_rows // 2
    blocks = my_rows // BLOCK
    pieces = BLOCK // PIECE

    tp = lax.axis_index("tp")
    side = lax.axis_index("side")
    rep = lax.axis_index("rep")
    x, k = rep // 2, rep % 2
    flip_tp = 1 - tp
    flip_rep = (1 - x) * 2 + k
    sib_rep = x * 2 + (1 - k)

    own, znb, xnb, dia = (x, tp), (x, flip_tp), (1 - x, tp), (1 - x, flip_tp)

    def both(c, b):
        return wbuf.at[c, :, b[0], k, b[1]]

    def core_half(c, core):
        return wbuf.at[c, :, :, core]

    def chunk_of(e):
        return e + jnp.where(e >= mid, mid, 0)

    def relayed(e):
        return ((mod(e, 6) == 5) & (e < mid)) | ((mod(e, 3) == 2) & (e >= mid + chunks))

    def by_z(e):
        return ((mod(div(e, 6) + mod(e, 6), 2) == 1) & (e < mid + chunks)) | ((mod(e, 3) == 1) & (e >= mid + chunks))

    def count(e0, e1, fn):
        return sum(1 for e in range(e0, e1) if fn(e))

    n_early = count(0, mid, relayed)

    def relay_index(e):
        return jnp.where(e < mid, div(e, 6), n_early + div(e - mid - chunks, 3))

    def zsem(e):
        return rs.at[0, mod(e, RING)]

    def xsem(e):
        return rs.at[1, mod(e, RING)]

    def dsem(e):
        return rs.at[2, mod(e, RING)]

    def sb_of(e):
        l = div(e, chunks)
        j = e - l * chunks
        g = jnp.where(j < lead, 0, 1 + div(j - lead, GROUP))
        return sbsem.at[jnp.where(e < mid, l * groups + g, EARLY * groups + l - EARLY)]

    def sb_mid(f):
        return sbsem.at[EARLY * groups + EARLY + div(f, chunks)]

    def send(src, dst, ssem, rsem_, t, s, r):
        pltpu.make_async_remote_copy(
            src_ref=src, dst_ref=dst, send_sem=ssem, recv_sem=rsem_,
            device_id={"tp": t, "side": s, "rep": r}, device_id_type=MESH,
        ).start()

    def wait(ref, sem):
        pltpu.make_async_copy(ref, ref, sem).wait()

    def run(fn, lo, hi):
        def body(c, _):
            fn(c)
            return 0

        lax.fori_loop(lo, hi, body, 0)

    def piece_rows(t, b, j):
        return pl.ds(pl.multiple_of(t * my_rows + b * BLOCK + j * PIECE, PIECE), PIECE)

    def sb_wait(c0, width, sem):
        wait(wbuf.at[pl.ds(c0, width), :, :, 1 - k], sem)

    def load_group(c0, g, slot):
        def load(j):
            pltpu.make_async_copy(wbuf.at[c0 + j], wv.at[slot, j], fsem.at[slot]).start()

        for j in range(lead):
            load(j)

        @pl.when(g > 0)
        def _():
            for j in range(lead, GROUP):
                load(j)

    def wait_group(g, slot):
        @pl.when(g == 0)
        def _():
            wait(wv.at[slot, pl.ds(0, lead)], fsem.at[slot])

        @pl.when(g > 0)
        def _():
            wait(wv.at[slot], fsem.at[slot])

    def width_of(g):
        return jnp.where(g == 0, lead, GROUP)

    def first_of(l, g):
        return l * chunks + jnp.where(g == 0, 0, lead + (g - 1) * GROUP)

    def matmuls(slot, hb, width):
        def weight(j, m):
            return wv[slot, j, m].reshape(d, UNIT)

        rows = h[hb]
        acts = []
        for j in range(width):
            a = lax.dot_general(weight(j, 0), rows, (((0,), (0,)), ((), ())), preferred_element_type=jnp.float32)
            acts.append(gelu(a).astype(jnp.bfloat16))
        down = jnp.concatenate([weight(j, 1) for j in range(width)], axis=1)
        return jnp.dot(down, jnp.concatenate(acts, axis=0), preferred_element_type=jnp.float32)

    def group_part(slot, g, hb, pb):
        @pl.when(g == 0)
        def _():
            p[pb] = matmuls(slot, hb, lead)

        @pl.when((g > 0) & (g < groups - 1))
        def _():
            p[pb] = p[pb] + matmuls(slot, hb, GROUP)

        @pl.when(g == groups - 1)
        def _():
            s = p[pb] + matmuls(slot, hb, GROUP)
            h[hb] = (h[hb].astype(jnp.float32) + s).astype(jnp.bfloat16)

    parts = ((w_up, g_up, nu), (w_dn, g_dn, nd))
    steps = gen + mid

    def chunk_at(s):
        return jnp.where(mod(s, 3) == 2, mid + div(s, 3), chunk_of(2 * div(s, 3) + mod(s, 3)))

    def cols_of(c):
        return div(c, chunks), pl.ds(pl.multiple_of(mod(c, chunks) * UNIT, UNIT), UNIT)

    def loads(s):
        l, cols = cols_of(chunk_at(s))
        slot = mod(s, LOAD_SLOTS)
        for m in range(2):
            for i, r in enumerate(parts[m][:2]):
                pltpu.make_async_copy(r.at[l, :, cols], fin.at[slot, 2 * m + i], lsem.at[slot]).start()

    def cast(s):
        slot, lslot = mod(s, STAGE_SLOTS), mod(s, LOAD_SLOTS)
        wait(fin.at[lslot], lsem.at[lslot])
        rate = rate_ref[0]
        for m in range(2):
            new = fin[lslot, 2 * m] - rate * fin[lslot, 2 * m + 1]
            fnew[lslot, m] = new
            stage[slot, m] = new.astype(jnp.bfloat16)

    @pl.when(side == 0)
    def _():
        for s in range(LOAD_SLOTS):
            loads(s)
        cast(0)

    barrier = pltpu.get_barrier_semaphore()
    peers = [(tp, 1 - side, rep)] + [
        (t, side, r) for t, r in ((flip_tp, rep), (tp, flip_rep), (flip_tp, flip_rep), (tp, sib_rep))
    ]
    for t, s_, r in peers:
        pl.semaphore_signal(
            barrier, inc=1, device_id={"tp": t, "side": s_, "rep": r}, device_id_type=MESH
        )
    pl.semaphore_wait(barrier, len(peers))

    @pl.when(side == 0)
    def _():
        def stores(s):
            l, cols = cols_of(chunk_at(s))
            slot = mod(s, LOAD_SLOTS)
            for m in range(2):
                pltpu.make_async_copy(fnew.at[slot, m], parts[m][2].at[l, :, cols], stsem.at[slot]).start()

        def wait_stored(s):
            slot = mod(s, LOAD_SLOTS)
            wait(fnew.at[slot], stsem.at[slot])

        def own_copy(s):
            slot = s % STAGE_SLOTS
            return pltpu.make_async_copy(stage.at[slot], both(chunk_at(s), own), csem.at[slot])

        def gathered_too(s):
            e = 2 * (s // 3) + s % 3
            return (s % 3 != 2) & (e >= mid) & (e < mid + chunks)

        def post(s):
            slot = s % STAGE_SLOTS
            src = stage.at[slot]
            stores(s)

            @pl.when(s % 3 != 2)
            def _():
                e = 2 * (s // 3) + s % 3
                c = chunk_of(e)
                send(src, both(c, own), tss.at[slot, 0], ysem.at[e], tp, 1, rep)

                @pl.when(gathered_too(s))
                def _():
                    own_copy(s).start()

                @pl.when(relayed(e))
                def _():
                    send(src, both(c, own), tss.at[slot, 1], rlsem.at[relay_index(e)], flip_tp, 0, flip_rep)

                @pl.when(e >= RELAY_LAG)
                def _():
                    relay(e - RELAY_LAG)

            @pl.when(s % 3 == 2)
            def _():
                f = div(s, 3)
                c = mid + f
                own_copy(s).start()
                send(src, both(c, own), tss.at[slot, 0], zsem(f), flip_tp, 0, rep)
                send(src, both(c, own), tss.at[slot, 1], xsem(f), tp, 0, flip_rep)

        def relay(e):
            @pl.when(relayed(e))
            def _():
                c = chunk_of(e)
                sem = rlsem.at[relay_index(e)]
                wait(both(c, dia), sem)
                send(both(c, dia), both(c, dia), ss.at[0, div(e, chunks)], sem, tp, 1, rep)

        def wait_sent(s):
            slot = s % STAGE_SLOTS
            is_mid = s % 3 == 2
            wait(stage.at[slot], tss.at[slot, 0])

            @pl.when(is_mid | relayed(2 * (s // 3) + s % 3))
            def _():
                wait(stage.at[slot], tss.at[slot, 1])

        def own_stage(f):
            c = mid + f
            send(both(c, own), both(c, own), ss.at[1, 0], zsem(f), flip_tp, 0, rep)
            send(both(c, own), both(c, own), ss.at[1, 1], xsem(f), tp, 0, flip_rep)

        def n_stage(f):
            c = mid + f
            wait(both(c, znb), zsem(f))
            wait(both(c, xnb), xsem(f))

            @pl.when(mod(f, 2) == 0)
            def _():
                send(both(c, znb), both(c, znb), ss.at[2, div(f, chunks)], dsem(f), tp, 0, flip_rep)

            @pl.when(mod(f, 2) == 1)
            def _():
                send(both(c, xnb), both(c, xnb), ss.at[3, div(f, chunks)], dsem(f), flip_tp, 0, rep)

        def d_stage(f):
            c = mid + f
            wait(both(c, dia), dsem(f))

            @pl.when(f < mid)
            def _():
                own_copy(3 * f + 2).wait()

            send(core_half(c, k), core_half(c, k), ss.at[4, div(f, chunks)], sb_mid(f), tp, 0, sib_rep)

        def body(s, _):
            @pl.when(s + LOAD_SLOTS - 1 < steps)
            def _():
                loads(s + LOAD_SLOTS - 1)

            @pl.when(s >= STAGE_SLOTS)
            def _():
                wait_sent(s - STAGE_SLOTS)

                @pl.when(gathered_too(s - STAGE_SLOTS))
                def _():
                    own_copy(s - STAGE_SLOTS).wait()

            @pl.when(s >= LOAD_SLOTS)
            def _():
                wait_stored(s - LOAD_SLOTS)

            cast(s)
            @pl.when(s >= 2)
            def _():
                post(s - 1)

            @pl.when(s % 3 == 2)
            def _():
                f = s // 3

                @pl.when(f >= N_LAG)
                def _():
                    n_stage(f - N_LAG)

                @pl.when(f >= D_LAG)
                def _():
                    d_stage(f - D_LAG)

            return 0

        post(0)
        lax.fori_loop(1, steps, body, 0)
        post(steps - 1)
        run(relay, gen - RELAY_LAG, gen)
        run(n_stage, mid - N_LAG, mid)
        run(d_stage, mid - D_LAG, mid)
        for s in range(steps - LOAD_SLOTS, steps):
            wait_stored(s)
        for s in range(steps - STAGE_SLOTS, steps):
            if s % 3 != 2 and mid <= 2 * (s // 3) + s % 3 < mid + chunks:
                own_copy(s).wait()
        for l in range(EARLY):
            sb_wait(mid + l * chunks, chunks, sb_mid(l * chunks))

        load_group(mid, 0, 0)
        per_block = EARLY * groups
        few = (blocks - MORE) * per_block
        n_visits = few + MORE * (per_block + groups)

        def place(t):
            u = t - few
            more = jnp.where(u >= per_block + groups, 1, 0)
            b = jnp.where(t < few, div(t, per_block), blocks - MORE + more)
            return b, jnp.where(t < few, mod(t, per_block), u - more * (per_block + groups))

        def give_back(b):
            send(h.at[b], h.at[blocks + b], hs.at[b], hr.at[b], tp, 1, rep)

        def visit(t, _):
            b, q = place(t)
            g, slot = mod(q, groups), mod(q, 2)
            wait_group(g, slot)

            for fn, after in ((own_stage, 0), (n_stage, 8), (d_stage, 18)):

                @pl.when((t >= after) & (t < after + chunks))
                def _():
                    fn(mid + t - after)

            @pl.when(t == few)
            def _():
                sb_wait(2 * mid, chunks, sb_mid(mid))

            @pl.when(t + 1 < n_visits)
            def _():
                _, nq = place(t + 1)
                ng = mod(nq, groups)
                load_group(first_of(EARLY + div(nq, groups), ng), ng, 1 - slot)

            @pl.when(q == 0)
            def _():
                @pl.when(b > 0)
                def _():
                    give_back(b - 1)

                wait(h.at[b], hr.at[b])

            group_part(slot, g, b, 0)
            return 0

        lax.fori_loop(0, n_visits, visit, 0)
        run(lambda b: wait(h.at[b], hs.at[b]), 0, blocks - 2)
        give_back(blocks - 1)

        def relay_out(i, _):
            @pl.when(i < n_relay)
            def _():
                wait(rin.at[i], rsem.at[0, i])
                send(rin.at[i], rx.at[i], psem.at[0, 0], rsem.at[1, i], flip_tp, 0, rep)

            @pl.when(i >= 1)
            def _():
                q = i - 1
                wait(rx.at[q], rsem.at[1, q])
                b, j, first = 0, 0, 0
                for rb, n in RELAYED:
                    b = jnp.where(q >= first, rb, b)
                    j = jnp.where(q >= first, q - first, j)
                    first += n
                send(rx.at[q], out.at[piece_rows(flip_tp, b, j)], psem.at[0, 1], osem.at[0], tp, 1, rep)

            return 0

        lax.fori_loop(0, n_relay + 1, relay_out, 0)
        wait(rin, psem.at[0, 0])
        wait(rx, psem.at[0, 1])
        run(wait_sent, steps - STAGE_SLOTS, steps)
        run(lambda b: wait(h.at[b], hs.at[b]), blocks - 2, blocks)
        for l in range(2 * EARLY):
            n = count(l * chunks, (l + 1) * chunks, relayed)
            if n:
                wait(wbuf.at[pl.ds(0, n), :, 0, 0, 0], ss.at[0, l])
        for i in range(2):
            wait(wbuf.at[pl.ds(0, chunks), :, 0, 0, 0], ss.at[1, i])
        for l in range(EARLY + 1):
            for m in range(2):
                n = count(l * chunks, (l + 1) * chunks, lambda f: f % 2 == m)
                wait(wbuf.at[pl.ds(0, n), :, 0, 0, 0], ss.at[2 + m, l])
            wait(wbuf.at[pl.ds(0, chunks), :, :, 0], ss.at[4, l])

    @pl.when(side == 1)
    def _():
        def y_stage(e):
            c, l = chunk_of(e), div(e, chunks)
            wait(both(c, own), ysem.at[e])
            send(both(c, own), both(c, own), ss.at[0, l], zsem(e), flip_tp, 1, rep)
            send(both(c, own), both(c, own), ss.at[1, l], xsem(e), tp, 1, flip_rep)

        def n_stage(e):
            c, l = chunk_of(e), div(e, chunks)
            wait(both(c, znb), zsem(e))
            wait(both(c, xnb), xsem(e))
            direct = jnp.logical_not(relayed(e))

            @pl.when(direct & jnp.logical_not(by_z(e)))
            def _():
                send(both(c, znb), both(c, znb), ss.at[2, l], dsem(e), tp, 1, flip_rep)

            @pl.when(direct & by_z(e))
            def _():
                send(both(c, xnb), both(c, xnb), ss.at[3, l], dsem(e), flip_tp, 1, rep)

        def d_stage(e):
            c = chunk_of(e)

            @pl.when(relayed(e))
            def _():
                wait(both(c, dia), rlsem.at[relay_index(e)])

            @pl.when(jnp.logical_not(relayed(e)))
            def _():
                wait(both(c, dia), dsem(e))

            send(core_half(c, k), core_half(c, k), ss.at[4, div(e, chunks)], sb_of(e), tp, 1, sib_rep)

        turn = EARLY * groups * blocks

        def front(i, t):
            a, s1, jump, s2 = FRONTS[i]
            late = 16 * jump + s1 * turn + s2 * (t - turn)
            return jnp.minimum(gen, a + (jnp.where(t <= turn, s1 * t, late) >> 4))

        def pload(b):
            rows = pl.ds(pl.multiple_of(tp * my_rows + b * BLOCK, BLOCK), BLOCK)
            return pltpu.make_async_copy(prompts.at[rows], rows_buf.at[b % 2], iosem.at[b % 2])

        pload(0).start()
        for b in range(blocks):
            if b + 1 < blocks:
                pload(b + 1).start()
            pload(b).wait()
            for j in range(pieces):
                h[b, :, pl.ds(j * PIECE, PIECE)] = rows_buf[b % 2, pl.ds(j * PIECE, PIECE), :].T

        n_pro = FRONTS[0][0]
        for e in range(n_pro):
            y_stage(e)
            for i, fn in ((1, n_stage), (2, d_stage)):
                if e >= n_pro - FRONTS[i][0]:
                    fn(e - (n_pro - FRONTS[i][0]))
        sb_wait(0, lead, sbsem.at[0])
        load_group(0, 0, 0)

        def put(b, j):
            src = rows_buf.at[mod(b, 2), pl.ds(j * PIECE, PIECE), :]
            rows = piece_rows(tp, b, j)
            pltpu.make_async_copy(src, out.at[rows], psem.at[mod(b, 2), 0]).start()
            n, i, first = 0, 0, 0
            for rb, m in RELAYED:
                n = jnp.where(b == rb, m, n)
                i = jnp.where(b == rb, first + min(j, m - 1), i)
                first += m

            @pl.when(j < n)
            def _():
                send(src, rin.at[i], psem.at[mod(b, 2), 1], rsem.at[0, i], tp, 0, rep)

            @pl.when(j >= n)
            def _():
                send(src, out.at[rows], psem.at[mod(b, 2), 1], osem.at[0], flip_tp, 1, rep)

        def put_wait(b):
            for i in range(2):
                wait(rows_buf.at[mod(b, 2)], psem.at[mod(b, 2), i])

        n_rest = groups - 1
        wide = turn - n_rest * blocks
        n_first = blocks - MORE
        n_tasks = n_first + blocks
        first_late, last_late = 2 * EARLY, 2 * EARLY + 1

        def late_task(q):
            u = q - 2 * FIRST_LATE
            each = (u >= 0) & (u < 2 * (n_first - FIRST_LATE))
            first = (q < FIRST_LATE) | (each & ((u & 1) == 0))
            b = jnp.where(q < FIRST_LATE, q, jnp.where(u < 0, q - FIRST_LATE, jnp.where(each, FIRST_LATE + (u >> 1), q - n_first)))
            return jnp.where(first, first_late, last_late), b

        def rest(t):
            u = t - wide
            b = (u * (128 // n_rest + 1)) >> 7
            return b, 1 + u - n_rest * b

        def give(b):
            send(h.at[b], h.at[b], hs.at[b], hr.at[b], tp, 0, rep)

        def forward(t):
            for i, fn in enumerate((y_stage, n_stage, d_stage)):
                run(fn, front(i, t), front(i, t + 1))

        def early_visit(t, _):
            split = t >= wide
            rb, rg = rest(t)
            l = jnp.where(split, EARLY - 1, div(t, groups * blocks))
            g = jnp.where(split, rg, mod(div(t, blocks), groups))
            b = jnp.where(split, rb, mod(t, blocks))
            slot = mod(jnp.where(split, t - wide + 1, div(t, blocks)), 2)

            @pl.when(split | (b == 0))
            def _():
                wait_group(g, slot)

            forward(t)

            @pl.when((t > wide) & (rg == 1))
            def _():
                give(rb - 1)

            @pl.when((t < wide) & (b == blocks // 2))
            def _():
                c0 = first_of(l, g) + width_of(g)
                ng = mod(g + 1, groups)
                sem = sb_of(c0)

                @pl.when(ng == 0)
                def _():
                    sb_wait(c0, lead, sem)

                @pl.when(ng > 0)
                def _():
                    sb_wait(c0, GROUP, sem)

                load_group(c0, ng, 1 - slot)

            @pl.when(t == wide)
            def _():
                for g_ in range(2, groups):
                    c0 = (EARLY - 1) * chunks + lead + (g_ - 1) * GROUP
                    sb_wait(c0, GROUP, sb_of(c0))

            @pl.when(split & (t + 1 < turn))
            def _():
                _, ng = rest(t + 1)
                load_group(first_of(EARLY - 1, ng), ng, 1 - slot)

            @pl.when(t == turn - 1)
            def _():
                sb_wait(2 * mid, chunks, sb_of(mid))
                load_group(2 * mid, 0, 1 - slot)

            group_part(slot, g, b, b)
            return 0

        def late_visit(u, _):
            l, b = late_task(div(u, groups))
            g = mod(u, groups)
            slot = mod(u + n_rest * blocks + 1, 2)
            hb = blocks + b
            wait_group(g, slot)

            @pl.when(u < FIRST_LATE * groups)
            def _():
                forward(turn + u)

                @pl.when(u == 0)
                def _():
                    give(blocks - 1)

                @pl.when(u == FIRST_LATE * groups - 1)
                def _():
                    for i, fn in enumerate((y_stage, n_stage, d_stage)):
                        run(fn, front(i, turn + u + 1), gen)
                    sb_wait(2 * mid + chunks, chunks, sb_of(mid + chunks))

            @pl.when(u + 1 < n_tasks * groups)
            def _():
                nl, _ = late_task(div(u + 1, groups))
                ng = mod(u + 1, groups)
                load_group(first_of(nl, ng), ng, 1 - slot)

            @pl.when((g == 0) & ((l == first_late) | (b >= n_first)))
            def _():
                wait(h.at[hb], hr.at[b])

            group_part(slot, g, hb, b)

            @pl.when((l == last_late) & (g == groups - 1))
            def _():
                @pl.when(b >= 2)
                def _():
                    put_wait(b - 2)

                for j in range(pieces):
                    cols = pl.ds(j * PIECE, PIECE)
                    rows_buf[mod(b, 2), cols, :] = h[hb, :, cols].T
                    if j >= 1:
                        put(b, j - 1)
                put(b, pieces - 1)

            return 0

        lax.fori_loop(0, turn, early_visit, 0)
        lax.fori_loop(0, n_tasks * groups, late_visit, 0)
        for b in range(blocks - 2, blocks):
            put_wait(b)
        run(lambda b: wait(h.at[b], hs.at[b]), 0, blocks)
        wait(out.at[pl.ds(pl.multiple_of(flip_tp * my_rows, BLOCK), my_rows)], osem.at[0])
        for l in range(2 * EARLY):
            for i in range(5):
                if i == 4:
                    wait(wbuf.at[pl.ds(0, chunks), :, :, 0], ss.at[i, l])
                else:
                    kinds = (None, None, lambda e: not relayed(e) and not by_z(e), lambda e: not relayed(e) and by_z(e))
                    n = chunks if i < 2 else count(l * chunks, (l + 1) * chunks, kinds[i])
                    wait(wbuf.at[pl.ds(0, n), :, 0, 0, 0], ss.at[i, l])


def finish_kernel(up, dn, rows, new_up, new_dn, out, buf, zbuf, lsem, ssem, zsem):
    layers = up.shape[0]
    n_rows = rows.shape[0]
    slots, band, hidden = buf.shape
    side = lax.axis_index("side")
    items = [(i, o, l) for l in range(layers) for i, o in ((up, new_up), (dn, new_dn))]
    piece = zbuf.shape[1]
    n_pieces = n_rows // piece
    n_slots = zbuf.shape[0]

    def pipeline(n, n_slots, load, store, zeros):
        for i in range(min(n_slots, n)):
            load(i).start()
        half = n_slots // 2
        done = 0
        for i in range(n):
            load(i).wait()
            store(i).start()
            upto = len(zeros) * (i + 1) // n
            for cp in zeros[done:upto]:
                cp.start()
            done = upto
            nxt = i + half
            if i >= half and nxt < n:
                store(nxt - n_slots).wait()
                load(nxt).start()
        for i in range(max(n - n_slots, 0), n):
            store(i).wait()
        for cp in zeros:
            cp.wait()

    @pl.when(side == 0)
    def _():
        zbuf[0] = jnp.zeros(zbuf.shape[1:], zbuf.dtype)
        zeros = [
            pltpu.make_async_copy(zbuf.at[0], out.at[pl.ds(i * piece, piece)], zsem.at[i]) for i in range(n_pieces)
        ]

        def load(i):
            src, _, l = items[i]
            return pltpu.make_async_copy(src.at[l], buf.at[i % slots], lsem.at[i % slots])

        def store(i):
            _, dst, l = items[i]
            return pltpu.make_async_copy(buf.at[i % slots], dst.at[l], ssem.at[i % slots])

        pipeline(len(items), slots, load, store, zeros)

    @pl.when(side == 1)
    def _():
        buf[0] = jnp.zeros(buf.shape[1:], buf.dtype)
        zeros = [pltpu.make_async_copy(buf.at[0], dst.at[l], zsem.at[i]) for i, (_, dst, l) in enumerate(items)]

        def load(i):
            return pltpu.make_async_copy(rows.at[pl.ds(i * piece, piece)], zbuf.at[i % n_slots], lsem.at[i % n_slots])

        def store(i):
            return pltpu.make_async_copy(zbuf.at[i % n_slots], out.at[pl.ds(i * piece, piece)], ssem.at[i % n_slots])

        pipeline(n_pieces, n_slots, load, store, zeros)


def solution(mesh):
    up_spec = P("side", None, ("rep", "tp"), None)
    down_spec = P("side", None, None, ("rep", "tp"))
    tok_spec = P("side", "rep", None, None)

    def device_step(w_up, w_down, g_up, g_down, learn_rate, prompts):
        layers, band, hidden = w_up.shape[1:]
        n_rows, d = prompts.shape[2:]
        chunks = hidden // UNIT
        total = layers * chunks
        my_rows = n_rows // 2
        blocks, pieces = my_rows // BLOCK, BLOCK // PIECE
        weights = (w_up[0], jnp.swapaxes(w_down[0], 1, 2), g_up[0], jnp.swapaxes(g_down[0], 1, 2))
        smem = pl.BlockSpec(memory_space=pltpu.SMEM)
        hbm = pl.BlockSpec(memory_space=pl.ANY)
        bf16 = jnp.bfloat16
        relay = jax.ShapeDtypeStruct((sum(n for _, n in RELAYED), PIECE, d), bf16)
        new_w = jax.ShapeDtypeStruct((layers, band, hidden), jnp.float32)
        rows = jax.ShapeDtypeStruct((n_rows, d), bf16)
        rows_mid, up_mid, dn_mid, _, _, _ = pl.pallas_call(
            sync_kernel,
            name="sync_and_forward",
            out_shape=(
                rows,
                new_w,
                new_w,
                jax.ShapeDtypeStruct((total, 2, 2, 2, 2, band, UNIT), bf16),
                relay,
                relay,
            ),
            in_specs=[smem] + [hbm] * 5,
            out_specs=(hbm,) * 6,
            scratch_shapes=[
                pltpu.VMEM((2 * blocks, d, BLOCK), bf16),
                pltpu.VMEM((blocks, d, BLOCK), jnp.float32),
                pltpu.VMEM((2, GROUP, 2, 2, 2, 2, band, UNIT), bf16),
                pltpu.VMEM((LOAD_SLOTS, 4, band, UNIT), jnp.float32),
                pltpu.VMEM((LOAD_SLOTS, 2, band, UNIT), jnp.float32),
                pltpu.VMEM((STAGE_SLOTS, 2, band, UNIT), bf16),
                pltpu.VMEM((2, BLOCK, d), bf16),
                pltpu.SemaphoreType.DMA((2 * EARLY * chunks,)),
                pltpu.SemaphoreType.DMA((3, RING)),
                pltpu.SemaphoreType.DMA((EARLY * chunks // 6 + chunks // 3 + 1,)),
                pltpu.SemaphoreType.DMA((EARLY * (-(-chunks // GROUP)) + 2 * EARLY + 1,)),
                pltpu.SemaphoreType.DMA((5, 2 * EARLY)),
                pltpu.SemaphoreType.DMA((LOAD_SLOTS,)),
                pltpu.SemaphoreType.DMA((LOAD_SLOTS,)),
                pltpu.SemaphoreType.DMA((2,)),
                pltpu.SemaphoreType.DMA((STAGE_SLOTS, 2)),
                pltpu.SemaphoreType.DMA((STAGE_SLOTS,)),
                pltpu.SemaphoreType.DMA((2,)),
                pltpu.SemaphoreType.DMA((2, 2)),
                pltpu.SemaphoreType.DMA((1,)),
                pltpu.SemaphoreType.DMA((2, sum(n for _, n in RELAYED))),
                pltpu.SemaphoreType.DMA((blocks,)),
                pltpu.SemaphoreType.DMA((blocks,)),
            ],
            compiler_params=pltpu.CompilerParams(
                collective_id=0, has_side_effects=True, vmem_limit_bytes=60 * 1024 * 1024
            ),
        )(learn_rate, *weights, prompts[0, 0])
        new_up, new_dn, gen_out = pl.pallas_call(
            finish_kernel,
            name="write_outputs",
            out_shape=(new_w, new_w, rows),
            in_specs=[hbm] * 3,
            out_specs=(hbm,) * 3,
            scratch_shapes=[
                pltpu.VMEM((8, band, hidden), jnp.float32),
                pltpu.VMEM((8, n_rows // 16, d), bf16),
                pltpu.SemaphoreType.DMA((8,)),
                pltpu.SemaphoreType.DMA((8,)),
                pltpu.SemaphoreType.DMA((max(16, 2 * layers),)),
            ],
            compiler_params=pltpu.CompilerParams(vmem_limit_bytes=62 * 1024 * 1024),
        )(up_mid, dn_mid, rows_mid)
        return new_up[None], jnp.swapaxes(new_dn, 1, 2)[None], gen_out[None, None]

    return jax.shard_map(
        device_step,
        mesh=mesh,
        in_specs=(up_spec, down_spec, up_spec, down_spec, P("side"), tok_spec),
        out_specs=(up_spec, down_spec, tok_spec),
        check_vma=False,
    )
```

```python
import jax
import jax.numpy as jnp
from jax import lax
from jax.experimental import pallas as pl
from jax.experimental.pallas import tpu as pltpu
from jax.sharding import PartitionSpec as P

MESH = pl.DeviceIdType.MESH
UNIT = 256
GROUP = 5
BLOCK = 512
PIECE = 128
EARLY = 2
LOAD_SLOTS = 4
STAGE_SLOTS = 36
RING = 32
N_LAG, D_LAG = 3, 6
RELAY_LAG = 4
FIRST_LATE = 2
MORE = 2
RELAYED = ((5, 2), (6, 2))
FRONTS = ((10, 15, 1, 40), (8, 14, 1, 44), (6, 13, 3, 24))
GELU_A = 0.7978845608028654
GELU_B = 0.7978845608028654 * 0.044715


def div(a, n):
    if isinstance(a, int):
        return a // n
    if n & (n - 1) == 0:
        return a >> (n.bit_length() - 1)
    return (a * ((1 << 16) // n + 1)) >> 16


def mod(a, n):
    return a - n * div(a, n)


def gelu(a):
    return a * (0.5 * jnp.tanh(a * (GELU_A + GELU_B * (a * a))) + 0.5)


def sync_kernel(
    rate_ref, w_up, w_dn, g_up, g_dn, prompts, out, nu, nd, wbuf, rin, rx,
    h, p, wv, fin, fnew, stage, rows_buf,
    ysem, rs, rlsem, sbsem, ss, lsem, stsem, fsem, tss, csem, iosem, psem, osem, rsem, hs, hr,
):
    layers, band, hidden = w_up.shape
    chunks = hidden // UNIT
    n_relay = sum(n for _, n in RELAYED)
    groups = -(-chunks // GROUP)
    lead = chunks - (groups - 1) * GROUP
    mid = EARLY * chunks
    gen = 2 * mid
    n_rows, d = out.shape
    my_rows = n_rows // 2
    blocks = my_rows // BLOCK
    pieces = BLOCK // PIECE

    tp = lax.axis_index("tp")
    side = lax.axis_index("side")
    rep = lax.axis_index("rep")
    x, k = rep // 2, rep % 2
    flip_tp = 1 - tp
    flip_rep = (1 - x) * 2 + k
    sib_rep = x * 2 + (1 - k)

    own, znb, xnb, dia = (x, tp), (x, flip_tp), (1 - x, tp), (1 - x, flip_tp)

    def both(c, b):
        return wbuf.at[c, :, b[0], k, b[1]]

    def core_half(c, core):
        return wbuf.at[c, :, :, core]

    def chunk_of(e):
        return e + jnp.where(e >= mid, mid, 0)

    def relayed(e):
        return ((mod(e, 6) == 5) & (e < mid)) | ((mod(e, 3) == 2) & (e >= mid + chunks))

    def by_z(e):
        return ((mod(div(e, 6) + mod(e, 6), 2) == 1) & (e < mid + chunks)) | ((mod(e, 3) == 1) & (e >= mid + chunks))

    def count(e0, e1, fn):
        return sum(1 for e in range(e0, e1) if fn(e))

    n_early = count(0, mid, relayed)

    def relay_index(e):
        return jnp.where(e < mid, div(e, 6), n_early + div(e - mid - chunks, 3))

    def zsem(e):
        return rs.at[0, mod(e, RING)]

    def xsem(e):
        return rs.at[1, mod(e, RING)]

    def dsem(e):
        return rs.at[2, mod(e, RING)]

    def sb_of(e):
        l = div(e, chunks)
        j = e - l * chunks
        g = jnp.where(j < lead, 0, 1 + div(j - lead, GROUP))
        return sbsem.at[jnp.where(e < mid, l * groups + g, EARLY * groups + l - EARLY)]

    def sb_mid(f):
        return sbsem.at[EARLY * groups + EARLY + div(f, chunks)]

    def send(src, dst, ssem, rsem_, t, s, r):
        pltpu.make_async_remote_copy(
            src_ref=src, dst_ref=dst, send_sem=ssem, recv_sem=rsem_,
            device_id={"tp": t, "side": s, "rep": r}, device_id_type=MESH,
        ).start()

    def wait(ref, sem):
        pltpu.make_async_copy(ref, ref, sem).wait()

    def run(fn, lo, hi):
        def body(c, _):
            fn(c)
            return 0

        lax.fori_loop(lo, hi, body, 0)

    def piece_rows(t, b, j):
        return pl.ds(pl.multiple_of(t * my_rows + b * BLOCK + j * PIECE, PIECE), PIECE)

    def sb_wait(c0, width, sem):
        wait(wbuf.at[pl.ds(c0, width), :, :, 1 - k], sem)

    def load_group(c0, g, slot):
        def load(j):
            pltpu.make_async_copy(wbuf.at[c0 + j], wv.at[slot, j], fsem.at[slot]).start()

        for j in range(lead):
            load(j)

        @pl.when(g > 0)
        def _():
            for j in range(lead, GROUP):
                load(j)

    def wait_group(g, slot):
        @pl.when(g == 0)
        def _():
            wait(wv.at[slot, pl.ds(0, lead)], fsem.at[slot])

        @pl.when(g > 0)
        def _():
            wait(wv.at[slot], fsem.at[slot])

    def width_of(g):
        return jnp.where(g == 0, lead, GROUP)

    def first_of(l, g):
        return l * chunks + jnp.where(g == 0, 0, lead + (g - 1) * GROUP)

    def matmuls(slot, hb, width):
        def weight(j, m):
            return wv[slot, j, m].reshape(d, UNIT)

        rows = h[hb]
        acts = []
        for j in range(width):
            a = lax.dot_general(weight(j, 0), rows, (((0,), (0,)), ((), ())), preferred_element_type=jnp.float32)
            acts.append(gelu(a).astype(jnp.bfloat16))
        down = jnp.concatenate([weight(j, 1) for j in range(width)], axis=1)
        return jnp.dot(down, jnp.concatenate(acts, axis=0), preferred_element_type=jnp.float32)

    def group_part(slot, g, hb, pb):
        @pl.when(g == 0)
        def _():
            p[pb] = matmuls(slot, hb, lead)

        @pl.when((g > 0) & (g < groups - 1))
        def _():
            p[pb] = p[pb] + matmuls(slot, hb, GROUP)

        @pl.when(g == groups - 1)
        def _():
            s = p[pb] + matmuls(slot, hb, GROUP)
            h[hb] = (h[hb].astype(jnp.float32) + s).astype(jnp.bfloat16)

    parts = ((w_up, g_up, nu), (w_dn, g_dn, nd))
    steps = gen + mid

    def chunk_at(s):
        return jnp.where(mod(s, 3) == 2, mid + div(s, 3), chunk_of(2 * div(s, 3) + mod(s, 3)))

    def cols_of(c):
        return div(c, chunks), pl.ds(pl.multiple_of(mod(c, chunks) * UNIT, UNIT), UNIT)

    def loads(s):
        l, cols = cols_of(chunk_at(s))
        slot = mod(s, LOAD_SLOTS)
        for m in range(2):
            for i, r in enumerate(parts[m][:2]):
                pltpu.make_async_copy(r.at[l, :, cols], fin.at[slot, 2 * m + i], lsem.at[slot]).start()

    def cast(s):
        slot, lslot = mod(s, STAGE_SLOTS), mod(s, LOAD_SLOTS)
        wait(fin.at[lslot], lsem.at[lslot])
        rate = rate_ref[0]
        for m in range(2):
            new = fin[lslot, 2 * m] - rate * fin[lslot, 2 * m + 1]
            fnew[lslot, m] = new
            stage[slot, m] = new.astype(jnp.bfloat16)

    @pl.when(side == 0)
    def _():
        for s in range(LOAD_SLOTS):
            loads(s)
        cast(0)

    barrier = pltpu.get_barrier_semaphore()
    peers = [(tp, 1 - side, rep)] + [
        (t, side, r) for t, r in ((flip_tp, rep), (tp, flip_rep), (flip_tp, flip_rep), (tp, sib_rep))
    ]
    for t, s_, r in peers:
        pl.semaphore_signal(
            barrier, inc=1, device_id={"tp": t, "side": s_, "rep": r}, device_id_type=MESH
        )
    pl.semaphore_wait(barrier, len(peers))

    @pl.when(side == 0)
    def _():
        def stores(s):
            l, cols = cols_of(chunk_at(s))
            slot = mod(s, LOAD_SLOTS)
            for m in range(2):
                pltpu.make_async_copy(fnew.at[slot, m], parts[m][2].at[l, :, cols], stsem.at[slot]).start()

        def wait_stored(s):
            slot = mod(s, LOAD_SLOTS)
            wait(fnew.at[slot], stsem.at[slot])

        def own_copy(s):
            slot = s % STAGE_SLOTS
            return pltpu.make_async_copy(stage.at[slot], both(chunk_at(s), own), csem.at[slot])

        def gathered_too(s):
            e = 2 * (s // 3) + s % 3
            return (s % 3 != 2) & (e >= mid) & (e < mid + chunks)

        def post(s):
            slot = s % STAGE_SLOTS
            src = stage.at[slot]
            stores(s)

            @pl.when(s % 3 != 2)
            def _():
                e = 2 * (s // 3) + s % 3
                c = chunk_of(e)
                send(src, both(c, own), tss.at[slot, 0], ysem.at[e], tp, 1, rep)

                @pl.when(gathered_too(s))
                def _():
                    own_copy(s).start()

                @pl.when(relayed(e))
                def _():
                    send(src, both(c, own), tss.at[slot, 1], rlsem.at[relay_index(e)], flip_tp, 0, flip_rep)

                @pl.when(e >= RELAY_LAG)
                def _():
                    relay(e - RELAY_LAG)

            @pl.when(s % 3 == 2)
            def _():
                f = div(s, 3)
                c = mid + f
                own_copy(s).start()
                send(src, both(c, own), tss.at[slot, 0], zsem(f), flip_tp, 0, rep)
                send(src, both(c, own), tss.at[slot, 1], xsem(f), tp, 0, flip_rep)

        def relay(e):
            @pl.when(relayed(e))
            def _():
                c = chunk_of(e)
                sem = rlsem.at[relay_index(e)]
                wait(both(c, dia), sem)
                send(both(c, dia), both(c, dia), ss.at[0, div(e, chunks)], sem, tp, 1, rep)

        def wait_sent(s):
            slot = s % STAGE_SLOTS
            is_mid = s % 3 == 2
            wait(stage.at[slot], tss.at[slot, 0])

            @pl.when(is_mid | relayed(2 * (s // 3) + s % 3))
            def _():
                wait(stage.at[slot], tss.at[slot, 1])

        def own_stage(f):
            c = mid + f
            send(both(c, own), both(c, own), ss.at[1, 0], zsem(f), flip_tp, 0, rep)
            send(both(c, own), both(c, own), ss.at[1, 1], xsem(f), tp, 0, flip_rep)

        def n_stage(f):
            c = mid + f
            wait(both(c, znb), zsem(f))
            wait(both(c, xnb), xsem(f))

            @pl.when(mod(f, 2) == 0)
            def _():
                send(both(c, znb), both(c, znb), ss.at[2, div(f, chunks)], dsem(f), tp, 0, flip_rep)

            @pl.when(mod(f, 2) == 1)
            def _():
                send(both(c, xnb), both(c, xnb), ss.at[3, div(f, chunks)], dsem(f), flip_tp, 0, rep)

        def d_stage(f):
            c = mid + f
            wait(both(c, dia), dsem(f))

            @pl.when(f < mid)
            def _():
                own_copy(3 * f + 2).wait()

            send(core_half(c, k), core_half(c, k), ss.at[4, div(f, chunks)], sb_mid(f), tp, 0, sib_rep)

        def body(s, _):
            @pl.when(s + LOAD_SLOTS - 1 < steps)
            def _():
                loads(s + LOAD_SLOTS - 1)

            @pl.when(s >= STAGE_SLOTS)
            def _():
                wait_sent(s - STAGE_SLOTS)

                @pl.when(gathered_too(s - STAGE_SLOTS))
                def _():
                    own_copy(s - STAGE_SLOTS).wait()

            @pl.when(s >= LOAD_SLOTS)
            def _():
                wait_stored(s - LOAD_SLOTS)

            cast(s)
            @pl.when(s >= 2)
            def _():
                post(s - 1)

            @pl.when(s % 3 == 2)
            def _():
                f = s // 3

                @pl.when(f >= N_LAG)
                def _():
                    n_stage(f - N_LAG)

                @pl.when(f >= D_LAG)
                def _():
                    d_stage(f - D_LAG)

            return 0

        post(0)
        lax.fori_loop(1, steps, body, 0)
        post(steps - 1)
        run(relay, gen - RELAY_LAG, gen)
        run(n_stage, mid - N_LAG, mid)
        run(d_stage, mid - D_LAG, mid)
        for s in range(steps - LOAD_SLOTS, steps):
            wait_stored(s)
        for s in range(steps - STAGE_SLOTS, steps):
            if s % 3 != 2 and mid <= 2 * (s // 3) + s % 3 < mid + chunks:
                own_copy(s).wait()
        for l in range(EARLY):
            sb_wait(mid + l * chunks, chunks, sb_mid(l * chunks))

        load_group(mid, 0, 0)
        per_block = EARLY * groups
        few = (blocks - MORE) * per_block
        n_visits = few + MORE * (per_block + groups)

        def place(t):
            u = t - few
            more = jnp.where(u >= per_block + groups, 1, 0)
            b = jnp.where(t < few, div(t, per_block), blocks - MORE + more)
            return b, jnp.where(t < few, mod(t, per_block), u - more * (per_block + groups))

        def give_back(b):
            send(h.at[b], h.at[blocks + b], hs.at[b], hr.at[b], tp, 1, rep)

        def visit(t, _):
            b, q = place(t)
            g, slot = mod(q, groups), mod(q, 2)
            wait_group(g, slot)

            for fn, after in ((own_stage, 0), (n_stage, 8), (d_stage, 18)):

                @pl.when((t >= after) & (t < after + chunks))
                def _():
                    fn(mid + t - after)

            @pl.when(t == few)
            def _():
                sb_wait(2 * mid, chunks, sb_mid(mid))

            @pl.when(t + 1 < n_visits)
            def _():
                _, nq = place(t + 1)
                ng = mod(nq, groups)
                load_group(first_of(EARLY + div(nq, groups), ng), ng, 1 - slot)

            @pl.when(q == 0)
            def _():
                @pl.when(b > 0)
                def _():
                    give_back(b - 1)

                wait(h.at[b], hr.at[b])

            group_part(slot, g, b, 0)
            return 0

        lax.fori_loop(0, n_visits, visit, 0)
        run(lambda b: wait(h.at[b], hs.at[b]), 0, blocks - 2)
        give_back(blocks - 1)

        def relay_out(i, _):
            @pl.when(i < n_relay)
            def _():
                wait(rin.at[i], rsem.at[0, i])
                send(rin.at[i], rx.at[i], psem.at[0, 0], rsem.at[1, i], flip_tp, 0, rep)

            @pl.when(i >= 1)
            def _():
                q = i - 1
                wait(rx.at[q], rsem.at[1, q])
                b, j, first = 0, 0, 0
                for rb, n in RELAYED:
                    b = jnp.where(q >= first, rb, b)
                    j = jnp.where(q >= first, q - first, j)
                    first += n
                send(rx.at[q], out.at[piece_rows(flip_tp, b, j)], psem.at[0, 1], osem.at[0], tp, 1, rep)

            return 0

        lax.fori_loop(0, n_relay + 1, relay_out, 0)
        wait(rin, psem.at[0, 0])
        wait(rx, psem.at[0, 1])
        run(wait_sent, steps - STAGE_SLOTS, steps)
        run(lambda b: wait(h.at[b], hs.at[b]), blocks - 2, blocks)
        for l in range(2 * EARLY):
            n = count(l * chunks, (l + 1) * chunks, relayed)
            if n:
                wait(wbuf.at[pl.ds(0, n), :, 0, 0, 0], ss.at[0, l])
        for i in range(2):
            wait(wbuf.at[pl.ds(0, chunks), :, 0, 0, 0], ss.at[1, i])
        for l in range(EARLY + 1):
            for m in range(2):
                n = count(l * chunks, (l + 1) * chunks, lambda f: f % 2 == m)
                wait(wbuf.at[pl.ds(0, n), :, 0, 0, 0], ss.at[2 + m, l])
            wait(wbuf.at[pl.ds(0, chunks), :, :, 0], ss.at[4, l])

    @pl.when(side == 1)
    def _():
        def y_stage(e):
            c, l = chunk_of(e), div(e, chunks)
            wait(both(c, own), ysem.at[e])
            send(both(c, own), both(c, own), ss.at[0, l], zsem(e), flip_tp, 1, rep)
            send(both(c, own), both(c, own), ss.at[1, l], xsem(e), tp, 1, flip_rep)

        def n_stage(e):
            c, l = chunk_of(e), div(e, chunks)
            wait(both(c, znb), zsem(e))
            wait(both(c, xnb), xsem(e))
            direct = jnp.logical_not(relayed(e))

            @pl.when(direct & jnp.logical_not(by_z(e)))
            def _():
                send(both(c, znb), both(c, znb), ss.at[2, l], dsem(e), tp, 1, flip_rep)

            @pl.when(direct & by_z(e))
            def _():
                send(both(c, xnb), both(c, xnb), ss.at[3, l], dsem(e), flip_tp, 1, rep)

        def d_stage(e):
            c = chunk_of(e)

            @pl.when(relayed(e))
            def _():
                wait(both(c, dia), rlsem.at[relay_index(e)])

            @pl.when(jnp.logical_not(relayed(e)))
            def _():
                wait(both(c, dia), dsem(e))

            send(core_half(c, k), core_half(c, k), ss.at[4, div(e, chunks)], sb_of(e), tp, 1, sib_rep)

        turn = EARLY * groups * blocks

        def front(i, t):
            a, s1, jump, s2 = FRONTS[i]
            late = 16 * jump + s1 * turn + s2 * (t - turn)
            return jnp.minimum(gen, a + (jnp.where(t <= turn, s1 * t, late) >> 4))

        def pload(b):
            rows = pl.ds(pl.multiple_of(tp * my_rows + b * BLOCK, BLOCK), BLOCK)
            return pltpu.make_async_copy(prompts.at[rows], rows_buf.at[b % 2], iosem.at[b % 2])

        pload(0).start()
        for b in range(blocks):
            if b + 1 < blocks:
                pload(b + 1).start()
            pload(b).wait()
            for j in range(pieces):
                h[b, :, pl.ds(j * PIECE, PIECE)] = rows_buf[b % 2, pl.ds(j * PIECE, PIECE), :].T

        n_pro = FRONTS[0][0]
        for e in range(n_pro):
            y_stage(e)
            for i, fn in ((1, n_stage), (2, d_stage)):
                if e >= n_pro - FRONTS[i][0]:
                    fn(e - (n_pro - FRONTS[i][0]))
        sb_wait(0, lead, sbsem.at[0])
        load_group(0, 0, 0)

        def put(b, j):
            src = rows_buf.at[mod(b, 2), pl.ds(j * PIECE, PIECE), :]
            rows = piece_rows(tp, b, j)
            pltpu.make_async_copy(src, out.at[rows], psem.at[mod(b, 2), 0]).start()
            n, i, first = 0, 0, 0
            for rb, m in RELAYED:
                n = jnp.where(b == rb, m, n)
                i = jnp.where(b == rb, first + min(j, m - 1), i)
                first += m

            @pl.when(j < n)
            def _():
                send(src, rin.at[i], psem.at[mod(b, 2), 1], rsem.at[0, i], tp, 0, rep)

            @pl.when(j >= n)
            def _():
                send(src, out.at[rows], psem.at[mod(b, 2), 1], osem.at[0], flip_tp, 1, rep)

        def put_wait(b):
            for i in range(2):
                wait(rows_buf.at[mod(b, 2)], psem.at[mod(b, 2), i])

        n_rest = groups - 1
        wide = turn - n_rest * blocks
        n_first = blocks - MORE
        n_tasks = n_first + blocks
        first_late, last_late = 2 * EARLY, 2 * EARLY + 1

        def late_task(q):
            u = q - 2 * FIRST_LATE
            each = (u >= 0) & (u < 2 * (n_first - FIRST_LATE))
            first = (q < FIRST_LATE) | (each & ((u & 1) == 0))
            b = jnp.where(q < FIRST_LATE, q, jnp.where(u < 0, q - FIRST_LATE, jnp.where(each, FIRST_LATE + (u >> 1), q - n_first)))
            return jnp.where(first, first_late, last_late), b

        def rest(t):
            u = t - wide
            b = (u * (128 // n_rest + 1)) >> 7
            return b, 1 + u - n_rest * b

        def give(b):
            send(h.at[b], h.at[b], hs.at[b], hr.at[b], tp, 0, rep)

        def forward(t):
            for i, fn in enumerate((y_stage, n_stage, d_stage)):
                run(fn, front(i, t), front(i, t + 1))

        def early_visit(t, _):
            split = t >= wide
            rb, rg = rest(t)
            l = jnp.where(split, EARLY - 1, div(t, groups * blocks))
            g = jnp.where(split, rg, mod(div(t, blocks), groups))
            b = jnp.where(split, rb, mod(t, blocks))
            slot = mod(jnp.where(split, t - wide + 1, div(t, blocks)), 2)

            @pl.when(split | (b == 0))
            def _():
                wait_group(g, slot)

            forward(t)

            @pl.when((t > wide) & (rg == 1))
            def _():
                give(rb - 1)

            @pl.when((t < wide) & (b == blocks // 2))
            def _():
                c0 = first_of(l, g) + width_of(g)
                ng = mod(g + 1, groups)
                sem = sb_of(c0)

                @pl.when(ng == 0)
                def _():
                    sb_wait(c0, lead, sem)

                @pl.when(ng > 0)
                def _():
                    sb_wait(c0, GROUP, sem)

                load_group(c0, ng, 1 - slot)

            @pl.when(t == wide)
            def _():
                for g_ in range(2, groups):
                    c0 = (EARLY - 1) * chunks + lead + (g_ - 1) * GROUP
                    sb_wait(c0, GROUP, sb_of(c0))

            @pl.when(split & (t + 1 < turn))
            def _():
                _, ng = rest(t + 1)
                load_group(first_of(EARLY - 1, ng), ng, 1 - slot)

            @pl.when(t == turn - 1)
            def _():
                sb_wait(2 * mid, chunks, sb_of(mid))
                load_group(2 * mid, 0, 1 - slot)

            group_part(slot, g, b, b)
            return 0

        def late_visit(u, _):
            l, b = late_task(div(u, groups))
            g = mod(u, groups)
            slot = mod(u + n_rest * blocks + 1, 2)
            hb = blocks + b
            wait_group(g, slot)

            @pl.when(u < FIRST_LATE * groups)
            def _():
                forward(turn + u)

                @pl.when(u == 0)
                def _():
                    give(blocks - 1)

                @pl.when(u == FIRST_LATE * groups - 1)
                def _():
                    for i, fn in enumerate((y_stage, n_stage, d_stage)):
                        run(fn, front(i, turn + u + 1), gen)
                    sb_wait(2 * mid + chunks, chunks, sb_of(mid + chunks))

            @pl.when(u + 1 < n_tasks * groups)
            def _():
                nl, _ = late_task(div(u + 1, groups))
                ng = mod(u + 1, groups)
                load_group(first_of(nl, ng), ng, 1 - slot)

            @pl.when((g == 0) & ((l == first_late) | (b >= n_first)))
            def _():
                wait(h.at[hb], hr.at[b])

            group_part(slot, g, hb, b)

            @pl.when((l == last_late) & (g == groups - 1))
            def _():
                @pl.when(b >= 2)
                def _():
                    put_wait(b - 2)

                for j in range(pieces):
                    cols = pl.ds(j * PIECE, PIECE)
                    rows_buf[mod(b, 2), cols, :] = h[hb, :, cols].T
                    if j >= 1:
                        put(b, j - 1)
                put(b, pieces - 1)

            return 0

        lax.fori_loop(0, turn, early_visit, 0)
        lax.fori_loop(0, n_tasks * groups, late_visit, 0)
        for b in range(blocks - 2, blocks):
            put_wait(b)
        run(lambda b: wait(h.at[b], hs.at[b]), 0, blocks)
        wait(out.at[pl.ds(pl.multiple_of(flip_tp * my_rows, BLOCK), my_rows)], osem.at[0])
        for l in range(2 * EARLY):
            for i in range(5):
                if i == 4:
                    wait(wbuf.at[pl.ds(0, chunks), :, :, 0], ss.at[i, l])
                else:
                    kinds = (None, None, lambda e: not relayed(e) and not by_z(e), lambda e: not relayed(e) and by_z(e))
                    n = chunks if i < 2 else count(l * chunks, (l + 1) * chunks, kinds[i])
                    wait(wbuf.at[pl.ds(0, n), :, 0, 0, 0], ss.at[i, l])


def finish_kernel(up, dn, rows, new_up, new_dn, out, buf, zbuf, lsem, ssem, zsem):
    layers = up.shape[0]
    n_rows = rows.shape[0]
    slots, band, hidden = buf.shape
    side = lax.axis_index("side")
    items = [(i, o, l) for l in range(layers) for i, o in ((up, new_up), (dn, new_dn))]
    piece = zbuf.shape[1]
    n_pieces = n_rows // piece
    n_slots = zbuf.shape[0]

    def pipeline(n, n_slots, load, store, zeros):
        for i in range(min(n_slots, n)):
            load(i).start()
        half = n_slots // 2
        done = 0
        for i in range(n):
            load(i).wait()
            store(i).start()
            upto = len(zeros) * (i + 1) // n
            for cp in zeros[done:upto]:
                cp.start()
            done = upto
            nxt = i + half
            if i >= half and nxt < n:
                store(nxt - n_slots).wait()
                load(nxt).start()
        for i in range(max(n - n_slots, 0), n):
            store(i).wait()
        for cp in zeros:
            cp.wait()

    @pl.when(side == 0)
    def _():
        zbuf[0] = jnp.zeros(zbuf.shape[1:], zbuf.dtype)
        zeros = [
            pltpu.make_async_copy(zbuf.at[0], out.at[pl.ds(i * piece, piece)], zsem.at[i]) for i in range(n_pieces)
        ]

        def load(i):
            src, _, l = items[i]
            return pltpu.make_async_copy(src.at[l], buf.at[i % slots], lsem.at[i % slots])

        def store(i):
            _, dst, l = items[i]
            return pltpu.make_async_copy(buf.at[i % slots], dst.at[l], ssem.at[i % slots])

        pipeline(len(items), slots, load, store, zeros)

    @pl.when(side == 1)
    def _():
        buf[0] = jnp.zeros(buf.shape[1:], buf.dtype)
        zeros = [pltpu.make_async_copy(buf.at[0], dst.at[l], zsem.at[i]) for i, (_, dst, l) in enumerate(items)]

        def load(i):
            return pltpu.make_async_copy(rows.at[pl.ds(i * piece, piece)], zbuf.at[i % n_slots], lsem.at[i % n_slots])

        def store(i):
            return pltpu.make_async_copy(zbuf.at[i % n_slots], out.at[pl.ds(i * piece, piece)], ssem.at[i % n_slots])

        pipeline(n_pieces, n_slots, load, store, zeros)


def solution(mesh):
    up_spec = P("side", None, ("rep", "tp"), None)
    down_spec = P("side", None, None, ("rep", "tp"))
    tok_spec = P("side", "rep", None, None)

    def device_step(w_up, w_down, g_up, g_down, learn_rate, prompts):
        layers, band, hidden = w_up.shape[1:]
        n_rows, d = prompts.shape[2:]
        chunks = hidden // UNIT
        total = layers * chunks
        my_rows = n_rows // 2
        blocks, pieces = my_rows // BLOCK, BLOCK // PIECE
        weights = (w_up[0], jnp.swapaxes(w_down[0], 1, 2), g_up[0], jnp.swapaxes(g_down[0], 1, 2))
        smem = pl.BlockSpec(memory_space=pltpu.SMEM)
        hbm = pl.BlockSpec(memory_space=pl.ANY)
        bf16 = jnp.bfloat16
        relay = jax.ShapeDtypeStruct((sum(n for _, n in RELAYED), PIECE, d), bf16)
        new_w = jax.ShapeDtypeStruct((layers, band, hidden), jnp.float32)
        rows = jax.ShapeDtypeStruct((n_rows, d), bf16)
        rows_mid, up_mid, dn_mid, _, _, _ = pl.pallas_call(
            sync_kernel,
            name="sync_and_forward",
            out_shape=(
                rows,
                new_w,
                new_w,
                jax.ShapeDtypeStruct((total, 2, 2, 2, 2, band, UNIT), bf16),
                relay,
                relay,
            ),
            in_specs=[smem] + [hbm] * 5,
            out_specs=(hbm,) * 6,
            scratch_shapes=[
                pltpu.VMEM((2 * blocks, d, BLOCK), bf16),
                pltpu.VMEM((blocks, d, BLOCK), jnp.float32),
                pltpu.VMEM((2, GROUP, 2, 2, 2, 2, band, UNIT), bf16),
                pltpu.VMEM((LOAD_SLOTS, 4, band, UNIT), jnp.float32),
                pltpu.VMEM((LOAD_SLOTS, 2, band, UNIT), jnp.float32),
                pltpu.VMEM((STAGE_SLOTS, 2, band, UNIT), bf16),
                pltpu.VMEM((2, BLOCK, d), bf16),
                pltpu.SemaphoreType.DMA((2 * EARLY * chunks,)),
                pltpu.SemaphoreType.DMA((3, RING)),
                pltpu.SemaphoreType.DMA((EARLY * chunks // 6 + chunks // 3 + 1,)),
                pltpu.SemaphoreType.DMA((EARLY * (-(-chunks // GROUP)) + 2 * EARLY + 1,)),
                pltpu.SemaphoreType.DMA((5, 2 * EARLY)),
                pltpu.SemaphoreType.DMA((LOAD_SLOTS,)),
                pltpu.SemaphoreType.DMA((LOAD_SLOTS,)),
                pltpu.SemaphoreType.DMA((2,)),
                pltpu.SemaphoreType.DMA((STAGE_SLOTS, 2)),
                pltpu.SemaphoreType.DMA((STAGE_SLOTS,)),
                pltpu.SemaphoreType.DMA((2,)),
                pltpu.SemaphoreType.DMA((2, 2)),
                pltpu.SemaphoreType.DMA((1,)),
                pltpu.SemaphoreType.DMA((2, sum(n for _, n in RELAYED))),
                pltpu.SemaphoreType.DMA((blocks,)),
                pltpu.SemaphoreType.DMA((blocks,)),
            ],
            compiler_params=pltpu.CompilerParams(
                collective_id=0, has_side_effects=True, vmem_limit_bytes=60 * 1024 * 1024
            ),
        )(learn_rate, *weights, prompts[0, 0])
        new_up, new_dn, gen_out = pl.pallas_call(
            finish_kernel,
            name="write_outputs",
            out_shape=(new_w, new_w, rows),
            in_specs=[hbm] * 3,
            out_specs=(hbm,) * 3,
            scratch_shapes=[
                pltpu.VMEM((8, band, hidden), jnp.float32),
                pltpu.VMEM((8, n_rows // 16, d), bf16),
                pltpu.SemaphoreType.DMA((8,)),
                pltpu.SemaphoreType.DMA((8,)),
                pltpu.SemaphoreType.DMA((max(16, 2 * layers),)),
            ],
            compiler_params=pltpu.CompilerParams(vmem_limit_bytes=62 * 1024 * 1024),
        )(up_mid, dn_mid, rows_mid)
        return new_up[None], jnp.swapaxes(new_dn, 1, 2)[None], gen_out[None, None]

    return jax.shard_map(
        device_step,
        mesh=mesh,
        in_specs=(up_spec, down_spec, up_spec, down_spec, P("side"), tok_spec),
        out_specs=(up_spec, down_spec, tok_spec),
        check_vma=False,
    )
```

```python
import jax
import jax.numpy as jnp
from jax import lax
from jax.experimental import pallas as pl
from jax.experimental.pallas import tpu as pltpu
from jax.sharding import PartitionSpec as P

MESH = pl.DeviceIdType.MESH
UNIT = 256
GROUP = 5
BLOCK = 512
PIECE = 128
EARLY = 2
LOAD_SLOTS = 4
STAGE_SLOTS = 32
RING = 24
N_LAG, D_LAG = 3, 6
RELAY_LAG = 4
FIRST_LATE = 2
MORE = 2
RELAYED = ((5, 2), (6, 2))
FRONTS = ((10, 15, 1, 40), (8, 14, 1, 44), (6, 13, 3, 24))
GELU_A = 0.7978845608028654
GELU_B = 0.7978845608028654 * 0.044715


def div(a, n):
    if isinstance(a, int):
        return a // n
    if n & (n - 1) == 0:
        return a >> (n.bit_length() - 1)
    return (a * ((1 << 16) // n + 1)) >> 16


def mod(a, n):
    return a - n * div(a, n)


def gelu(a):
    return a * (0.5 * jnp.tanh(a * (GELU_A + GELU_B * (a * a))) + 0.5)


def sync_kernel(
    rate_ref, w_up, w_dn, g_up, g_dn, prompts, out, nu, nd, wbuf, rin, rx,
    h, p, wv, fin, fnew, stage, rows_buf,
    ysem, rs, rlsem, sbsem, ss, lsem, stsem, fsem, tss, csem, iosem, psem, osem, rsem, hs, hr,
):
    layers, band, hidden = w_up.shape
    chunks = hidden // UNIT
    n_relay = sum(n for _, n in RELAYED)
    groups = -(-chunks // GROUP)
    lead = chunks - (groups - 1) * GROUP
    mid = EARLY * chunks
    gen = 2 * mid
    n_rows, d = out.shape
    my_rows = n_rows // 2
    blocks = my_rows // BLOCK
    pieces = BLOCK // PIECE

    tp = lax.axis_index("tp")
    side = lax.axis_index("side")
    rep = lax.axis_index("rep")
    x, k = rep // 2, rep % 2
    flip_tp = 1 - tp
    flip_rep = (1 - x) * 2 + k
    sib_rep = x * 2 + (1 - k)

    own, znb, xnb, dia = (x, tp), (x, flip_tp), (1 - x, tp), (1 - x, flip_tp)

    def both(c, b):
        return wbuf.at[c, :, b[0], k, b[1]]

    def core_half(c, core):
        return wbuf.at[c, :, :, core]

    def chunk_of(e):
        return e + jnp.where(e >= mid, mid, 0)

    def relayed(e):
        return ((mod(e, 6) == 5) & (e < mid)) | ((mod(e, 3) == 2) & (e >= mid + chunks))

    def by_z(e):
        return ((mod(div(e, 6) + mod(e, 6), 2) == 1) & (e < mid + chunks)) | ((mod(e, 3) == 1) & (e >= mid + chunks))

    def count(e0, e1, fn):
        return sum(1 for e in range(e0, e1) if fn(e))

    n_early = count(0, mid, relayed)

    def relay_index(e):
        return jnp.where(e < mid, div(e, 6), n_early + div(e - mid - chunks, 3))

    def zsem(e):
        return rs.at[0, mod(e, RING)]

    def xsem(e):
        return rs.at[1, mod(e, RING)]

    def dsem(e):
        return rs.at[2, mod(e, RING)]

    def sb_of(e):
        l = div(e, chunks)
        j = e - l * chunks
        g = jnp.where(j < lead, 0, 1 + div(j - lead, GROUP))
        return sbsem.at[jnp.where(e < mid, l * groups + g, EARLY * groups + l - EARLY)]

    def sb_mid(f):
        return sbsem.at[EARLY * groups + EARLY + div(f, chunks)]

    def send(src, dst, ssem, rsem_, t, s, r):
        pltpu.make_async_remote_copy(
            src_ref=src, dst_ref=dst, send_sem=ssem, recv_sem=rsem_,
            device_id={"tp": t, "side": s, "rep": r}, device_id_type=MESH,
        ).start()

    def wait(ref, sem):
        pltpu.make_async_copy(ref, ref, sem).wait()

    def run(fn, lo, hi):
        def body(c, _):
            fn(c)
            return 0

        lax.fori_loop(lo, hi, body, 0)

    def piece_rows(t, b, j):
        return pl.ds(pl.multiple_of(t * my_rows + b * BLOCK + j * PIECE, PIECE), PIECE)

    def sb_wait(c0, width, sem):
        wait(wbuf.at[pl.ds(c0, width), :, :, 1 - k], sem)

    def load_group(c0, g, slot):
        def load(j):
            pltpu.make_async_copy(wbuf.at[c0 + j], wv.at[slot, j], fsem.at[slot]).start()

        for j in range(lead):
            load(j)

        @pl.when(g > 0)
        def _():
            for j in range(lead, GROUP):
                load(j)

    def wait_group(g, slot):
        @pl.when(g == 0)
        def _():
            wait(wv.at[slot, pl.ds(0, lead)], fsem.at[slot])

        @pl.when(g > 0)
        def _():
            wait(wv.at[slot], fsem.at[slot])

    def width_of(g):
        return jnp.where(g == 0, lead, GROUP)

    def first_of(l, g):
        return l * chunks + jnp.where(g == 0, 0, lead + (g - 1) * GROUP)

    def matmuls(slot, hb, width):
        def weight(j, m):
            return wv[slot, j, m].reshape(d, UNIT)

        rows = h[hb]
        acts = []
        for j in range(width):
            a = lax.dot_general(weight(j, 0), rows, (((0,), (0,)), ((), ())), preferred_element_type=jnp.float32)
            acts.append(gelu(a).astype(jnp.bfloat16))
        down = jnp.concatenate([weight(j, 1) for j in range(width)], axis=1)
        return jnp.dot(down, jnp.concatenate(acts, axis=0), preferred_element_type=jnp.float32)

    def group_part(slot, g, hb, pb):
        @pl.when(g == 0)
        def _():
            p[pb] = matmuls(slot, hb, lead)

        @pl.when((g > 0) & (g < groups - 1))
        def _():
            p[pb] = p[pb] + matmuls(slot, hb, GROUP)

        @pl.when(g == groups - 1)
        def _():
            s = p[pb] + matmuls(slot, hb, GROUP)
            h[hb] = (h[hb].astype(jnp.float32) + s).astype(jnp.bfloat16)

    parts = ((w_up, g_up, nu), (w_dn, g_dn, nd))
    steps = gen + mid

    def chunk_at(s):
        return jnp.where(mod(s, 3) == 2, mid + div(s, 3), chunk_of(2 * div(s, 3) + mod(s, 3)))

    def cols_of(c):
        return div(c, chunks), pl.ds(pl.multiple_of(mod(c, chunks) * UNIT, UNIT), UNIT)

    def loads(s):
        l, cols = cols_of(chunk_at(s))
        slot = mod(s, LOAD_SLOTS)
        for m in range(2):
            for i, r in enumerate(parts[m][:2]):
                pltpu.make_async_copy(r.at[l, :, cols], fin.at[slot, 2 * m + i], lsem.at[slot]).start()

    def cast(s):
        slot, lslot = mod(s, STAGE_SLOTS), mod(s, LOAD_SLOTS)
        wait(fin.at[lslot], lsem.at[lslot])
        rate = rate_ref[0]
        for m in range(2):
            new = fin[lslot, 2 * m] - rate * fin[lslot, 2 * m + 1]
            fnew[lslot, m] = new
            stage[slot, m] = new.astype(jnp.bfloat16)

    @pl.when(side == 0)
    def _():
        for s in range(LOAD_SLOTS):
            loads(s)
        cast(0)

    barrier = pltpu.get_barrier_semaphore()
    peers = [(tp, 1 - side, rep)] + [
        (t, side, r) for t, r in ((flip_tp, rep), (tp, flip_rep), (flip_tp, flip_rep), (tp, sib_rep))
    ]
    for t, s_, r in peers:
        pl.semaphore_signal(
            barrier, inc=1, device_id={"tp": t, "side": s_, "rep": r}, device_id_type=MESH
        )
    pl.semaphore_wait(barrier, len(peers))

    @pl.when(side == 0)
    def _():
        def stores(s):
            l, cols = cols_of(chunk_at(s))
            slot = mod(s, LOAD_SLOTS)
            for m in range(2):
                pltpu.make_async_copy(fnew.at[slot, m], parts[m][2].at[l, :, cols], stsem.at[slot]).start()

        def wait_stored(s):
            slot = mod(s, LOAD_SLOTS)
            wait(fnew.at[slot], stsem.at[slot])

        def own_copy(s):
            slot = s % STAGE_SLOTS
            return pltpu.make_async_copy(stage.at[slot], both(chunk_at(s), own), csem.at[slot])

        def gathered_too(s):
            e = 2 * (s // 3) + s % 3
            return (s % 3 != 2) & (e >= mid) & (e < mid + chunks)

        def post(s):
            slot = s % STAGE_SLOTS
            src = stage.at[slot]
            stores(s)

            @pl.when(s % 3 != 2)
            def _():
                e = 2 * (s // 3) + s % 3
                c = chunk_of(e)
                send(src, both(c, own), tss.at[slot, 0], ysem.at[e], tp, 1, rep)

                @pl.when(gathered_too(s))
                def _():
                    own_copy(s).start()

                @pl.when(relayed(e))
                def _():
                    send(src, both(c, own), tss.at[slot, 1], rlsem.at[relay_index(e)], flip_tp, 0, flip_rep)

                @pl.when(e >= RELAY_LAG)
                def _():
                    relay(e - RELAY_LAG)

            @pl.when(s % 3 == 2)
            def _():
                f = div(s, 3)
                c = mid + f
                own_copy(s).start()
                send(src, both(c, own), tss.at[slot, 0], zsem(f), flip_tp, 0, rep)
                send(src, both(c, own), tss.at[slot, 1], xsem(f), tp, 0, flip_rep)

        def relay(e):
            @pl.when(relayed(e))
            def _():
                c = chunk_of(e)
                sem = rlsem.at[relay_index(e)]
                wait(both(c, dia), sem)
                send(both(c, dia), both(c, dia), ss.at[0, div(e, chunks)], sem, tp, 1, rep)

        def wait_sent(s):
            slot = s % STAGE_SLOTS
            is_mid = s % 3 == 2
            wait(stage.at[slot], tss.at[slot, 0])

            @pl.when(is_mid | relayed(2 * (s // 3) + s % 3))
            def _():
                wait(stage.at[slot], tss.at[slot, 1])

        def own_stage(f):
            c = mid + f
            send(both(c, own), both(c, own), ss.at[1, 0], zsem(f), flip_tp, 0, rep)
            send(both(c, own), both(c, own), ss.at[1, 1], xsem(f), tp, 0, flip_rep)

        def n_stage(f):
            c = mid + f
            wait(both(c, znb), zsem(f))
            wait(both(c, xnb), xsem(f))

            @pl.when(mod(f, 2) == 0)
            def _():
                send(both(c, znb), both(c, znb), ss.at[2, div(f, chunks)], dsem(f), tp, 0, flip_rep)

            @pl.when(mod(f, 2) == 1)
            def _():
                send(both(c, xnb), both(c, xnb), ss.at[3, div(f, chunks)], dsem(f), flip_tp, 0, rep)

        def d_stage(f):
            c = mid + f
            wait(both(c, dia), dsem(f))

            @pl.when(f < mid)
            def _():
                own_copy(3 * f + 2).wait()

            send(core_half(c, k), core_half(c, k), ss.at[4, div(f, chunks)], sb_mid(f), tp, 0, sib_rep)

        def body(s, _):
            @pl.when(s + LOAD_SLOTS - 1 < steps)
            def _():
                loads(s + LOAD_SLOTS - 1)

            @pl.when(s >= STAGE_SLOTS)
            def _():
                wait_sent(s - STAGE_SLOTS)

                @pl.when(gathered_too(s - STAGE_SLOTS))
                def _():
                    own_copy(s - STAGE_SLOTS).wait()

            @pl.when(s >= LOAD_SLOTS)
            def _():
                wait_stored(s - LOAD_SLOTS)

            cast(s)
            @pl.when(s >= 2)
            def _():
                post(s - 1)

            @pl.when(s % 3 == 2)
            def _():
                f = s // 3

                @pl.when(f >= N_LAG)
                def _():
                    n_stage(f - N_LAG)

                @pl.when(f >= D_LAG)
                def _():
                    d_stage(f - D_LAG)

            return 0

        post(0)
        lax.fori_loop(1, steps, body, 0)
        post(steps - 1)
        run(relay, gen - RELAY_LAG, gen)
        run(n_stage, mid - N_LAG, mid)
        run(d_stage, mid - D_LAG, mid)
        for s in range(steps - LOAD_SLOTS, steps):
            wait_stored(s)
        for s in range(steps - STAGE_SLOTS, steps):
            if s % 3 != 2 and mid <= 2 * (s // 3) + s % 3 < mid + chunks:
                own_copy(s).wait()
        for l in range(EARLY):
            sb_wait(mid + l * chunks, chunks, sb_mid(l * chunks))

        load_group(mid, 0, 0)
        per_block = EARLY * groups
        few = (blocks - MORE) * per_block
        n_visits = few + MORE * (per_block + groups)

        def place(t):
            u = t - few
            more = jnp.where(u >= per_block + groups, 1, 0)
            b = jnp.where(t < few, div(t, per_block), blocks - MORE + more)
            return b, jnp.where(t < few, mod(t, per_block), u - more * (per_block + groups))

        def give_back(b):
            send(h.at[b], h.at[blocks + b], hs.at[b], hr.at[b], tp, 1, rep)

        def visit(t, _):
            b, q = place(t)
            g, slot = mod(q, groups), mod(q, 2)
            wait_group(g, slot)

            for fn, after in ((own_stage, 0), (n_stage, 8), (d_stage, 18)):

                @pl.when((t >= after) & (t < after + chunks))
                def _():
                    fn(mid + t - after)

            @pl.when(t == few)
            def _():
                sb_wait(2 * mid, chunks, sb_mid(mid))

            @pl.when(t + 1 < n_visits)
            def _():
                _, nq = place(t + 1)
                ng = mod(nq, groups)
                load_group(first_of(EARLY + div(nq, groups), ng), ng, 1 - slot)

            @pl.when(q == 0)
            def _():
                @pl.when(b > 0)
                def _():
                    give_back(b - 1)

                wait(h.at[b], hr.at[b])

            group_part(slot, g, b, 0)
            return 0

        lax.fori_loop(0, n_visits, visit, 0)
        run(lambda b: wait(h.at[b], hs.at[b]), 0, blocks - 2)
        give_back(blocks - 1)

        def relay_out(i, _):
            @pl.when(i < n_relay)
            def _():
                wait(rin.at[i], rsem.at[0, i])
                send(rin.at[i], rx.at[i], psem.at[0, 0], rsem.at[1, i], flip_tp, 0, rep)

            @pl.when(i >= 1)
            def _():
                q = i - 1
                wait(rx.at[q], rsem.at[1, q])
                b, j, first = 0, 0, 0
                for rb, n in RELAYED:
                    b = jnp.where(q >= first, rb, b)
                    j = jnp.where(q >= first, q - first, j)
                    first += n
                send(rx.at[q], out.at[piece_rows(flip_tp, b, j)], psem.at[0, 1], osem.at[0], tp, 1, rep)

            return 0

        lax.fori_loop(0, n_relay + 1, relay_out, 0)
        wait(rin, psem.at[0, 0])
        wait(rx, psem.at[0, 1])
        run(wait_sent, steps - STAGE_SLOTS, steps)
        run(lambda b: wait(h.at[b], hs.at[b]), blocks - 2, blocks)
        for l in range(2 * EARLY):
            n = count(l * chunks, (l + 1) * chunks, relayed)
            if n:
                wait(wbuf.at[pl.ds(0, n), :, 0, 0, 0], ss.at[0, l])
        for i in range(2):
            wait(wbuf.at[pl.ds(0, chunks), :, 0, 0, 0], ss.at[1, i])
        for l in range(EARLY + 1):
            for m in range(2):
                n = count(l * chunks, (l + 1) * chunks, lambda f: f % 2 == m)
                wait(wbuf.at[pl.ds(0, n), :, 0, 0, 0], ss.at[2 + m, l])
            wait(wbuf.at[pl.ds(0, chunks), :, :, 0], ss.at[4, l])

    @pl.when(side == 1)
    def _():
        def y_stage(e):
            c, l = chunk_of(e), div(e, chunks)
            wait(both(c, own), ysem.at[e])
            send(both(c, own), both(c, own), ss.at[0, l], zsem(e), flip_tp, 1, rep)
            send(both(c, own), both(c, own), ss.at[1, l], xsem(e), tp, 1, flip_rep)

        def n_stage(e):
            c, l = chunk_of(e), div(e, chunks)
            wait(both(c, znb), zsem(e))
            wait(both(c, xnb), xsem(e))
            direct = jnp.logical_not(relayed(e))

            @pl.when(direct & jnp.logical_not(by_z(e)))
            def _():
                send(both(c, znb), both(c, znb), ss.at[2, l], dsem(e), tp, 1, flip_rep)

            @pl.when(direct & by_z(e))
            def _():
                send(both(c, xnb), both(c, xnb), ss.at[3, l], dsem(e), flip_tp, 1, rep)

        def d_stage(e):
            c = chunk_of(e)

            @pl.when(relayed(e))
            def _():
                wait(both(c, dia), rlsem.at[relay_index(e)])

            @pl.when(jnp.logical_not(relayed(e)))
            def _():
                wait(both(c, dia), dsem(e))

            send(core_half(c, k), core_half(c, k), ss.at[4, div(e, chunks)], sb_of(e), tp, 1, sib_rep)

        turn = EARLY * groups * blocks

        def front(i, t):
            a, s1, jump, s2 = FRONTS[i]
            late = 16 * jump + s1 * turn + s2 * (t - turn)
            return jnp.minimum(gen, a + (jnp.where(t <= turn, s1 * t, late) >> 4))

        def pload(b):
            rows = pl.ds(pl.multiple_of(tp * my_rows + b * BLOCK, BLOCK), BLOCK)
            return pltpu.make_async_copy(prompts.at[rows], rows_buf.at[b % 2], iosem.at[b % 2])

        pload(0).start()
        for b in range(blocks):
            if b + 1 < blocks:
                pload(b + 1).start()
            pload(b).wait()
            for j in range(pieces):
                h[b, :, pl.ds(j * PIECE, PIECE)] = rows_buf[b % 2, pl.ds(j * PIECE, PIECE), :].T

        n_pro = FRONTS[0][0]
        for e in range(n_pro):
            y_stage(e)
            for i, fn in ((1, n_stage), (2, d_stage)):
                if e >= n_pro - FRONTS[i][0]:
                    fn(e - (n_pro - FRONTS[i][0]))
        sb_wait(0, lead, sbsem.at[0])
        load_group(0, 0, 0)

        def put(b, j):
            src = rows_buf.at[mod(b, 2), pl.ds(j * PIECE, PIECE), :]
            rows = piece_rows(tp, b, j)
            pltpu.make_async_copy(src, out.at[rows], psem.at[mod(b, 2), 0]).start()
            n, i, first = 0, 0, 0
            for rb, m in RELAYED:
                n = jnp.where(b == rb, m, n)
                i = jnp.where(b == rb, first + min(j, m - 1), i)
                first += m

            @pl.when(j < n)
            def _():
                send(src, rin.at[i], psem.at[mod(b, 2), 1], rsem.at[0, i], tp, 0, rep)

            @pl.when(j >= n)
            def _():
                send(src, out.at[rows], psem.at[mod(b, 2), 1], osem.at[0], flip_tp, 1, rep)

        def put_wait(b):
            for i in range(2):
                wait(rows_buf.at[mod(b, 2)], psem.at[mod(b, 2), i])

        n_rest = groups - 1
        wide = turn - n_rest * blocks
        n_first = blocks - MORE
        n_tasks = n_first + blocks
        first_late, last_late = 2 * EARLY, 2 * EARLY + 1

        def late_task(q):
            u = q - 2 * FIRST_LATE
            each = (u >= 0) & (u < 2 * (n_first - FIRST_LATE))
            first = (q < FIRST_LATE) | (each & ((u & 1) == 0))
            b = jnp.where(q < FIRST_LATE, q, jnp.where(u < 0, q - FIRST_LATE, jnp.where(each, FIRST_LATE + (u >> 1), q - n_first)))
            return jnp.where(first, first_late, last_late), b

        def rest(t):
            u = t - wide
            b = (u * (128 // n_rest + 1)) >> 7
            return b, 1 + u - n_rest * b

        def give(b):
            send(h.at[b], h.at[b], hs.at[b], hr.at[b], tp, 0, rep)

        def forward(t):
            for i, fn in enumerate((y_stage, n_stage, d_stage)):
                run(fn, front(i, t), front(i, t + 1))

        def early_visit(t, _):
            split = t >= wide
            rb, rg = rest(t)
            l = jnp.where(split, EARLY - 1, div(t, groups * blocks))
            g = jnp.where(split, rg, mod(div(t, blocks), groups))
            b = jnp.where(split, rb, mod(t, blocks))
            slot = mod(jnp.where(split, t - wide + 1, div(t, blocks)), 2)

            @pl.when(split | (b == 0))
            def _():
                wait_group(g, slot)

            forward(t)

            @pl.when((t > wide) & (rg == 1))
            def _():
                give(rb - 1)

            @pl.when((t < wide) & (b == blocks // 2))
            def _():
                c0 = first_of(l, g) + width_of(g)
                ng = mod(g + 1, groups)
                sem = sb_of(c0)

                @pl.when(ng == 0)
                def _():
                    sb_wait(c0, lead, sem)

                @pl.when(ng > 0)
                def _():
                    sb_wait(c0, GROUP, sem)

                load_group(c0, ng, 1 - slot)

            @pl.when(t == wide)
            def _():
                for g_ in range(2, groups):
                    c0 = (EARLY - 1) * chunks + lead + (g_ - 1) * GROUP
                    sb_wait(c0, GROUP, sb_of(c0))

            @pl.when(split & (t + 1 < turn))
            def _():
                _, ng = rest(t + 1)
                load_group(first_of(EARLY - 1, ng), ng, 1 - slot)

            @pl.when(t == turn - 1)
            def _():
                sb_wait(2 * mid, chunks, sb_of(mid))
                load_group(2 * mid, 0, 1 - slot)

            group_part(slot, g, b, b)
            return 0

        def late_visit(u, _):
            l, b = late_task(div(u, groups))
            g = mod(u, groups)
            slot = mod(u + n_rest * blocks + 1, 2)
            hb = blocks + b
            wait_group(g, slot)

            @pl.when(u < FIRST_LATE * groups)
            def _():
                forward(turn + u)

                @pl.when(u == 0)
                def _():
                    give(blocks - 1)

                @pl.when(u == FIRST_LATE * groups - 1)
                def _():
                    for i, fn in enumerate((y_stage, n_stage, d_stage)):
                        run(fn, front(i, turn + u + 1), gen)
                    sb_wait(2 * mid + chunks, chunks, sb_of(mid + chunks))

            @pl.when(u + 1 < n_tasks * groups)
            def _():
                nl, _ = late_task(div(u + 1, groups))
                ng = mod(u + 1, groups)
                load_group(first_of(nl, ng), ng, 1 - slot)

            @pl.when((g == 0) & ((l == first_late) | (b >= n_first)))
            def _():
                wait(h.at[hb], hr.at[b])

            group_part(slot, g, hb, b)

            @pl.when((l == last_late) & (g == groups - 1))
            def _():
                @pl.when(b >= 2)
                def _():
                    put_wait(b - 2)

                for j in range(pieces):
                    cols = pl.ds(j * PIECE, PIECE)
                    rows_buf[mod(b, 2), cols, :] = h[hb, :, cols].T
                    if j >= 1:
                        put(b, j - 1)
                put(b, pieces - 1)

            return 0

        lax.fori_loop(0, turn, early_visit, 0)
        lax.fori_loop(0, n_tasks * groups, late_visit, 0)
        for b in range(blocks - 2, blocks):
            put_wait(b)
        run(lambda b: wait(h.at[b], hs.at[b]), 0, blocks)
        wait(out.at[pl.ds(pl.multiple_of(flip_tp * my_rows, BLOCK), my_rows)], osem.at[0])
        for l in range(2 * EARLY):
            for i in range(5):
                if i == 4:
                    wait(wbuf.at[pl.ds(0, chunks), :, :, 0], ss.at[i, l])
                else:
                    kinds = (None, None, lambda e: not relayed(e) and not by_z(e), lambda e: not relayed(e) and by_z(e))
                    n = chunks if i < 2 else count(l * chunks, (l + 1) * chunks, kinds[i])
                    wait(wbuf.at[pl.ds(0, n), :, 0, 0, 0], ss.at[i, l])


def finish_kernel(up, dn, rows, new_up, new_dn, out, buf, zbuf, lsem, ssem, zsem):
    layers = up.shape[0]
    n_rows = rows.shape[0]
    slots, band, hidden = buf.shape
    side = lax.axis_index("side")
    items = [(i, o, l) for l in range(layers) for i, o in ((up, new_up), (dn, new_dn))]
    piece = zbuf.shape[1]
    n_pieces = n_rows // piece
    n_slots = zbuf.shape[0]

    def pipeline(n, n_slots, load, store, zeros):
        for i in range(min(n_slots, n)):
            load(i).start()
        half = n_slots // 2
        done = 0
        for i in range(n):
            load(i).wait()
            store(i).start()
            upto = len(zeros) * (i + 1) // n
            for cp in zeros[done:upto]:
                cp.start()
            done = upto
            nxt = i + half
            if i >= half and nxt < n:
                store(nxt - n_slots).wait()
                load(nxt).start()
        for i in range(max(n - n_slots, 0), n):
            store(i).wait()
        for cp in zeros:
            cp.wait()

    @pl.when(side == 0)
    def _():
        zbuf[0] = jnp.zeros(zbuf.shape[1:], zbuf.dtype)
        zeros = [
            pltpu.make_async_copy(zbuf.at[0], out.at[pl.ds(i * piece, piece)], zsem.at[i]) for i in range(n_pieces)
        ]

        def load(i):
            src, _, l = items[i]
            return pltpu.make_async_copy(src.at[l], buf.at[i % slots], lsem.at[i % slots])

        def store(i):
            _, dst, l = items[i]
            return pltpu.make_async_copy(buf.at[i % slots], dst.at[l], ssem.at[i % slots])

        pipeline(len(items), slots, load, store, zeros)

    @pl.when(side == 1)
    def _():
        buf[0] = jnp.zeros(buf.shape[1:], buf.dtype)
        zeros = [pltpu.make_async_copy(buf.at[0], dst.at[l], zsem.at[i]) for i, (_, dst, l) in enumerate(items)]

        def load(i):
            return pltpu.make_async_copy(rows.at[pl.ds(i * piece, piece)], zbuf.at[i % n_slots], lsem.at[i % n_slots])

        def store(i):
            return pltpu.make_async_copy(zbuf.at[i % n_slots], out.at[pl.ds(i * piece, piece)], ssem.at[i % n_slots])

        pipeline(n_pieces, n_slots, load, store, zeros)


def solution(mesh):
    up_spec = P("side", None, ("rep", "tp"), None)
    down_spec = P("side", None, None, ("rep", "tp"))
    tok_spec = P("side", "rep", None, None)

    def device_step(w_up, w_down, g_up, g_down, learn_rate, prompts):
        layers, band, hidden = w_up.shape[1:]
        n_rows, d = prompts.shape[2:]
        chunks = hidden // UNIT
        total = layers * chunks
        my_rows = n_rows // 2
        blocks, pieces = my_rows // BLOCK, BLOCK // PIECE
        weights = (w_up[0], jnp.swapaxes(w_down[0], 1, 2), g_up[0], jnp.swapaxes(g_down[0], 1, 2))
        smem = pl.BlockSpec(memory_space=pltpu.SMEM)
        hbm = pl.BlockSpec(memory_space=pl.ANY)
        bf16 = jnp.bfloat16
        relay = jax.ShapeDtypeStruct((sum(n for _, n in RELAYED), PIECE, d), bf16)
        new_w = jax.ShapeDtypeStruct((layers, band, hidden), jnp.float32)
        rows = jax.ShapeDtypeStruct((n_rows, d), bf16)
        rows_mid, up_mid, dn_mid, _, _, _ = pl.pallas_call(
            sync_kernel,
            name="sync_and_forward",
            out_shape=(
                rows,
                new_w,
                new_w,
                jax.ShapeDtypeStruct((total, 2, 2, 2, 2, band, UNIT), bf16),
                relay,
                relay,
            ),
            in_specs=[smem] + [hbm] * 5,
            out_specs=(hbm,) * 6,
            scratch_shapes=[
                pltpu.VMEM((2 * blocks, d, BLOCK), bf16),
                pltpu.VMEM((blocks, d, BLOCK), jnp.float32),
                pltpu.VMEM((2, GROUP, 2, 2, 2, 2, band, UNIT), bf16),
                pltpu.VMEM((LOAD_SLOTS, 4, band, UNIT), jnp.float32),
                pltpu.VMEM((LOAD_SLOTS, 2, band, UNIT), jnp.float32),
                pltpu.VMEM((STAGE_SLOTS, 2, band, UNIT), bf16),
                pltpu.VMEM((2, BLOCK, d), bf16),
                pltpu.SemaphoreType.DMA((2 * EARLY * chunks,)),
                pltpu.SemaphoreType.DMA((3, RING)),
                pltpu.SemaphoreType.DMA((EARLY * chunks // 6 + chunks // 3 + 1,)),
                pltpu.SemaphoreType.DMA((EARLY * (-(-chunks // GROUP)) + 2 * EARLY + 1,)),
                pltpu.SemaphoreType.DMA((5, 2 * EARLY)),
                pltpu.SemaphoreType.DMA((LOAD_SLOTS,)),
                pltpu.SemaphoreType.DMA((LOAD_SLOTS,)),
                pltpu.SemaphoreType.DMA((2,)),
                pltpu.SemaphoreType.DMA((STAGE_SLOTS, 2)),
                pltpu.SemaphoreType.DMA((STAGE_SLOTS,)),
                pltpu.SemaphoreType.DMA((2,)),
                pltpu.SemaphoreType.DMA((2, 2)),
                pltpu.SemaphoreType.DMA((1,)),
                pltpu.SemaphoreType.DMA((2, sum(n for _, n in RELAYED))),
                pltpu.SemaphoreType.DMA((blocks,)),
                pltpu.SemaphoreType.DMA((blocks,)),
            ],
            compiler_params=pltpu.CompilerParams(
                collective_id=0, has_side_effects=True, vmem_limit_bytes=60 * 1024 * 1024
            ),
        )(learn_rate, *weights, prompts[0, 0])
        new_up, new_dn, gen_out = pl.pallas_call(
            finish_kernel,
            name="write_outputs",
            out_shape=(new_w, new_w, rows),
            in_specs=[hbm] * 3,
            out_specs=(hbm,) * 3,
            scratch_shapes=[
                pltpu.VMEM((8, band, hidden), jnp.float32),
                pltpu.VMEM((8, n_rows // 16, d), bf16),
                pltpu.SemaphoreType.DMA((8,)),
                pltpu.SemaphoreType.DMA((8,)),
                pltpu.SemaphoreType.DMA((max(16, 2 * layers),)),
            ],
            compiler_params=pltpu.CompilerParams(vmem_limit_bytes=62 * 1024 * 1024),
        )(up_mid, dn_mid, rows_mid)
        return new_up[None], jnp.swapaxes(new_dn, 1, 2)[None], gen_out[None, None]

    return jax.shard_map(
        device_step,
        mesh=mesh,
        in_specs=(up_spec, down_spec, up_spec, down_spec, P("side"), tok_spec),
        out_specs=(up_spec, down_spec, tok_spec),
        check_vma=False,
    )
```
